32 devices in a mesh: gx: 4 (over y, x), gy: 2 (over core), gz: 4 (over z).
Axes of the slice: x: 2, y: 2, z: 4, core: 2. Of those that a mesh axis runs over, the one named last changes fastest.
Arguments:
- old_pos: float32 [3, 4, 2, 4, 1536], P(None, 'gx', 'gy', 'gz'), may hold values from -6 to 6
- displacement: float32 [3, 4, 2, 4, 1536], P(None, 'gx', 'gy', 'gz'), may hold values from -0.3 to 0.3
- inv_mass: float32 [4, 2, 4, 1536], P('gx', 'gy', 'gz'), may hold values from 0.0625 to 1
- bond_head: int32 [4, 2, 4, 1024], P('gx', 'gy', 'gz'), may hold values from 0 to 1535, as said below
- bond_tail: int32 [4, 2, 4, 1024], P('gx', 'gy', 'gz'), may hold values from 0 to 1967, as said below
- send_list: int32 [4, 2, 4, 16], P('gx', 'gy', 'gz'), may hold values from 0 to 1535, as said below
Outputs:
- new_pos: float32 [3, 4, 2, 4, 1536], P(None, 'gx', 'gy', 'gz')
- multipliers: float32 [4, 2, 4, 1024], P('gx', 'gy', 'gz')
The draws below stay inside these ranges and needn't reach their ends.
Inputs may be any that keep to these rules, and one draw needn't show every extreme that they name: `bond_head`: distinct atoms of the owning domain; no atom is the first atom of two constraints. `bond_tail`: below 1536: an atom of the owning domain other than the constraint's first atom, never in send_list; otherwise a slot 1536 + block * 16 + entry with block in 0..26 other than 13, distinct within a domain; 192 constraints of each domain use such slots. `send_list`: distinct atoms of the domain; a send atom is never a constraint's first atom and never a local second atom.
All inputs are finite; a program needn't handle non-finite values.
Results may differ from the reference program's by a relative error of at most 0.0011.
Values sent between devices are 32-bit elements; how exact they have to be, the bound alone decides.
No kernel may reach another device: no remote copies, remote signals or barrier semaphores. Data moves between devices by JAX's collectives and lax.ppermute only.
A program may use at most 64 MiB of HBM per device.

```python
import math
import jax
import jax.numpy as jnp
from jax import lax

ATOM_DEV = 1536
CON_DEV = 1024
SEND = 16
HALO_CON = 192
ORDER = 4
DOM_X = 4
DOM_Y = 2
DOM_Z = 4


def layout(key):
    base = jax.random.fold_in(key, 7)
    keys = jax.random.split(base, DOM_X * DOM_Y * DOM_Z)

    def domain(dom_key):
        key_perm, key_pick, key_slot = jax.random.split(dom_key, 3)
        order = jax.random.permutation(key_perm, ATOM_DEV).astype(jnp.int32)
        sending = order[ATOM_DEV - SEND:]
        heads = order[:CON_DEV]
        local_tail = order[1:CON_DEV + 1]
        picked = jax.random.permutation(key_pick, CON_DEV).astype(jnp.int32)[:HALO_CON]
        slots = jax.random.permutation(key_slot, 26 * SEND).astype(jnp.int32)[:HALO_CON]
        block = slots // SEND
        block = block + (block >= 13).astype(jnp.int32)
        halo_tail = ATOM_DEV + block * SEND + slots % SEND
        tails = local_tail.at[picked].set(halo_tail.astype(jnp.int32))
        return (sending, heads, tails)
    sending, heads, tails = jax.vmap(domain)(keys)
    return (sending.reshape(DOM_X, DOM_Y, DOM_Z, SEND).astype(jnp.int32), heads.reshape(DOM_X, DOM_Y, DOM_Z, CON_DEV).astype(jnp.int32), tails.reshape(DOM_X, DOM_Y, DOM_Z, CON_DEV).astype(jnp.int32))


def draw_bond_head(key, part):
    return layout(key)[1]


def draw_bond_tail(key, part):
    return layout(key)[2]


def draw_send_list(key, part):
    return layout(key)[0]


def block_scale(own_key, shape, cuts, smallest, high):
    def one(position, shards_of):
        heights = jax.random.uniform(jax.random.fold_in(jax.random.fold_in(own_key, 6), position), (shards_of,), jnp.float32, smallest / len(cuts), high / len(cuts))
        return jnp.repeat(jnp.exp(heights), shape[position] // shards_of).reshape((-1,) + (1,) * (len(shape) - position - 1))

    factor_of = one(*cuts[0])
    for cut in cuts[1:]:
        factor_of = factor_of * one(*cut)
    return factor_of


def scatter_about(rng, extent, width, most, pieces=(), kind=jnp.bfloat16):
    array = jax.random.normal(rng, extent, jnp.float32) * width
    if len(pieces) > 0:
        array = block_scale(rng, extent, pieces, -0.22, 0.18) * array
    return jnp.clip(array, min=-most, max=most).astype(kind)


def setup_inputs(seed: int = 0) -> dict:
    splits = jax.random.split(jax.random.key(seed), 7)
    old_pos = scatter_about(splits[0], (3, DOM_X, DOM_Y, DOM_Z, ATOM_DEV), 1.0, 6.0, ((1, 4), (2, 2), (3, 4)), jnp.float32)
    displacement = scatter_about(splits[1], (3, DOM_X, DOM_Y, DOM_Z, ATOM_DEV), 0.05, 0.3, ((1, 4), (2, 2), (3, 4)), jnp.float32)
    inv_mass = jnp.clip(jnp.exp(math.log(1.0) - 2.7725887 * jax.random.uniform(splits[2], (DOM_X, DOM_Y, DOM_Z, ATOM_DEV), jnp.float32) ** block_scale(splits[2], (DOM_X, DOM_Y, DOM_Z, ATOM_DEV), ((0, 4), (1, 2), (2, 4)), -0.2, 0.2)), 0.0625, 1.0)
    bond_head = draw_bond_head(jax.random.fold_in(splits[6], 71), 0)
    bond_tail = draw_bond_tail(jax.random.fold_in(splits[6], 71), 0)
    send_list = draw_send_list(jax.random.fold_in(splits[6], 71), 0)
    return {"old_pos": old_pos, "displacement": displacement, "inv_mass": inv_mass, "bond_head": bond_head, "bond_tail": bond_tail, "send_list": send_list}


def global_index(bond_head, bond_tail, send_list):
    axis_x = jnp.arange(DOM_X, dtype=jnp.int32)[:, None, None, None]
    axis_y = jnp.arange(DOM_Y, dtype=jnp.int32)[None, :, None, None]
    axis_z = jnp.arange(DOM_Z, dtype=jnp.int32)[None, None, :, None]
    flat_dev = (axis_x * DOM_Y + axis_y) * DOM_Z + axis_z
    head = (flat_dev * ATOM_DEV + bond_head).reshape(-1)
    is_local = bond_tail < ATOM_DEV
    slot = jnp.maximum(bond_tail - ATOM_DEV, 0)
    block = slot // SEND
    entry = slot % SEND
    near_x = (axis_x + block // 9 - 1) % DOM_X
    near_y = (axis_y + block // 3 % 3 - 1) % DOM_Y
    near_z = (axis_z + block % 3 - 1) % DOM_Z
    neigh = (near_x * DOM_Y + near_y) * DOM_Z + near_z
    remote = send_list.reshape(-1)[(neigh * SEND + entry).reshape(-1)].reshape(neigh.shape)
    tail = jnp.where(is_local, flat_dev * ATOM_DEV + bond_tail, neigh * ATOM_DEV + remote)
    return (head.astype(jnp.int32), tail.reshape(-1).astype(jnp.int32))

def reference(old_pos, displacement, inv_mass, bond_head, bond_tail, send_list):
    head, tail = global_index(bond_head, bond_tail, send_list)
    old_flat = old_pos.reshape(3, -1)
    pos_now = old_flat + displacement.reshape(3, -1)
    masses = inv_mass.reshape(1, -1)
    total_atoms = old_flat.shape[1]
    bond_old = old_flat[:, head] - old_flat[:, tail]
    length = jnp.maximum(jnp.sqrt(lax.optimization_barrier(jnp.sum(bond_old * bond_old, axis=0))), 0.5)
    direction = bond_old / length
    bond_scale = 1.0 / jnp.sqrt(masses[0, head] + masses[0, tail])

    def spread(values):
        weighted = bond_scale * values * direction
        buffer = jnp.zeros((3, total_atoms), jnp.float32)
        buffer = buffer.at[:, head].add(weighted).at[:, tail].add(-weighted)
        return masses * buffer

    def couple(values):
        shift_vec = spread(values)
        return values - bond_scale * lax.optimization_barrier(jnp.sum(direction * (shift_vec[:, head] - shift_vec[:, tail]), axis=0))

    def expand(right_side):
        solution = right_side
        series = right_side
        for sweep in range(ORDER):
            series = couple(series)
            solution = solution + series
        return solution
    right_one = bond_scale * (lax.optimization_barrier(jnp.sum(direction * (pos_now[:, head] - pos_now[:, tail]), axis=0)) - length)
    sol_one = expand(right_one)
    pos_now = pos_now - spread(sol_one)
    stretch = pos_now[:, head] - pos_now[:, tail]
    current = lax.optimization_barrier(jnp.sum(stretch * stretch, axis=0))
    target = jnp.sqrt(jnp.maximum(2.0 * length * length - current, 0.5 * length * length))
    sol_two = expand(bond_scale * (length - target))
    pos_now = pos_now - spread(sol_two)
    return (pos_now.reshape(old_pos.shape), (sol_one + sol_two).reshape(bond_head.shape))
```

```python
import math

import jax
import jax.numpy as jnp
from jax import lax
from jax.experimental import pallas as pl
from jax.experimental.pallas import tpu as pltpu
from jax.sharding import PartitionSpec as P

ORDER = 4
HALO = 192
LANES = 128
NQ = 11
AXES = ("gx", "gy", "gz")
OFFSETS = [(b // 9 - 1, b // 3 % 3 - 1, b % 3 - 1) for b in range(27)]
F32 = jnp.float32
I32 = jnp.int32
SYM = [(0, 0), (1, 1), (2, 2), (0, 1), (0, 2), (1, 2)]


def iota(shape, dim):
    return lax.broadcasted_iota(I32, shape, dim)


def pick(table, index):
    return jnp.take_along_axis(table, index, axis=1, mode="promise_in_bounds")


def spread_row(row, like):
    return jnp.broadcast_to(row, like.shape)


def gather_rows(rows, high, low, base=0):
    result = jnp.zeros(high.shape, rows[0].dtype)
    for r, row in enumerate(rows):
        result = jnp.where(high == base + r, pick(spread_row(row, high), low), result)
    return result


def value_rows(value):
    return [value[r:r + 1, :] for r in range(value.shape[0])]


def gather_value(value, index):
    return gather_rows(value_rows(value), index >> 7, index & 127)


def load_flat(ref, lead, scratch, base, count):
    for r in range(count):
        scratch[base + r:base + r + 1, :] = ref[(*lead, pl.ds(r * LANES, LANES))].reshape(1, LANES)


def axis_sizes(mesh):
    return tuple(mesh.shape[a] for a in AXES)


def my_place():
    return tuple(lax.axis_index(a) for a in AXES)


def one_hot_scatter(values, index, high_rows):
    parts = []
    spots = []
    for r in range(index.shape[0]):
        high = index[r:r + 1, :] >> 7
        low = index[r:r + 1, :] & 127
        hit = jnp.broadcast_to(high, (high_rows, LANES)) == iota((high_rows, LANES), 0)
        parts.append(jnp.concatenate(
            [jnp.where(hit, jnp.broadcast_to(v[r:r + 1, :], (high_rows, LANES)), 0.0) for v in values],
            axis=0).astype(jnp.bfloat16))
        spots.append(jnp.where(
            jnp.broadcast_to(low, (LANES, LANES)) == iota((LANES, LANES), 0), 1.0, 0.0).astype(jnp.bfloat16))
    left = jnp.concatenate(parts, axis=1)
    right = jnp.concatenate(spots, axis=1)
    table = lax.dot_general(left, right, (((1,), (1,)), ((), ())), preferred_element_type=F32)
    return [table[i * high_rows:(i + 1) * high_rows] for i in range(len(values))]


def inverse_tables(index, valid, high_rows):
    where_from = iota(index.shape, 0) * LANES + iota(index.shape, 1)
    spot = jnp.where(valid, index, -1)
    ones = jnp.ones(index.shape, F32)
    upper, lower, count = one_hot_scatter(
        [(where_from >> 5).astype(F32), (where_from & 31).astype(F32), ones], spot, high_rows)
    table = (upper * 32.0 + lower).astype(I32)
    return jnp.where(count > 0.5, table, -1), count


def send_kernel(size, old_ref, move_ref, mass_ref, send_ref, out_ref, table):
    atom_rows = size["atom_rows"]
    send = size["send"]
    pad_rows = size["atom_pad"]
    table[...] = jnp.zeros(table.shape, F32)
    for d in range(3):
        load_flat(old_ref, (d, 0, 0, 0), table, d * pad_rows, atom_rows)
        load_flat(move_ref, (d, 0, 0, 0), table, (3 + d) * pad_rows, atom_rows)
    load_flat(mass_ref, (0, 0, 0), table, 6 * pad_rows, atom_rows)
    lane = iota((pad_rows, LANES), 1)
    index = size["load_send"](send_ref)
    index = jnp.broadcast_to(index, (pad_rows, LANES))
    low = index & 127
    hit = (index >> 7) == iota((pad_rows, LANES), 0)
    message = jnp.zeros((1, LANES), F32)
    for q in range(7):
        got = jnp.where(hit, pick(table[q * pad_rows:(q + 1) * pad_rows, :], low), 0.0)
        row = jnp.sum(got, axis=0, keepdims=True)
        message = jnp.where(lane[0:1] // send == q, row, message)
    for d in range(out_ref.shape[0]):
        out_ref[d, :, :] = message


def chain_sum(value, prev, extra):
    def body(_, carry):
        total, current = carry
        current = gather_value(current, prev)
        return total + current, current

    return lax.fori_loop(0, extra, body, (value, value))[0]


class Local:
    def __init__(self, direction, diag, kappa, tail_mass, following, child, prev, last, extra, many):
        self.e, self.diag, self.kappa, self.tail_mass = direction, diag, kappa, tail_mass
        self.following, self.child, self.prev, self.last = following, child, prev, last
        self.extra, self.many = extra, many

    def total(self, value):
        return chain_sum(value, self.prev, self.extra) if self.many else value

    def apply(self, value):
        result = self.diag * value + self.kappa * gather_value(value, self.following)
        result = result + gather_value(self.total(self.kappa * value), self.child)
        if self.many:
            for d in range(3):
                force = self.e[d] * value
                others = gather_value(self.total(force), self.last) - force
                result = result - jnp.where(self.last >= 0, self.tail_mass * self.e[d] * others, 0.0)
        return result

    def at_head(self, force):
        return force - gather_value(self.total(force), self.child)

    def at_tail(self, force):
        below = gather_value(self.total(force), self.last) if self.many else force
        return gather_value(force, self.following) - below


def both_ways(extra, run):
    @pl.when(extra == 0)
    def _():
        run(False)

    @pl.when(extra > 0)
    def _():
        run(True)


F_NAMES = ["e0", "e1", "e2", "p0", "p1", "p2", "length", "scale", "head_mass", "tail_mass", "diag", "kappa",
           "base1", "g0", "g1", "g2", "g3"]
I_NAMES = ["following", "child", "prev", "last", "root", "slot", "cidx", "extra", "tinv0", "tinv1", "hinv0", "hinv1"]


def f_get(ref, name):
    i = F_NAMES.index(name)
    return ref[8 * i:8 * i + 8, :]


def i_get(ref, name):
    i = I_NAMES.index(name)
    return ref[8 * i:8 * i + 8, :]


def f_put(ref, name, value):
    i = F_NAMES.index(name)
    ref[8 * i:8 * i + 8, :] = value


def i_put(ref, name, value):
    i = I_NAMES.index(name)
    ref[8 * i:8 * i + 8, :] = value


def local_from(state_f, state_i, extra, many):
    return Local([f_get(state_f, f"e{d}") for d in range(3)], f_get(state_f, "diag"), f_get(state_f, "kappa"),
                 f_get(state_f, "tail_mass"), i_get(state_i, "following"), i_get(state_i, "child"),
                 i_get(state_i, "prev"), i_get(state_i, "last"), extra, many)


def compact_rows(values, cidx):
    high = cidx >> 7
    low = cidx & 127
    lane = iota((1, LANES), 1)
    firsts, rests = [], []
    for value in values:
        got = gather_rows(value_rows(value), high, low)
        firsts.append(got[0:1])
        rests.append(got[1:2])
    rows = list(firsts)
    for i in range(0, len(rests), 2):
        other = rests[i + 1] if i + 1 < len(rests) else rests[i]
        rows.append(jnp.where(lane < 64, rests[i], other))
    return rows


def geometry_kernel(size, old_ref, move_ref, mass_ref, head_ref, tail_ref, send_ref, got_ref,
                    state_f, state_i, out_ref, table, remote, rtab, cons):
    X, Y, Z = size["mesh"]
    send = size["send"]
    atom_rows, pad_rows = size["atom_rows"], size["atom_pad"]
    atoms = atom_rows * LANES
    shape = (8, LANES)
    here = iota(shape, 0) * LANES + iota(shape, 1)
    load_flat(head_ref, (0, 0, 0), cons, 0, 8)
    load_flat(tail_ref, (0, 0, 0), cons, 8, 8)
    head = cons[0:8, :]
    tail = cons[8:16, :]
    local = tail < atoms
    for d in range(3):
        load_flat(old_ref, (d, 0, 0, 0), table, d * pad_rows, atom_rows)
        load_flat(move_ref, (d, 0, 0, 0), table, (3 + d) * pad_rows, atom_rows)
    load_flat(mass_ref, (0, 0, 0), table, 6 * pad_rows, atom_rows)
    for d in range(3):
        for r in range(atom_rows):
            a, b = d * pad_rows + r, (3 + d) * pad_rows + r
            table[b:b + 1, :] = table[a:a + 1, :] + table[b:b + 1, :]

    ext_rows = size["ext_rows"]
    tinv, count = inverse_tables(tail, tail >= 0, ext_rows)
    hinv, _ = inverse_tables(head, head >= 0, pad_rows)
    most = jnp.max(jnp.where(iota(count.shape, 0) < atom_rows, count, 0.0))
    extra = jnp.maximum(most.astype(I32) - 1, 0)
    send_row = size["load_send"](send_ref)
    atom_id = iota((pad_rows, LANES), 0) * LANES + iota((pad_rows, LANES), 1)
    for e in range(send):
        which = jnp.broadcast_to(send_row[:, e:e + 1], (pad_rows, LANES))
        hinv = jnp.where(atom_id == which, 8 * LANES + e, hinv)
    cons[16:16 + ext_rows, :] = tinv
    i_put(state_i, "prev", jnp.full(shape, -1, I32))
    i_put(state_i, "last", jnp.where(local, here, -1))

    @pl.when(extra > 0)
    def _():
        def body(c, carry):
            prev, last, inv = carry
            mark = jnp.max(jnp.where(here == c, tail, -1))
            same = tail == mark
            prev = jnp.where(same & (here > c), c, prev)
            last = jnp.where(same & local, c, last)
            spots = iota(inv.shape, 0) * LANES + iota(inv.shape, 1)
            inv = jnp.where(spots == mark, c, inv)
            return prev, last, inv

        prev, last, inv = lax.fori_loop(
            0, 8 * LANES, body, (jnp.full(shape, -1, I32), jnp.full(shape, -1, I32), tinv))
        i_put(state_i, "prev", prev)
        i_put(state_i, "last", last)
        cons[16:16 + ext_rows, :] = inv

    tinv = cons[16:16 + ext_rows, :]
    tail_high, tail_low = tail >> 7, tail & 127
    head_high, head_low = head >> 7, head & 127
    hinv_rows = value_rows(hinv)[:atom_rows]
    following = gather_rows(hinv_rows, tail_high, tail_low)
    following = jnp.where(local, following, -1)
    following = jnp.where(following < 8 * LANES, following, -1)
    child = gather_rows(value_rows(tinv)[:atom_rows], head_high, head_low)
    root = jnp.where(local, -1, tail - atoms)
    slot = root
    for _ in range(3):
        ahead = gather_value(root + 1, following) - 1
        root = jnp.where(root < 0, ahead, root)
    slots = tinv[atom_rows:atom_rows + 4]
    used = slots >= 0
    used_f = jnp.where(used, 1.0, 0.0)
    before = lax.dot_general(
        jnp.concatenate([used_f, jnp.zeros((4, LANES), F32)], axis=0).astype(jnp.bfloat16),
        jnp.where(iota((LANES, LANES), 0) < iota((LANES, LANES), 1), 1.0, 0.0).astype(jnp.bfloat16),
        (((1,), (0,)), ((), ())), preferred_element_type=F32)
    rank_rows = []
    offset = jnp.zeros((1, 1), F32)
    for r in range(4):
        rank_rows.append(before[r:r + 1] + offset)
        offset = offset + jnp.sum(used_f[r:r + 1], axis=1, keepdims=True)
    rank = jnp.concatenate(rank_rows, axis=0)
    number = jnp.where(used, rank, -1.0)
    place = number.astype(I32)
    index4 = jnp.concatenate([place, jnp.where(place >= LANES, place + 64, -1)], axis=0)
    from8 = jnp.concatenate([slots, slots], axis=0)
    upper, lower = one_hot_scatter([(from8 >> 5).astype(F32), (from8 & 31).astype(F32)], index4, 8)
    cidx = (upper * 32.0 + lower).astype(I32)

    gx, gy, gz = my_place()
    for b, (dx, dy, dz) in enumerate(OFFSETS):
        at = (lax.rem(gx + (dx + X), X) * Y + lax.rem(gy + (dy + Y), Y)) * Z + lax.rem(gz + (dz + Z), Z)
        remote[b:b + 1, :] = got_ref[at, :, :]
    sub, lane = iota(shape, 0), iota(shape, 1)
    own = lane // send == sub
    for j in range(4):
        block = remote[8 * j:8 * j + 8, :]
        for q in range(7):
            got = jnp.where(own, pick(block, q * send + lane % send), 0.0)
            row = jnp.sum(got, axis=0, keepdims=True)
            rtab[4 * q + j:4 * q + j + 1, :] = row
    for d in range(3):
        rtab[4 * (3 + d):4 * (3 + d) + 4, :] = rtab[4 * d:4 * d + 4, :] + rtab[4 * (3 + d):4 * (3 + d) + 4, :]

    def rows_of(q):
        return [table[q * pad_rows + r:q * pad_rows + r + 1, :] for r in range(atom_rows)]

    def ext_rows_of(q):
        return rows_of(q) + [rtab[4 * q + j:4 * q + j + 1, :] for j in range(4)]

    head_at = [gather_rows(rows_of(q), head_high, head_low) for q in range(7)]
    tail_at = [gather_rows(ext_rows_of(q), tail_high, tail_low) for q in range(7)]
    bond = [head_at[d] - tail_at[d] for d in range(3)]
    gap = [head_at[3 + d] - tail_at[3 + d] for d in range(3)]
    length = jnp.maximum(jnp.sqrt(bond[0] * bond[0] + bond[1] * bond[1] + bond[2] * bond[2]), 0.5)
    direction = [bond[d] / length for d in range(3)]
    scale = 1.0 / jnp.sqrt(head_at[6] + tail_at[6])
    force = [scale * direction[d] for d in range(3)]
    head_mass = head_at[6]
    tail_mass = jnp.where(local, tail_at[6], 0.0)
    norm = force[0] * force[0] + force[1] * force[1] + force[2] * force[2]
    diag = 1.0 - norm * (head_mass + tail_mass)
    ahead = [gather_value(force[d], following) for d in range(3)]
    kappa = tail_mass * (force[0] * ahead[0] + force[1] * ahead[1] + force[2] * ahead[2])
    right = scale * ((direction[0] * gap[0] + direction[1] * gap[1] + direction[2] * gap[2]) - length)
    for d in range(3):
        f_put(state_f, f"e{d}", force[d])
        f_put(state_f, f"p{d}", gap[d])
    f_put(state_f, "length", length)
    f_put(state_f, "scale", scale)
    f_put(state_f, "head_mass", head_mass)
    f_put(state_f, "tail_mass", tail_mass)
    f_put(state_f, "diag", diag)
    f_put(state_f, "kappa", kappa)
    i_put(state_i, "following", following)
    i_put(state_i, "child", child)
    i_put(state_i, "root", root)
    i_put(state_i, "slot", slot)
    i_put(state_i, "cidx", cidx)
    i_put(state_i, "extra", jnp.broadcast_to(extra, shape))
    i_put(state_i, "tinv0", tinv[0:8])
    i_put(state_i, "tinv1", tinv[8:16])
    i_put(state_i, "hinv0", hinv[0:8])
    i_put(state_i, "hinv1", hinv[8:16])

    def run(many):
        operator = local_from(state_f, state_i, extra, many)
        terms = [right]
        unit = [jnp.where(local, 0.0, 1.0)]
        for k in range(ORDER):
            terms.append(operator.apply(terms[-1]))
            if k < ORDER - 1:
                unit.append(operator.apply(unit[-1]))
        base = terms[0]
        for term in terms[1:]:
            base = base + term
        f_put(state_f, "base1", base)
        summed = unit[0]
        f_put(state_f, "g0", summed)
        for k in range(1, ORDER):
            summed = summed + unit[k]
            f_put(state_f, f"g{k}", summed)
        rows = compact_rows(force + unit[1:] + terms, cidx)
        rows = rows + value_rows(number)
        for r, row in enumerate(rows):
            out_ref[0, r, :, :] = row

    both_ways(extra, run)
    for d in range(1, out_ref.shape[0]):
        for r in range(size["rows2"]):
            out_ref[d, r, :, :] = out_ref[0, r, :, :]


def lane_fields(tile):
    lane = iota((1, LANES), 1)
    return lane


def block_masks(tile, send, rows):
    per = LANES // send
    block = iota((rows, LANES), 1) // send + per * tile
    return block // 9 - 1, block // 3 % 3 - 1, block % 3 - 1, [b for b in range(per * tile, per * tile + per)]


def choose(options, field, values):
    result = options[values[0]]
    for v in values[1:]:
        result = jnp.where(field == v, options[v], result)
    return result


def expand_dense(size, load_row, number_rows, slots, dense):
    X, Y, Z = size["mesh"]
    R = Y * Z
    nq = len(slots)
    for x in range(X):
        for l in range(4):
            number = load_row(number_rows, x, l)
            high = number >> 7
            low = number & 127
            for i, q in enumerate(slots):
                first, rest, half = q
                a = pick(load_row("q", x, first), low)
                b = pick(load_row("q", x, rest), (low & 63) + 64 * half)
                value = jnp.where(number < 0, 0.0, jnp.where(high == 0, a, b))
                dense[x, i, :, l * LANES:(l + 1) * LANES] = value


def aligned(size, dense, q, target, tile):
    X, Y, Z = size["mesh"]
    send = size["send"]
    R = Y * Z
    dx, dy, dz, blocks = block_masks(tile, send, R)
    blocks = [b for b in blocks if b < 27]
    span = pl.ds(tile * LANES, LANES)
    offs = [sorted({OFFSETS[b][k] for b in blocks}) for k in range(3)]
    value = choose({o: dense[lax.rem(target + (X - o), X), q, :, span] for o in offs[0]}, dx, offs[0])
    row_z = iota((R, LANES), 0) % Z
    options = {0: value}
    if 1 in offs[2]:
        options[1] = jnp.where(row_z == 0, turn(value, Z - 1, R), turn(value, -1, R))
    if -1 in offs[2]:
        options[-1] = jnp.where(row_z == Z - 1, turn(value, -(Z - 1), R), turn(value, 1, R))
    value = choose(options, dz, offs[2])
    value = choose({o: turn(value, -o * Z, R) for o in offs[1]}, dy, offs[1])
    return value


def turn(value, by, rows):
    shift = (-by) % rows
    return value if shift == 0 else pltpu.roll(value, shift, 0)


def lane_total(parts, send):
    total = parts[0]
    for part in parts[1:]:
        total = total + part
    step = LANES // 2
    while step >= send:
        total = total + pltpu.roll(total, step, 1)
        step //= 2
    return total


def times(matrix, vector):
    full = {}
    for i, (a, b) in enumerate(SYM):
        full[a, b] = full[b, a] = matrix[i]
    return [full[a, 0] * vector[0] + full[a, 1] * vector[1] + full[a, 2] * vector[2] for a in range(3)]


def recurrence(first, matrices, mass):
    sums, scaled = [], []
    for k in range(ORDER + 1):
        value = first[k]
        for j in range(k):
            back = times(matrices[k - 1 - j], scaled[j])
            value = [value[d] - back[d] for d in range(3)]
        sums.append(value)
        scaled.append([mass * value[d] for d in range(3)])
    total = sums[0]
    for value in sums[1:]:
        total = [total[d] + value[d] for d in range(3)]
    return scaled, total, [mass * total[d] for d in range(3)]


def own_rows(size, place, tiles, tile):
    X, Y, Z = size["mesh"]
    R = Y * Z
    gx, gy, gz = place
    dx, dy, dz, blocks = block_masks(tile, size["send"], R)
    blocks = [b for b in blocks if b < 27]
    wanted = lax.rem(gy + dy + Y, Y) * Z + lax.rem(gz + dz + Z, Z)
    offs = sorted({OFFSETS[b][0] for b in blocks})
    value = choose({o: tiles[o + 1] for o in offs}, dx, offs)
    return jnp.sum(jnp.where(wanted == iota((R, LANES), 0), value, 0.0), axis=0, keepdims=True)


def strided(ref, first, rows, stride):
    if rows <= 8:
        return ref[pl.ds(first, rows, stride=stride), :]
    return jnp.concatenate(
        [ref[pl.ds(first + 8 * i * stride, 8, stride=stride), :] for i in range(rows // 8)], axis=0)


def middle_kernel(size, state_f, state_i, got1, got2, out_ref, pair_ref, force_ref, matrix_ref, keep_ref, dense):
    X, Y, Z = size["mesh"]
    send = size["send"]
    R = Y * Z
    rows2 = size["rows2"]
    place = my_place()
    gx, gy, gz = place

    def load_row(kind, x, r):
        row = strided(got2, x * R * rows2 + (size["map_row"] + r if kind == "map" else r), R, rows2)
        return row.astype(I32) if kind == "map" else row

    expand_dense(size, load_row, "map", [(q, NQ + q // 2, q % 2) for q in range(NQ)], dense)
    scaled_tiles, total_tiles, own_total = [], [], None
    for t in range(3):
        target = lax.rem(gx + (t - 1 + X), X)
        sums = {}
        for tile in range(4):
            q = [aligned(size, dense, i, target, tile) for i in range(NQ)]
            force, unit, terms = q[0:3], q[3:6], q[6:11]
            for d in range(3):
                force_ref[t, d, :, tile * LANES:(tile + 1) * LANES] = force[d]
                for k in range(ORDER + 1):
                    sums.setdefault(("v", k, d), []).append(force[d] * terms[k])
            for s, (a, b) in enumerate(SYM):
                square = force[a] * force[b]
                sums.setdefault(("b", 0, s), []).append(square)
                for k in range(3):
                    sums.setdefault(("b", k + 1, s), []).append(square * unit[k])
        sums = {key: lane_total(parts, send) for key, parts in sums.items()}
        mass = pick(strided(got1, target * R, R, 1), 6 * send + iota((R, LANES), 1) % send)
        matrices = [[sums["b", k, s] for s in range(6)] for k in range(ORDER)]
        for k in range(ORDER):
            for s in range(6):
                matrix_ref[t, 6 * k + s, :, :] = matrices[k][s]
        matrix_ref[t, 24, :, :] = mass
        scaled, total, full = recurrence(
            [[sums["v", k, d] for d in range(3)] for k in range(ORDER + 1)], matrices, mass)
        scaled_tiles.append(scaled)
        total_tiles.append(full)
        if t == 1:
            own_total = total
    me = gy * Z + gz
    keep_ref[...] = jnp.zeros(keep_ref.shape, F32)
    mine = iota((R, LANES), 0) == me
    for d in range(3):
        keep_ref[d:d + 1, :] = jnp.sum(jnp.where(mine, own_total[d], 0.0), axis=0, keepdims=True)
    corrections = [[] for _ in range(ORDER)]
    moves = [[] for _ in range(3)]
    for tile in range(4):
        force = []
        for d in range(3):
            value = dense[gx, d, :, tile * LANES:(tile + 1) * LANES]
            row = jnp.sum(jnp.where(mine, value, 0.0), axis=0, keepdims=True)
            keep_ref[8 + 4 * d + tile:9 + 4 * d + tile, :] = row
            force.append(row)
        for j in range(ORDER):
            rows = [own_rows(size, place, [scaled_tiles[t][j][d] for t in range(3)], tile) for d in range(3)]
            corrections[j].append(force[0] * rows[0] + force[1] * rows[1] + force[2] * rows[2])
        for d in range(3):
            moves[d].append(own_rows(size, place, [total_tiles[t][d] for t in range(3)], tile))
    root = i_get(state_i, "root")
    slot = i_get(state_i, "slot")
    solved = f_get(state_f, "base1")
    for j in range(ORDER):
        at = gather_rows(corrections[j], root >> 7, root & 127)
        solved = solved - f_get(state_f, f"g{ORDER - 1 - j}") * at
    moved = [gather_rows(moves[d], slot >> 7, slot & 127) for d in range(3)]
    extra = jnp.max(i_get(state_i, "extra"))
    cidx = i_get(state_i, "cidx")

    def run(many):
        operator = local_from(state_f, state_i, extra, many)
        local = slot < 0
        stretch = []
        for d in range(3):
            force = operator.e[d] * solved
            change = f_get(state_f, "head_mass") * operator.at_head(force)
            other = jnp.where(local, operator.tail_mass * operator.at_tail(force), -moved[d])
            stretch.append(f_get(state_f, f"p{d}") - (change - other))
        length = f_get(state_f, "length")
        current = stretch[0] * stretch[0] + stretch[1] * stretch[1] + stretch[2] * stretch[2]
        target = jnp.sqrt(jnp.maximum(2.0 * length * length - current, 0.5 * length * length))
        terms = [f_get(state_f, "scale") * (length - target)]
        for _ in range(ORDER):
            terms.append(operator.apply(terms[-1]))
        base = terms[0]
        for term in terms[1:]:
            base = base + term
        pair_ref[0:8, :] = solved
        pair_ref[8:16, :] = base
        rows = compact_rows(terms, cidx)
        for r, row in enumerate(rows):
            out_ref[0, r:r + 1, :] = row

    both_ways(extra, run)
    for d in range(1, out_ref.shape[0]):
        out_ref[d, :, :] = out_ref[0, :, :]


def final_kernel(size, old_ref, move_ref, mass_ref, state_f, state_i, got2, got3, pair_ref, force_ref, matrix_ref,
                 keep_ref, pos_ref, mult_ref, dense):
    X, Y, Z = size["mesh"]
    send = size["send"]
    R = Y * Z
    rows2 = size["rows2"]
    place = my_place()
    gx, gy, gz = place

    def load_row(kind, x, r):
        if kind == "map":
            return strided(got2, x * R * rows2 + size["map_row"] + r, R, rows2).astype(I32)
        return strided(got3, x * R * 8 + r, R, 8)

    nk = ORDER + 1
    expand_dense(size, load_row, "map", [(q, nk + q // 2, q % 2) for q in range(nk)], dense)
    scaled_tiles, own_total = [], None
    for t in range(3):
        target = lax.rem(gx + (t - 1 + X), X)
        sums = {}
        for tile in range(4):
            terms = [aligned(size, dense, i, target, tile) for i in range(nk)]
            for d in range(3):
                force = force_ref[t, d, :, tile * LANES:(tile + 1) * LANES]
                for k in range(nk):
                    sums.setdefault((k, d), []).append(force * terms[k])
        sums = {key: lane_total(parts, send) for key, parts in sums.items()}
        matrices = [[matrix_ref[t, 6 * k + s, :, :] for s in range(6)] for k in range(ORDER)]
        scaled, total, _ = recurrence(
            [[sums[k, d] for d in range(3)] for k in range(nk)], matrices, matrix_ref[t, 24, :, :])
        scaled_tiles.append(scaled)
        if t == 1:
            own_total = total
    mine = iota((R, LANES), 0) == gy * Z + gz
    corrections = [[] for _ in range(ORDER)]
    for tile in range(4):
        force = [keep_ref[8 + 4 * d + tile:9 + 4 * d + tile, :] for d in range(3)]
        for j in range(ORDER):
            rows = [own_rows(size, place, [scaled_tiles[t][j][d] for t in range(3)], tile) for d in range(3)]
            corrections[j].append(force[0] * rows[0] + force[1] * rows[1] + force[2] * rows[2])
    root = i_get(state_i, "root")
    solved = pair_ref[8:16, :]
    for j in range(ORDER):
        at = gather_rows(corrections[j], root >> 7, root & 127)
        solved = solved - f_get(state_f, f"g{ORDER - 1 - j}") * at
    both = pair_ref[0:8, :] + solved
    for r in range(8):
        mult_ref[0, 0, 0, pl.ds(r * LANES, LANES)] = both[r, :]
    extra = jnp.max(i_get(state_i, "extra"))

    def run(many):
        operator = local_from(state_f, state_i, extra, many)
        for d in range(3):
            force = operator.e[d] * both
            below = value_rows(operator.total(force))
            sent = keep_ref[d:d + 1, :] + jnp.sum(jnp.where(mine, own_total[d], 0.0), axis=0, keepdims=True)
            above = value_rows(force) + [-sent]
            for part, count in enumerate(size["atom_parts"]):
                hinv = i_get(state_i, f"hinv{part}")
                tinv = i_get(state_i, f"tinv{part}")
                change = gather_rows(above, hinv >> 7, hinv & 127) - gather_rows(below, tinv >> 7, tinv & 127)
                for r in range(count):
                    span = pl.ds((8 * part + r) * LANES, LANES)
                    start = old_ref[d, 0, 0, 0, span] + move_ref[d, 0, 0, 0, span]
                    pos_ref[d, 0, 0, 0, span] = start - mass_ref[0, 0, 0, span] * change[r, :]

    both_ways(extra, run)


def share(message):
    return lax.all_to_all(message, AXES, split_axis=0, concat_axis=0, tiled=True)


def make_per_device(mesh):
    sizes = axis_sizes(mesh)
    X, Y, Z = sizes
    devices = X * Y * Z
    R = Y * Z

    def per_device(old_pos, displacement, inv_mass, bond_head, bond_tail, send_list):
        atoms = old_pos.shape[-1]
        bonds = bond_head.shape[-1]
        send = send_list.shape[-1]
        atom_rows = atoms // LANES
        assert atoms % LANES == 0 and bonds == 8 * LANES and LANES % send == 0 and atom_rows <= 16
        rows2 = NQ + (NQ + 1) // 2 + 4

        def load_send(ref):
            one = ref[0, 0, 0:1, :]
            return jnp.concatenate([one] * (LANES // send), axis=1)

        size = dict(mesh=sizes, send=send, atom_rows=atom_rows, atom_pad=16, ext_rows=16, rows2=rows2,
                    map_row=NQ + (NQ + 1) // 2, load_send=load_send,
                    atom_parts=[min(8, atom_rows), max(atom_rows - 8, 0)])

        def call(kernel, outs, scratch, *args):
            def wrapped(*refs):
                kernel(size, *refs)

            return pl.pallas_call(
                wrapped, out_shape=outs, scratch_shapes=scratch,
                in_specs=[pl.BlockSpec(memory_space=pltpu.VMEM)] * len(args),
                out_specs=jax.tree.map(lambda _: pl.BlockSpec(memory_space=pltpu.VMEM), outs),
                compiler_params=pltpu.CompilerParams(vmem_limit_bytes=32 * 1024 * 1024),
            )(*args)

        S = jax.ShapeDtypeStruct
        one = call(send_kernel, S((devices, 1, LANES), F32), [pltpu.VMEM((7 * 16, LANES), F32)],
                   old_pos, displacement, inv_mass, send_list)
        got1 = share(one)
        state_f, state_i, two = call(
            geometry_kernel,
            (S((8 * len(F_NAMES), LANES), F32), S((8 * len(I_NAMES), LANES), I32), S((devices, rows2, 1, LANES), F32)),
            [pltpu.VMEM((7 * 16, LANES), F32), pltpu.VMEM((32, LANES), F32), pltpu.VMEM((32, LANES), F32),
             pltpu.VMEM((32, LANES), I32)],
            old_pos, displacement, inv_mass, bond_head, bond_tail, send_list, got1)
        got2 = share(two).reshape(devices * rows2, LANES)
        wide = 4 * LANES
        three, pair, force, matrix, keep = call(
            middle_kernel,
            (S((devices, 8, LANES), F32), S((16, LANES), F32), S((3, 3, R, wide), F32), S((3, 25, R, LANES), F32),
             S((24, LANES), F32)),
            [pltpu.VMEM((X, NQ, R, wide), F32)],
            state_f, state_i, got1.reshape(devices, LANES), got2)
        got3 = share(three).reshape(devices * 8, LANES)
        return call(
            final_kernel,
            (S(old_pos.shape, F32), S(bond_head.shape, F32)),
            [pltpu.VMEM((X, ORDER + 1, R, wide), F32)],
            old_pos, displacement, inv_mass, state_f, state_i, got2, got3, pair, force, matrix, keep)

    return per_device


def solution(mesh):
    return jax.shard_map(
        make_per_device(mesh),
        mesh=mesh,
        in_specs=(
            P(None, "gx", "gy", "gz", None),
            P(None, "gx", "gy", "gz", None),
            P("gx", "gy", "gz", None),
            P("gx", "gy", "gz", None),
            P("gx", "gy", "gz", None),
            P("gx", "gy", "gz", None),
        ),
        out_specs=(P(None, "gx", "gy", "gz", None), P("gx", "gy", "gz", None)),
        check_vma=False,
    )
```

```python
import math

import jax
import jax.numpy as jnp
from jax import lax
from jax.experimental import pallas as pl
from jax.experimental.pallas import tpu as pltpu
from jax.sharding import PartitionSpec as P

ORDER = 4
HALO = 192
LANES = 128
NQ = 11
AXES = ("gx", "gy", "gz")
OFFSETS = [(b // 9 - 1, b // 3 % 3 - 1, b % 3 - 1) for b in range(27)]
F32 = jnp.float32
I32 = jnp.int32
SYM = [(0, 0), (1, 1), (2, 2), (0, 1), (0, 2), (1, 2)]


def iota(shape, dim):
    return lax.broadcasted_iota(I32, shape, dim)


def pick(table, index):
    return jnp.take_along_axis(table, index, axis=1, mode="promise_in_bounds")


def spread_row(row, like):
    return jnp.broadcast_to(row, like.shape)


def gather_rows(rows, high, low, base=0):
    result = jnp.zeros(high.shape, rows[0].dtype)
    for r, row in enumerate(rows):
        result = jnp.where(high == base + r, pick(spread_row(row, high), low), result)
    return result


def value_rows(value):
    return [value[r:r + 1, :] for r in range(value.shape[0])]


def gather_value(value, index):
    return gather_rows(value_rows(value), index >> 7, index & 127)


def load_flat(ref, lead, scratch, base, count):
    for r in range(count):
        scratch[base + r:base + r + 1, :] = ref[(*lead, pl.ds(r * LANES, LANES))].reshape(1, LANES)


def axis_sizes(mesh):
    return tuple(mesh.shape[a] for a in AXES)


def my_place():
    return tuple(lax.axis_index(a) for a in AXES)


def one_hot_scatter(values, index, high_rows):
    parts = []
    spots = []
    for r in range(index.shape[0]):
        high = index[r:r + 1, :] >> 7
        low = index[r:r + 1, :] & 127
        hit = jnp.broadcast_to(high, (high_rows, LANES)) == iota((high_rows, LANES), 0)
        parts.append(jnp.concatenate(
            [jnp.where(hit, jnp.broadcast_to(v[r:r + 1, :], (high_rows, LANES)), 0.0) for v in values],
            axis=0).astype(jnp.bfloat16))
        spots.append(jnp.where(
            jnp.broadcast_to(low, (LANES, LANES)) == iota((LANES, LANES), 0), 1.0, 0.0).astype(jnp.bfloat16))
    left = jnp.concatenate(parts, axis=1)
    right = jnp.concatenate(spots, axis=1)
    table = lax.dot_general(left, right, (((1,), (1,)), ((), ())), preferred_element_type=F32)
    return [table[i * high_rows:(i + 1) * high_rows] for i in range(len(values))]


def inverse_tables(index, valid, high_rows):
    where_from = iota(index.shape, 0) * LANES + iota(index.shape, 1)
    spot = jnp.where(valid, index, -1)
    ones = jnp.ones(index.shape, F32)
    upper, lower, count = one_hot_scatter(
        [(where_from >> 5).astype(F32), (where_from & 31).astype(F32), ones], spot, high_rows)
    table = (upper * 32.0 + lower).astype(I32)
    return jnp.where(count > 0.5, table, -1), count


def send_kernel(size, old_hbm, move_hbm, mass_hbm, head_hbm, tail_hbm, send_hbm, out_ref, table, cons,
                old_ref, move_ref, mass_ref, head_ref, tail_ref, send_ref, sems):
    atom_rows = size["atom_rows"]
    send = size["send"]
    pad_rows = size["atom_pad"]
    copies = [pltpu.make_async_copy(src, dst, sems.at[i]) for i, (src, dst) in enumerate(
        [(old_hbm, old_ref), (move_hbm, move_ref), (mass_hbm, mass_ref), (send_hbm, send_ref), (head_hbm, head_ref),
         (tail_hbm, tail_ref)])]
    for copy in copies:
        copy.start()
    for copy in copies:
        copy.wait()
    table[...] = jnp.zeros(table.shape, F32)
    for r in range(atom_rows):
        span = pl.ds(r * LANES, LANES)
        for d in range(3):
            old = old_ref[d, 0, 0, 0, span].reshape(1, LANES)
            a, b = d * pad_rows + r, (3 + d) * pad_rows + r
            table[a:a + 1, :] = old
            table[b:b + 1, :] = old + move_ref[d, 0, 0, 0, span].reshape(1, LANES)
    load_flat(mass_ref, (0, 0, 0), table, 6 * pad_rows, atom_rows)
    load_flat(head_ref, (0, 0, 0), cons, 0, 8)
    load_flat(tail_ref, (0, 0, 0), cons, 8, 8)
    lane = iota((pad_rows, LANES), 1)
    send_row = size["load_send"](send_ref)
    cons[16:24, :] = jnp.broadcast_to(send_row, (8, LANES))
    index = jnp.broadcast_to(send_row, (pad_rows, LANES))
    low = index & 127
    hit = (index >> 7) == iota((pad_rows, LANES), 0)
    message = jnp.zeros((1, LANES), F32)
    for q in range(7):
        got = jnp.where(hit, pick(table[q * pad_rows:(q + 1) * pad_rows, :], low), 0.0)
        row = jnp.sum(got, axis=0, keepdims=True)
        message = jnp.where(lane[0:1] // send == q, row, message)
    for d in range(out_ref.shape[0]):
        out_ref[d, :, :] = message


def chain_sum(value, prev, extra):
    def body(_, carry):
        total, current = carry
        current = gather_value(current, prev)
        return total + current, current

    return lax.fori_loop(0, extra, body, (value, value))[0]


class Local:
    def __init__(self, direction, diag, kappa, tail_mass, following, child, prev, last, extra, many):
        self.e, self.diag, self.kappa, self.tail_mass = direction, diag, kappa, tail_mass
        self.following, self.child, self.prev, self.last = following, child, prev, last
        self.extra, self.many = extra, many

    def total(self, value):
        return chain_sum(value, self.prev, self.extra) if self.many else value

    def apply(self, value):
        result = self.diag * value + self.kappa * gather_value(value, self.following)
        result = result + gather_value(self.total(self.kappa * value), self.child)
        if self.many:
            for d in range(3):
                force = self.e[d] * value
                others = gather_value(self.total(force), self.last) - force
                result = result - jnp.where(self.last >= 0, self.tail_mass * self.e[d] * others, 0.0)
        return result

    def at_head(self, force):
        return force - gather_value(self.total(force), self.child)

    def at_tail(self, force):
        below = gather_value(self.total(force), self.last) if self.many else force
        return gather_value(force, self.following) - below


def both_ways(extra, run):
    @pl.when(extra == 0)
    def _():
        run(False)

    @pl.when(extra > 0)
    def _():
        run(True)


F_NAMES = ["e0", "e1", "e2", "p0", "p1", "p2", "length", "scale", "head_mass", "tail_mass", "diag", "kappa",
           "base1", "g0", "g1", "g2", "g3"]
I_NAMES = ["following", "child", "prev", "last", "root", "slot", "cidx", "extra", "tinv0", "tinv1", "hinv0", "hinv1"]


def f_get(ref, name):
    i = F_NAMES.index(name)
    return ref[8 * i:8 * i + 8, :]


def i_get(ref, name):
    i = I_NAMES.index(name)
    return ref[8 * i:8 * i + 8, :]


def f_put(ref, name, value):
    i = F_NAMES.index(name)
    ref[8 * i:8 * i + 8, :] = value


def i_put(ref, name, value):
    i = I_NAMES.index(name)
    ref[8 * i:8 * i + 8, :] = value


def local_from(state_f, state_i, extra, many):
    return Local([f_get(state_f, f"e{d}") for d in range(3)], f_get(state_f, "diag"), f_get(state_f, "kappa"),
                 f_get(state_f, "tail_mass"), i_get(state_i, "following"), i_get(state_i, "child"),
                 i_get(state_i, "prev"), i_get(state_i, "last"), extra, many)


def compact_rows(values, cidx):
    high = cidx >> 7
    low = cidx & 127
    lane = iota((1, LANES), 1)
    firsts, rests = [], []
    for value in values:
        got = gather_rows(value_rows(value), high, low)
        firsts.append(got[0:1])
        rests.append(got[1:2])
    rows = list(firsts)
    for i in range(0, len(rests), 2):
        other = rests[i + 1] if i + 1 < len(rests) else rests[i]
        rows.append(jnp.where(lane < 64, rests[i], other))
    return rows


def map_kernel(size, table, cons, state_i, number_ref, head_ref, tail_ref, work):
    atom_rows, pad_rows = size["atom_rows"], size["atom_pad"]
    send = size["send"]
    atoms = atom_rows * LANES
    shape = (8, LANES)
    here = iota(shape, 0) * LANES + iota(shape, 1)
    head = cons[0:8, :]
    tail = cons[8:16, :]
    local = tail < atoms

    ext_rows = size["ext_rows"]
    tinv, count = inverse_tables(tail, tail >= 0, ext_rows)
    hinv, _ = inverse_tables(head, head >= 0, pad_rows)
    most = jnp.max(jnp.where(iota(count.shape, 0) < atom_rows, count, 0.0))
    extra = jnp.maximum(most.astype(I32) - 1, 0)
    send_row = cons[16:17, :]
    atom_id = iota((pad_rows, LANES), 0) * LANES + iota((pad_rows, LANES), 1)
    for e in range(send):
        which = jnp.broadcast_to(send_row[:, e:e + 1], (pad_rows, LANES))
        hinv = jnp.where(atom_id == which, 8 * LANES + e, hinv)
    work[0:ext_rows, :] = tinv
    i_put(state_i, "prev", jnp.full(shape, -1, I32))
    i_put(state_i, "last", jnp.where(local, here, -1))

    @pl.when(extra > 0)
    def _():
        def body(c, carry):
            prev, last, inv = carry
            mark = jnp.max(jnp.where(here == c, tail, -1))
            same = tail == mark
            prev = jnp.where(same & (here > c), c, prev)
            last = jnp.where(same & local, c, last)
            spots = iota(inv.shape, 0) * LANES + iota(inv.shape, 1)
            inv = jnp.where(spots == mark, c, inv)
            return prev, last, inv

        prev, last, inv = lax.fori_loop(
            0, 8 * LANES, body, (jnp.full(shape, -1, I32), jnp.full(shape, -1, I32), tinv))
        i_put(state_i, "prev", prev)
        i_put(state_i, "last", last)
        work[0:ext_rows, :] = inv

    tinv = work[0:ext_rows, :]
    tail_high, tail_low = tail >> 7, tail & 127
    head_high, head_low = head >> 7, head & 127
    hinv_rows = value_rows(hinv)[:atom_rows]
    following = gather_rows(hinv_rows, tail_high, tail_low)
    following = jnp.where(local, following, -1)
    following = jnp.where(following < 8 * LANES, following, -1)
    child = gather_rows(value_rows(tinv)[:atom_rows], head_high, head_low)
    root = jnp.where(local, -1, tail - atoms)
    slot = root
    for _ in range(3):
        ahead = gather_value(root + 1, following) - 1
        root = jnp.where(root < 0, ahead, root)
    slots = tinv[atom_rows:atom_rows + 4]
    used = slots >= 0
    used_f = jnp.where(used, 1.0, 0.0)
    before = lax.dot_general(
        jnp.concatenate([used_f, jnp.zeros((4, LANES), F32)], axis=0).astype(jnp.bfloat16),
        jnp.where(iota((LANES, LANES), 0) < iota((LANES, LANES), 1), 1.0, 0.0).astype(jnp.bfloat16),
        (((1,), (0,)), ((), ())), preferred_element_type=F32)
    rank_rows = []
    offset = jnp.zeros((1, 1), F32)
    for r in range(4):
        rank_rows.append(before[r:r + 1] + offset)
        offset = offset + jnp.sum(used_f[r:r + 1], axis=1, keepdims=True)
    rank = jnp.concatenate(rank_rows, axis=0)
    number = jnp.where(used, rank, -1.0)
    place = number.astype(I32)
    index4 = jnp.concatenate([place, jnp.where(place >= LANES, place + 64, -1)], axis=0)
    from8 = jnp.concatenate([slots, slots], axis=0)
    upper, lower = one_hot_scatter([(from8 >> 5).astype(F32), (from8 & 31).astype(F32)], index4, 8)
    cidx = (upper * 32.0 + lower).astype(I32)

    number_ref[0:4, :] = number
    number_ref[4:8, :] = number
    i_put(state_i, "following", following)
    i_put(state_i, "child", child)
    i_put(state_i, "root", root)
    i_put(state_i, "slot", slot)
    i_put(state_i, "cidx", cidx)
    i_put(state_i, "extra", jnp.broadcast_to(extra, shape))
    i_put(state_i, "tinv0", tinv[0:8])
    i_put(state_i, "tinv1", tinv[8:16])
    i_put(state_i, "hinv0", hinv[0:8])
    i_put(state_i, "hinv1", hinv[8:16])

    def rows_of(q):
        return [table[q * pad_rows + r:q * pad_rows + r + 1, :] for r in range(atom_rows)]

    for q in range(7):
        head_ref[8 * q:8 * q + 8, :] = gather_rows(rows_of(q), head_high, head_low)
        tail_ref[8 * q:8 * q + 8, :] = gather_rows(rows_of(q), tail_high, tail_low)


def geometry_kernel(size, state_i, number_ref, head_ref, tail_ref, got_ref, state_f, out_ref, remote, rtab):
    X, Y, Z = size["mesh"]
    send = size["send"]
    shape = (8, LANES)
    slot = i_get(state_i, "slot")
    local = slot < 0
    following = i_get(state_i, "following")
    cidx = i_get(state_i, "cidx")
    extra = jnp.max(i_get(state_i, "extra"))
    gx, gy, gz = my_place()
    for b, (dx, dy, dz) in enumerate(OFFSETS):
        at = (lax.rem(gx + (dx + X), X) * Y + lax.rem(gy + (dy + Y), Y)) * Z + lax.rem(gz + (dz + Z), Z)
        remote[b:b + 1, :] = got_ref[at, :, :]
    sub, lane = iota(shape, 0), iota(shape, 1)
    own = lane // send == sub
    for j in range(4):
        block = remote[8 * j:8 * j + 8, :]
        for q in range(7):
            got = jnp.where(own, pick(block, q * send + lane % send), 0.0)
            row = jnp.sum(got, axis=0, keepdims=True)
            rtab[4 * q + j:4 * q + j + 1, :] = row
    slot_high, slot_low = slot >> 7, slot & 127
    head_at = [head_ref[8 * q:8 * q + 8, :] for q in range(7)]
    tail_at = []
    for q in range(7):
        afar = gather_rows([rtab[4 * q + j:4 * q + j + 1, :] for j in range(4)], slot_high, slot_low)
        tail_at.append(jnp.where(local, tail_ref[8 * q:8 * q + 8, :], afar))
    bond = [head_at[d] - tail_at[d] for d in range(3)]
    gap = [head_at[3 + d] - tail_at[3 + d] for d in range(3)]
    length = jnp.maximum(jnp.sqrt(bond[0] * bond[0] + bond[1] * bond[1] + bond[2] * bond[2]), 0.5)
    direction = [bond[d] / length for d in range(3)]
    scale = 1.0 / jnp.sqrt(head_at[6] + tail_at[6])
    force = [scale * direction[d] for d in range(3)]
    head_mass = head_at[6]
    tail_mass = jnp.where(local, tail_at[6], 0.0)
    norm = force[0] * force[0] + force[1] * force[1] + force[2] * force[2]
    diag = 1.0 - norm * (head_mass + tail_mass)
    ahead = [gather_value(force[d], following) for d in range(3)]
    kappa = tail_mass * (force[0] * ahead[0] + force[1] * ahead[1] + force[2] * ahead[2])
    right = scale * ((direction[0] * gap[0] + direction[1] * gap[1] + direction[2] * gap[2]) - length)
    for d in range(3):
        f_put(state_f, f"e{d}", force[d])
        f_put(state_f, f"p{d}", gap[d])
    f_put(state_f, "length", length)
    f_put(state_f, "scale", scale)
    f_put(state_f, "head_mass", head_mass)
    f_put(state_f, "tail_mass", tail_mass)
    f_put(state_f, "diag", diag)
    f_put(state_f, "kappa", kappa)
    def run(many):
        operator = local_from(state_f, state_i, extra, many)
        terms = [right]
        unit = [jnp.where(local, 0.0, 1.0)]
        for k in range(ORDER):
            terms.append(operator.apply(terms[-1]))
            if k < ORDER - 1:
                unit.append(operator.apply(unit[-1]))
        base = terms[0]
        for term in terms[1:]:
            base = base + term
        f_put(state_f, "base1", base)
        summed = unit[0]
        f_put(state_f, "g0", summed)
        for k in range(1, ORDER):
            summed = summed + unit[k]
            f_put(state_f, f"g{k}", summed)
        rows = compact_rows(force + unit[1:] + terms, cidx)
        rows = rows + value_rows(number_ref[0:4, :])
        for r, row in enumerate(rows):
            out_ref[0, r, :, :] = row

    both_ways(extra, run)
    for d in range(1, out_ref.shape[0]):
        for r in range(size["rows2"]):
            out_ref[d, r, :, :] = out_ref[0, r, :, :]


def lane_fields(tile):
    lane = iota((1, LANES), 1)
    return lane


def block_masks(tile, send, rows):
    per = LANES // send
    block = iota((rows, LANES), 1) // send + per * tile
    return block // 9 - 1, block // 3 % 3 - 1, block % 3 - 1, [b for b in range(per * tile, per * tile + per)]


def choose(options, field, values):
    result = options[values[0]]
    for v in values[1:]:
        result = jnp.where(field == v, options[v], result)
    return result


def expand_dense(size, load_row, number_rows, slots, dense):
    X, Y, Z = size["mesh"]
    R = Y * Z
    nq = len(slots)
    for x in range(X):
        for l in range(4):
            number = load_row(number_rows, x, l)
            high = number >> 7
            low = number & 127
            for i, q in enumerate(slots):
                first, rest, half = q
                a = pick(load_row("q", x, first), low)
                b = pick(load_row("q", x, rest), (low & 63) + 64 * half)
                value = jnp.where(number < 0, 0.0, jnp.where(high == 0, a, b))
                dense[x, i, :, l * LANES:(l + 1) * LANES] = value


def aligned(size, dense, q, target, tile):
    X, Y, Z = size["mesh"]
    send = size["send"]
    R = Y * Z
    dx, dy, dz, blocks = block_masks(tile, send, R)
    blocks = [b for b in blocks if b < 27]
    span = pl.ds(tile * LANES, LANES)
    offs = [sorted({OFFSETS[b][k] for b in blocks}) for k in range(3)]
    value = choose({o: dense[lax.rem(target + (X - o), X), q, :, span] for o in offs[0]}, dx, offs[0])
    row_z = iota((R, LANES), 0) % Z
    options = {0: value}
    if 1 in offs[2]:
        options[1] = jnp.where(row_z == 0, turn(value, Z - 1, R), turn(value, -1, R))
    if -1 in offs[2]:
        options[-1] = jnp.where(row_z == Z - 1, turn(value, -(Z - 1), R), turn(value, 1, R))
    value = choose(options, dz, offs[2])
    value = choose({o: turn(value, -o * Z, R) for o in offs[1]}, dy, offs[1])
    return value


def turn(value, by, rows):
    shift = (-by) % rows
    return value if shift == 0 else pltpu.roll(value, shift, 0)


def lane_totals(sums, send):
    stack = jnp.concatenate([parts[0] + parts[1] + parts[2] + parts[3] for parts in sums.values()], axis=0)
    pieces = []
    for _ in range(3):
        piece = stack.astype(jnp.bfloat16)
        pieces.append(piece)
        stack = stack - piece.astype(F32)
    same = iota((3 * LANES, LANES), 0) % send == iota((3 * LANES, LANES), 1) % send
    table = jnp.dot(jnp.concatenate(pieces, axis=1), jnp.where(same, 1.0, 0.0).astype(jnp.bfloat16),
                    preferred_element_type=F32)
    rows = table.shape[0] // len(sums)
    return {key: table[i * rows:(i + 1) * rows] for i, key in enumerate(sums)}


def times(matrix, vector):
    full = {}
    for i, (a, b) in enumerate(SYM):
        full[a, b] = full[b, a] = matrix[i]
    return [full[a, 0] * vector[0] + full[a, 1] * vector[1] + full[a, 2] * vector[2] for a in range(3)]


def recurrence(first, matrices, mass):
    sums, scaled = [], []
    for k in range(ORDER + 1):
        value = first[k]
        for j in range(k):
            back = times(matrices[k - 1 - j], scaled[j])
            value = [value[d] - back[d] for d in range(3)]
        sums.append(value)
        scaled.append([mass * value[d] for d in range(3)])
    total = sums[0]
    for value in sums[1:]:
        total = [total[d] + value[d] for d in range(3)]
    return scaled, total, [mass * total[d] for d in range(3)]


def own_rows(size, place, tiles, tile):
    X, Y, Z = size["mesh"]
    R = Y * Z
    gx, gy, gz = place
    dx, dy, dz, blocks = block_masks(tile, size["send"], R)
    blocks = [b for b in blocks if b < 27]
    wanted = lax.rem(gy + dy + Y, Y) * Z + lax.rem(gz + dz + Z, Z)
    offs = sorted({OFFSETS[b][0] for b in blocks})
    value = choose({o: tiles[o + 1] for o in offs}, dx, offs)
    return jnp.sum(jnp.where(wanted == iota((R, LANES), 0), value, 0.0), axis=0, keepdims=True)


def strided(ref, first, rows, stride):
    if rows <= 8:
        return ref[pl.ds(first, rows, stride=stride), :]
    return jnp.concatenate(
        [ref[pl.ds(first + 8 * i * stride, 8, stride=stride), :] for i in range(rows // 8)], axis=0)


def middle_kernel(size, state_f, state_i, got1, got2, out_ref, pair_ref, force_ref, matrix_ref, keep_ref, dense):
    X, Y, Z = size["mesh"]
    send = size["send"]
    R = Y * Z
    rows2 = size["rows2"]
    place = my_place()
    gx, gy, gz = place

    def load_row(kind, x, r):
        row = strided(got2, x * R * rows2 + (size["map_row"] + r if kind == "map" else r), R, rows2)
        return row.astype(I32) if kind == "map" else row

    expand_dense(size, load_row, "map", [(q, NQ + q // 2, q % 2) for q in range(NQ)], dense)
    scaled_tiles, total_tiles, own_total = [], [], None
    for t in range(3):
        target = lax.rem(gx + (t - 1 + X), X)
        sums = {}
        for tile in range(4):
            q = [aligned(size, dense, i, target, tile) for i in range(NQ)]
            force, unit, terms = q[0:3], q[3:6], q[6:11]
            for d in range(3):
                force_ref[t, d, :, tile * LANES:(tile + 1) * LANES] = force[d]
                for k in range(ORDER + 1):
                    sums.setdefault(("v", k, d), []).append(force[d] * terms[k])
            for s, (a, b) in enumerate(SYM):
                square = force[a] * force[b]
                sums.setdefault(("b", 0, s), []).append(square)
                for k in range(3):
                    sums.setdefault(("b", k + 1, s), []).append(square * unit[k])
        sums = lane_totals(sums, send)
        mass = pick(strided(got1, target * R, R, 1), 6 * send + iota((R, LANES), 1) % send)
        matrices = [[sums["b", k, s] for s in range(6)] for k in range(ORDER)]
        for k in range(ORDER):
            for s in range(6):
                matrix_ref[t, 6 * k + s, :, :] = matrices[k][s]
        matrix_ref[t, 24, :, :] = mass
        scaled, total, full = recurrence(
            [[sums["v", k, d] for d in range(3)] for k in range(ORDER + 1)], matrices, mass)
        scaled_tiles.append(scaled)
        total_tiles.append(full)
        if t == 1:
            own_total = total
    me = gy * Z + gz
    keep_ref[...] = jnp.zeros(keep_ref.shape, F32)
    mine = iota((R, LANES), 0) == me
    for d in range(3):
        keep_ref[d:d + 1, :] = jnp.sum(jnp.where(mine, own_total[d], 0.0), axis=0, keepdims=True)
    corrections = [[] for _ in range(ORDER)]
    moves = [[] for _ in range(3)]
    for tile in range(4):
        force = []
        for d in range(3):
            value = dense[gx, d, :, tile * LANES:(tile + 1) * LANES]
            row = jnp.sum(jnp.where(mine, value, 0.0), axis=0, keepdims=True)
            keep_ref[8 + 4 * d + tile:9 + 4 * d + tile, :] = row
            force.append(row)
        for j in range(ORDER):
            rows = [own_rows(size, place, [scaled_tiles[t][j][d] for t in range(3)], tile) for d in range(3)]
            corrections[j].append(force[0] * rows[0] + force[1] * rows[1] + force[2] * rows[2])
        for d in range(3):
            moves[d].append(own_rows(size, place, [total_tiles[t][d] for t in range(3)], tile))
    root = i_get(state_i, "root")
    slot = i_get(state_i, "slot")
    solved = f_get(state_f, "base1")
    for j in range(ORDER):
        at = gather_rows(corrections[j], root >> 7, root & 127)
        solved = solved - f_get(state_f, f"g{ORDER - 1 - j}") * at
    moved = [gather_rows(moves[d], slot >> 7, slot & 127) for d in range(3)]
    extra = jnp.max(i_get(state_i, "extra"))
    cidx = i_get(state_i, "cidx")

    def run(many):
        operator = local_from(state_f, state_i, extra, many)
        local = slot < 0
        stretch = []
        for d in range(3):
            force = operator.e[d] * solved
            change = f_get(state_f, "head_mass") * operator.at_head(force)
            other = jnp.where(local, operator.tail_mass * operator.at_tail(force), -moved[d])
            stretch.append(f_get(state_f, f"p{d}") - (change - other))
        length = f_get(state_f, "length")
        current = stretch[0] * stretch[0] + stretch[1] * stretch[1] + stretch[2] * stretch[2]
        target = jnp.sqrt(jnp.maximum(2.0 * length * length - current, 0.5 * length * length))
        terms = [f_get(state_f, "scale") * (length - target)]
        for _ in range(ORDER):
            terms.append(operator.apply(terms[-1]))
        base = terms[0]
        for term in terms[1:]:
            base = base + term
        pair_ref[0:8, :] = solved
        pair_ref[8:16, :] = base
        rows = compact_rows(terms, cidx)
        for r, row in enumerate(rows):
            out_ref[0, r:r + 1, :] = row

    both_ways(extra, run)
    for d in range(1, out_ref.shape[0]):
        out_ref[d, :, :] = out_ref[0, :, :]


def final_kernel(size, table, state_f, state_i, got2, got3, pair_ref, force_ref, matrix_ref,
                 keep_ref, pos_ref, mult_ref, dense):
    X, Y, Z = size["mesh"]
    send = size["send"]
    R = Y * Z
    rows2 = size["rows2"]
    place = my_place()
    gx, gy, gz = place

    def load_row(kind, x, r):
        if kind == "map":
            return strided(got2, x * R * rows2 + size["map_row"] + r, R, rows2).astype(I32)
        return strided(got3, x * R * 8 + r, R, 8)

    nk = ORDER + 1
    expand_dense(size, load_row, "map", [(q, nk + q // 2, q % 2) for q in range(nk)], dense)
    scaled_tiles, own_total = [], None
    for t in range(3):
        target = lax.rem(gx + (t - 1 + X), X)
        sums = {}
        for tile in range(4):
            terms = [aligned(size, dense, i, target, tile) for i in range(nk)]
            for d in range(3):
                force = force_ref[t, d, :, tile * LANES:(tile + 1) * LANES]
                for k in range(nk):
                    sums.setdefault((k, d), []).append(force * terms[k])
        sums = lane_totals(sums, send)
        matrices = [[matrix_ref[t, 6 * k + s, :, :] for s in range(6)] for k in range(ORDER)]
        scaled, total, _ = recurrence(
            [[sums[k, d] for d in range(3)] for k in range(nk)], matrices, matrix_ref[t, 24, :, :])
        scaled_tiles.append(scaled)
        if t == 1:
            own_total = total
    mine = iota((R, LANES), 0) == gy * Z + gz
    corrections = [[] for _ in range(ORDER)]
    for tile in range(4):
        force = [keep_ref[8 + 4 * d + tile:9 + 4 * d + tile, :] for d in range(3)]
        for j in range(ORDER):
            rows = [own_rows(size, place, [scaled_tiles[t][j][d] for t in range(3)], tile) for d in range(3)]
            corrections[j].append(force[0] * rows[0] + force[1] * rows[1] + force[2] * rows[2])
    root = i_get(state_i, "root")
    solved = pair_ref[8:16, :]
    for j in range(ORDER):
        at = gather_rows(corrections[j], root >> 7, root & 127)
        solved = solved - f_get(state_f, f"g{ORDER - 1 - j}") * at
    both = pair_ref[0:8, :] + solved
    for r in range(8):
        mult_ref[0, 0, 0, pl.ds(r * LANES, LANES)] = both[r, :]
    extra = jnp.max(i_get(state_i, "extra"))

    def run(many):
        operator = local_from(state_f, state_i, extra, many)
        for d in range(3):
            force = operator.e[d] * both
            below = value_rows(operator.total(force))
            sent = keep_ref[d:d + 1, :] + jnp.sum(jnp.where(mine, own_total[d], 0.0), axis=0, keepdims=True)
            above = value_rows(force) + [-sent]
            for part, count in enumerate(size["atom_parts"]):
                hinv = i_get(state_i, f"hinv{part}")
                tinv = i_get(state_i, f"tinv{part}")
                change = gather_rows(above, hinv >> 7, hinv & 127) - gather_rows(below, tinv >> 7, tinv & 127)
                for r in range(count):
                    span = pl.ds((8 * part + r) * LANES, LANES)
                    at = 8 * part + r
                    pos_ref[d, 0, 0, 0, span] = (table[(3 + d) * size["atom_pad"] + at, :]
                                                 - table[6 * size["atom_pad"] + at, :] * change[r, :])

    both_ways(extra, run)


def share(message):
    return lax.all_to_all(message, AXES, split_axis=0, concat_axis=0, tiled=True)


def make_per_device(mesh):
    sizes = axis_sizes(mesh)
    X, Y, Z = sizes
    devices = X * Y * Z
    R = Y * Z

    def per_device(old_pos, displacement, inv_mass, bond_head, bond_tail, send_list):
        atoms = old_pos.shape[-1]
        bonds = bond_head.shape[-1]
        send = send_list.shape[-1]
        atom_rows = atoms // LANES
        assert atoms % LANES == 0 and bonds == 8 * LANES and LANES % send == 0 and atom_rows <= 16
        rows2 = NQ + (NQ + 1) // 2 + 4

        def load_send(ref):
            one = ref[0, 0, 0:1, :]
            return jnp.concatenate([one] * (LANES // send), axis=1)

        size = dict(mesh=sizes, send=send, atom_rows=atom_rows, atom_pad=16, ext_rows=16, rows2=rows2,
                    map_row=NQ + (NQ + 1) // 2, load_send=load_send,
                    atom_parts=[min(8, atom_rows), max(atom_rows - 8, 0)])

        def call(kernel, outs, scratch, *args, space=pltpu.VMEM):
            def wrapped(*refs):
                kernel(size, *refs)

            return pl.pallas_call(
                wrapped, out_shape=outs, scratch_shapes=scratch,
                in_specs=[pl.BlockSpec(memory_space=space)] * len(args),
                out_specs=jax.tree.map(lambda _: pl.BlockSpec(memory_space=pltpu.VMEM), outs),
                compiler_params=pltpu.CompilerParams(vmem_limit_bytes=32 * 1024 * 1024),
            )(*[pltpu.with_memory_space_constraint(a, space) for a in args] if space == pltpu.HBM else args)

        S = jax.ShapeDtypeStruct
        one, table, cons = call(
            send_kernel, (S((devices, 1, LANES), F32), S((7 * 16, LANES), F32), S((24, LANES), I32)),
            [pltpu.VMEM(old_pos.shape, F32), pltpu.VMEM(old_pos.shape, F32), pltpu.VMEM(inv_mass.shape, F32),
             pltpu.VMEM(bond_head.shape, I32), pltpu.VMEM(bond_tail.shape, I32), pltpu.VMEM(send_list.shape, I32),
             pltpu.SemaphoreType.DMA((6,))],
            old_pos, displacement, inv_mass, bond_head, bond_tail, send_list, space=pltpu.HBM)
        got1 = share(one)
        state_i, number, head_at, tail_at = call(
            map_kernel,
            (S((8 * len(I_NAMES), LANES), I32), S((8, LANES), F32), S((56, LANES), F32), S((56, LANES), F32)),
            [pltpu.VMEM((16, LANES), I32)], table, cons)
        state_f, two = call(
            geometry_kernel,
            (S((8 * len(F_NAMES), LANES), F32), S((devices, rows2, 1, LANES), F32)),
            [pltpu.VMEM((32, LANES), F32), pltpu.VMEM((32, LANES), F32)],
            state_i, number, head_at, tail_at, got1)
        got2 = share(two).reshape(devices * rows2, LANES)
        wide = 4 * LANES
        three, pair, force, matrix, keep = call(
            middle_kernel,
            (S((devices, 8, LANES), F32), S((16, LANES), F32), S((3, 3, R, wide), F32), S((3, 25, R, LANES), F32),
             S((24, LANES), F32)),
            [pltpu.VMEM((X, NQ, R, wide), F32)],
            state_f, state_i, got1.reshape(devices, LANES), got2)
        got3 = share(three).reshape(devices * 8, LANES)
        return call(
            final_kernel,
            (S(old_pos.shape, F32), S(bond_head.shape, F32)),
            [pltpu.VMEM((X, ORDER + 1, R, wide), F32)],
            table, state_f, state_i, got2, got3, pair, force, matrix, keep)

    return per_device


def solution(mesh):
    return jax.shard_map(
        make_per_device(mesh),
        mesh=mesh,
        in_specs=(
            P(None, "gx", "gy", "gz", None),
            P(None, "gx", "gy", "gz", None),
            P("gx", "gy", "gz", None),
            P("gx", "gy", "gz", None),
            P("gx", "gy", "gz", None),
            P("gx", "gy", "gz", None),
        ),
        out_specs=(P(None, "gx", "gy", "gz", None), P("gx", "gy", "gz", None)),
        check_vma=False,
    )
```

```python
import math

import jax
import jax.numpy as jnp
from jax import lax
from jax.experimental import pallas as pl
from jax.experimental.pallas import tpu as pltpu
from jax.sharding import PartitionSpec as P

ORDER = 4
HALO = 192
LANES = 128
NQ = 11
AXES = ("gx", "gy", "gz")
OFFSETS = [(b // 9 - 1, b // 3 % 3 - 1, b % 3 - 1) for b in range(27)]
F32 = jnp.float32
I32 = jnp.int32
SYM = [(0, 0), (1, 1), (2, 2), (0, 1), (0, 2), (1, 2)]


def iota(shape, dim):
    return lax.broadcasted_iota(I32, shape, dim)


def pick(table, index):
    return jnp.take_along_axis(table, index, axis=1, mode="promise_in_bounds")


def spread_row(row, like):
    return jnp.broadcast_to(row, like.shape)


def gather_rows(rows, high, low, base=0):
    result = jnp.zeros(high.shape, rows[0].dtype)
    for r, row in enumerate(rows):
        result = jnp.where(high == base + r, pick(spread_row(row, high), low), result)
    return result


def value_rows(value):
    return [value[r:r + 1, :] for r in range(value.shape[0])]


def gather_value(value, index):
    return gather_rows(value_rows(value), index >> 7, index & 127)


def load_flat(ref, lead, scratch, base, count):
    for r in range(count):
        scratch[base + r:base + r + 1, :] = ref[(*lead, pl.ds(r * LANES, LANES))].reshape(1, LANES)


def axis_sizes(mesh):
    return tuple(mesh.shape[a] for a in AXES)


def my_place():
    return tuple(lax.axis_index(a) for a in AXES)


def one_hot_scatter(values, index, high_rows):
    parts = []
    spots = []
    for r in range(index.shape[0]):
        high = index[r:r + 1, :] >> 7
        low = index[r:r + 1, :] & 127
        hit = jnp.broadcast_to(high, (high_rows, LANES)) == iota((high_rows, LANES), 0)
        parts.append(jnp.concatenate(
            [jnp.where(hit, jnp.broadcast_to(v[r:r + 1, :], (high_rows, LANES)), 0.0) for v in values],
            axis=0).astype(jnp.bfloat16))
        spots.append(jnp.where(
            jnp.broadcast_to(low, (LANES, LANES)) == iota((LANES, LANES), 0), 1.0, 0.0).astype(jnp.bfloat16))
    left = jnp.concatenate(parts, axis=1)
    right = jnp.concatenate(spots, axis=1)
    table = lax.dot_general(left, right, (((1,), (1,)), ((), ())), preferred_element_type=F32)
    return [table[i * high_rows:(i + 1) * high_rows] for i in range(len(values))]


def inverse_tables(index, valid, high_rows):
    where_from = iota(index.shape, 0) * LANES + iota(index.shape, 1)
    spot = jnp.where(valid, index, -1)
    ones = jnp.ones(index.shape, F32)
    upper, lower, count = one_hot_scatter(
        [(where_from >> 5).astype(F32), (where_from & 31).astype(F32), ones], spot, high_rows)
    table = (upper * 32.0 + lower).astype(I32)
    return jnp.where(count > 0.5, table, -1), count


def send_kernel(size, old_hbm, move_hbm, mass_hbm, head_hbm, tail_hbm, send_hbm, out_ref, table, cons,
                old_ref, move_ref, mass_ref, head_ref, tail_ref, send_ref, sems):
    atom_rows = size["atom_rows"]
    send = size["send"]
    pad_rows = size["atom_pad"]
    copies = [pltpu.make_async_copy(src, dst, sems.at[i]) for i, (src, dst) in enumerate(
        [(old_hbm, old_ref), (move_hbm, move_ref), (mass_hbm, mass_ref), (send_hbm, send_ref), (head_hbm, head_ref),
         (tail_hbm, tail_ref)])]
    for copy in copies:
        copy.start()
    for copy in copies:
        copy.wait()
    table[...] = jnp.zeros(table.shape, F32)
    for r in range(atom_rows):
        span = pl.ds(r * LANES, LANES)
        for d in range(3):
            old = old_ref[d, 0, 0, 0, span].reshape(1, LANES)
            a, b = d * pad_rows + r, (3 + d) * pad_rows + r
            table[a:a + 1, :] = old
            table[b:b + 1, :] = old + move_ref[d, 0, 0, 0, span].reshape(1, LANES)
    load_flat(mass_ref, (0, 0, 0), table, 6 * pad_rows, atom_rows)
    load_flat(head_ref, (0, 0, 0), cons, 0, 8)
    load_flat(tail_ref, (0, 0, 0), cons, 8, 8)
    lane = iota((pad_rows, LANES), 1)
    send_row = size["load_send"](send_ref)
    cons[16:24, :] = jnp.broadcast_to(send_row, (8, LANES))
    index = jnp.broadcast_to(send_row, (pad_rows, LANES))
    low = index & 127
    hit = (index >> 7) == iota((pad_rows, LANES), 0)
    message = jnp.zeros((1, LANES), F32)
    for q in range(7):
        got = jnp.where(hit, pick(table[q * pad_rows:(q + 1) * pad_rows, :], low), 0.0)
        row = jnp.sum(got, axis=0, keepdims=True)
        message = jnp.where(lane[0:1] // send == q, row, message)
    for d in range(out_ref.shape[0]):
        out_ref[d, :, :] = message


def chain_sum(value, prev, extra):
    def body(_, carry):
        total, current = carry
        current = gather_value(current, prev)
        return total + current, current

    return lax.fori_loop(0, extra, body, (value, value))[0]


class Local:
    def __init__(self, direction, diag, kappa, tail_mass, following, child, prev, last, extra, many):
        self.e, self.diag, self.kappa, self.tail_mass = direction, diag, kappa, tail_mass
        self.following, self.child, self.prev, self.last = following, child, prev, last
        self.extra, self.many = extra, many

    def total(self, value):
        return chain_sum(value, self.prev, self.extra) if self.many else value

    def apply(self, value):
        result = self.diag * value + self.kappa * gather_value(value, self.following)
        result = result + gather_value(self.total(self.kappa * value), self.child)
        if self.many:
            for d in range(3):
                force = self.e[d] * value
                others = gather_value(self.total(force), self.last) - force
                result = result - jnp.where(self.last >= 0, self.tail_mass * self.e[d] * others, 0.0)
        return result

    def at_head(self, force):
        return force - gather_value(self.total(force), self.child)

    def at_tail(self, force):
        below = gather_value(self.total(force), self.last) if self.many else force
        return gather_value(force, self.following) - below


def both_ways(extra, run):
    @pl.when(extra == 0)
    def _():
        run(False)

    @pl.when(extra > 0)
    def _():
        run(True)


F_NAMES = ["e0", "e1", "e2", "p0", "p1", "p2", "length", "scale", "head_mass", "tail_mass", "diag", "kappa",
           "base1", "g0", "g1", "g2", "g3"]
I_NAMES = ["following", "child", "prev", "last", "root", "slot", "cidx", "extra", "tinv0", "tinv1", "hinv0", "hinv1"]


def f_get(ref, name):
    i = F_NAMES.index(name)
    return ref[8 * i:8 * i + 8, :]


def i_get(ref, name):
    i = I_NAMES.index(name)
    return ref[8 * i:8 * i + 8, :]


def f_put(ref, name, value):
    i = F_NAMES.index(name)
    ref[8 * i:8 * i + 8, :] = value


def i_put(ref, name, value):
    i = I_NAMES.index(name)
    ref[8 * i:8 * i + 8, :] = value


def local_from(state_f, state_i, extra, many):
    return Local([f_get(state_f, f"e{d}") for d in range(3)], f_get(state_f, "diag"), f_get(state_f, "kappa"),
                 f_get(state_f, "tail_mass"), i_get(state_i, "following"), i_get(state_i, "child"),
                 i_get(state_i, "prev"), i_get(state_i, "last"), extra, many)


def compact_rows(values, cidx):
    high = cidx >> 7
    low = cidx & 127
    lane = iota((1, LANES), 1)
    firsts, rests = [], []
    for value in values:
        got = gather_rows(value_rows(value), high, low)
        firsts.append(got[0:1])
        rests.append(got[1:2])
    rows = list(firsts)
    for i in range(0, len(rests), 2):
        other = rests[i + 1] if i + 1 < len(rests) else rests[i]
        rows.append(jnp.where(lane < 64, rests[i], other))
    return rows


def map_kernel(size, table, cons, state_i, number_ref, head_ref, tail_ref, work):
    atom_rows, pad_rows = size["atom_rows"], size["atom_pad"]
    send = size["send"]
    atoms = atom_rows * LANES
    shape = (8, LANES)
    here = iota(shape, 0) * LANES + iota(shape, 1)
    head = cons[0:8, :]
    tail = cons[8:16, :]
    local = tail < atoms

    ext_rows = size["ext_rows"]
    tinv, count = inverse_tables(tail, tail >= 0, ext_rows)
    hinv, _ = inverse_tables(head, head >= 0, pad_rows)
    most = jnp.max(jnp.where(iota(count.shape, 0) < atom_rows, count, 0.0))
    extra = jnp.maximum(most.astype(I32) - 1, 0)
    send_row = cons[16:17, :]
    atom_id = iota((pad_rows, LANES), 0) * LANES + iota((pad_rows, LANES), 1)
    for e in range(send):
        which = jnp.broadcast_to(send_row[:, e:e + 1], (pad_rows, LANES))
        hinv = jnp.where(atom_id == which, 8 * LANES + e, hinv)
    work[0:ext_rows, :] = tinv
    i_put(state_i, "prev", jnp.full(shape, -1, I32))
    i_put(state_i, "last", jnp.where(local, here, -1))

    @pl.when(extra > 0)
    def _():
        def body(c, carry):
            prev, last, inv = carry
            mark = jnp.max(jnp.where(here == c, tail, -1))
            same = tail == mark
            prev = jnp.where(same & (here > c), c, prev)
            last = jnp.where(same & local, c, last)
            spots = iota(inv.shape, 0) * LANES + iota(inv.shape, 1)
            inv = jnp.where(spots == mark, c, inv)
            return prev, last, inv

        prev, last, inv = lax.fori_loop(
            0, 8 * LANES, body, (jnp.full(shape, -1, I32), jnp.full(shape, -1, I32), tinv))
        i_put(state_i, "prev", prev)
        i_put(state_i, "last", last)
        work[0:ext_rows, :] = inv

    tinv = work[0:ext_rows, :]
    tail_high, tail_low = tail >> 7, tail & 127
    head_high, head_low = head >> 7, head & 127
    hinv_rows = value_rows(hinv)[:atom_rows]
    following = gather_rows(hinv_rows, tail_high, tail_low)
    following = jnp.where(local, following, -1)
    following = jnp.where(following < 8 * LANES, following, -1)
    child = gather_rows(value_rows(tinv)[:atom_rows], head_high, head_low)
    root = jnp.where(local, -1, tail - atoms)
    slot = root
    for _ in range(3):
        ahead = gather_value(root + 1, following) - 1
        root = jnp.where(root < 0, ahead, root)
    slots = tinv[atom_rows:atom_rows + 4]
    used = slots >= 0
    used_f = jnp.where(used, 1.0, 0.0)
    before = lax.dot_general(
        jnp.concatenate([used_f, jnp.zeros((4, LANES), F32)], axis=0).astype(jnp.bfloat16),
        jnp.where(iota((LANES, LANES), 0) < iota((LANES, LANES), 1), 1.0, 0.0).astype(jnp.bfloat16),
        (((1,), (0,)), ((), ())), preferred_element_type=F32)
    rank_rows = []
    offset = jnp.zeros((1, 1), F32)
    for r in range(4):
        rank_rows.append(before[r:r + 1] + offset)
        offset = offset + jnp.sum(used_f[r:r + 1], axis=1, keepdims=True)
    rank = jnp.concatenate(rank_rows, axis=0)
    number = jnp.where(used, rank, -1.0)
    place = number.astype(I32)
    index4 = jnp.concatenate([place, jnp.where(place >= LANES, place + 64, -1)], axis=0)
    from8 = jnp.concatenate([slots, slots], axis=0)
    upper, lower = one_hot_scatter([(from8 >> 5).astype(F32), (from8 & 31).astype(F32)], index4, 8)
    cidx = (upper * 32.0 + lower).astype(I32)

    number_ref[0:4, :] = number
    number_ref[4:8, :] = number
    i_put(state_i, "following", following)
    i_put(state_i, "child", child)
    i_put(state_i, "root", root)
    i_put(state_i, "slot", slot)
    i_put(state_i, "cidx", cidx)
    i_put(state_i, "extra", jnp.broadcast_to(extra, shape))
    i_put(state_i, "tinv0", tinv[0:8])
    i_put(state_i, "tinv1", tinv[8:16])
    i_put(state_i, "hinv0", hinv[0:8])
    i_put(state_i, "hinv1", hinv[8:16])

    def rows_of(q):
        return [table[q * pad_rows + r:q * pad_rows + r + 1, :] for r in range(atom_rows)]

    for q in range(7):
        head_ref[8 * q:8 * q + 8, :] = gather_rows(rows_of(q), head_high, head_low)
        tail_ref[8 * q:8 * q + 8, :] = gather_rows(rows_of(q), tail_high, tail_low)


def geometry_kernel(size, state_i, number_ref, head_ref, tail_ref, got_ref, state_f, out_ref, remote, rtab):
    X, Y, Z = size["mesh"]
    send = size["send"]
    shape = (8, LANES)
    slot = i_get(state_i, "slot")
    local = slot < 0
    following = i_get(state_i, "following")
    cidx = i_get(state_i, "cidx")
    extra = jnp.max(i_get(state_i, "extra"))
    gx, gy, gz = my_place()
    for b, (dx, dy, dz) in enumerate(OFFSETS):
        at = (lax.rem(gx + (dx + X), X) * Y + lax.rem(gy + (dy + Y), Y)) * Z + lax.rem(gz + (dz + Z), Z)
        remote[b:b + 1, :] = got_ref[at, :, :]
    sub, lane = iota(shape, 0), iota(shape, 1)
    own = lane // send == sub
    for j in range(4):
        block = remote[8 * j:8 * j + 8, :]
        for q in range(7):
            got = jnp.where(own, pick(block, q * send + lane % send), 0.0)
            row = jnp.sum(got, axis=0, keepdims=True)
            rtab[4 * q + j:4 * q + j + 1, :] = row
    slot_high, slot_low = slot >> 7, slot & 127
    head_at = [head_ref[8 * q:8 * q + 8, :] for q in range(7)]
    tail_at = []
    for q in range(7):
        afar = gather_rows([rtab[4 * q + j:4 * q + j + 1, :] for j in range(4)], slot_high, slot_low)
        tail_at.append(jnp.where(local, tail_ref[8 * q:8 * q + 8, :], afar))
    bond = [head_at[d] - tail_at[d] for d in range(3)]
    gap = [head_at[3 + d] - tail_at[3 + d] for d in range(3)]
    length = jnp.maximum(jnp.sqrt(bond[0] * bond[0] + bond[1] * bond[1] + bond[2] * bond[2]), 0.5)
    direction = [bond[d] / length for d in range(3)]
    scale = 1.0 / jnp.sqrt(head_at[6] + tail_at[6])
    force = [scale * direction[d] for d in range(3)]
    head_mass = head_at[6]
    tail_mass = jnp.where(local, tail_at[6], 0.0)
    norm = force[0] * force[0] + force[1] * force[1] + force[2] * force[2]
    diag = 1.0 - norm * (head_mass + tail_mass)
    ahead = [gather_value(force[d], following) for d in range(3)]
    kappa = tail_mass * (force[0] * ahead[0] + force[1] * ahead[1] + force[2] * ahead[2])
    right = scale * ((direction[0] * gap[0] + direction[1] * gap[1] + direction[2] * gap[2]) - length)
    for d in range(3):
        f_put(state_f, f"e{d}", force[d])
        f_put(state_f, f"p{d}", gap[d])
    f_put(state_f, "length", length)
    f_put(state_f, "scale", scale)
    f_put(state_f, "head_mass", head_mass)
    f_put(state_f, "tail_mass", tail_mass)
    f_put(state_f, "diag", diag)
    f_put(state_f, "kappa", kappa)
    def run(many):
        operator = local_from(state_f, state_i, extra, many)
        terms = [right]
        unit = [jnp.where(local, 0.0, 1.0)]
        for k in range(ORDER):
            terms.append(operator.apply(terms[-1]))
            if k < ORDER - 1:
                unit.append(operator.apply(unit[-1]))
        base = terms[0]
        for term in terms[1:]:
            base = base + term
        f_put(state_f, "base1", base)
        summed = unit[0]
        f_put(state_f, "g0", summed)
        for k in range(1, ORDER):
            summed = summed + unit[k]
            f_put(state_f, f"g{k}", summed)
        rows = compact_rows(force + unit[1:] + terms, cidx)
        rows = rows + value_rows(number_ref[0:4, :])
        for r, row in enumerate(rows):
            out_ref[0, r, :, :] = row

    both_ways(extra, run)
    for d in range(1, out_ref.shape[0]):
        for r in range(size["rows2"]):
            out_ref[d, r, :, :] = out_ref[0, r, :, :]


def lane_fields(tile):
    lane = iota((1, LANES), 1)
    return lane


def block_masks(tile, send, rows):
    per = LANES // send
    block = iota((rows, LANES), 1) // send + per * tile
    return block // 9 - 1, block // 3 % 3 - 1, block % 3 - 1, [b for b in range(per * tile, per * tile + per)]


def choose(options, field, values):
    result = options[values[0]]
    for v in values[1:]:
        result = jnp.where(field == v, options[v], result)
    return result


def expand_dense(size, load_row, number_rows, slots, dense):
    X, Y, Z = size["mesh"]
    R = Y * Z
    nq = len(slots)
    for x in range(X):
        for l in range(4):
            number = load_row(number_rows, x, l)
            high = number >> 7
            low = number & 127
            for i, q in enumerate(slots):
                first, rest, half = q
                a = pick(load_row("q", x, first), low)
                b = pick(load_row("q", x, rest), (low & 63) + 64 * half)
                value = jnp.where(number < 0, 0.0, jnp.where(high == 0, a, b))
                dense[x, i, :, l * LANES:(l + 1) * LANES] = value


def aligned(size, dense, q, target, tile):
    X, Y, Z = size["mesh"]
    send = size["send"]
    R = Y * Z
    dx, dy, dz, blocks = block_masks(tile, send, R)
    blocks = [b for b in blocks if b < 27]
    span = pl.ds(tile * LANES, LANES)
    offs = [sorted({OFFSETS[b][k] for b in blocks}) for k in range(3)]
    value = choose({o: dense[lax.rem(target + (X - o), X), q, :, span] for o in offs[0]}, dx, offs[0])
    row_z = iota((R, LANES), 0) % Z
    options = {0: value}
    if 1 in offs[2]:
        options[1] = jnp.where(row_z == 0, turn(value, Z - 1, R), turn(value, -1, R))
    if -1 in offs[2]:
        options[-1] = jnp.where(row_z == Z - 1, turn(value, -(Z - 1), R), turn(value, 1, R))
    value = choose(options, dz, offs[2])
    value = choose({o: turn(value, -o * Z, R) for o in offs[1]}, dy, offs[1])
    return value


def turn(value, by, rows):
    shift = (-by) % rows
    return value if shift == 0 else pltpu.roll(value, shift, 0)


def lane_totals(sums, send):
    stack = jnp.concatenate([parts[0] + parts[1] + parts[2] + parts[3] for parts in sums.values()], axis=0)
    pieces = []
    for _ in range(3):
        piece = stack.astype(jnp.bfloat16)
        pieces.append(piece)
        stack = stack - piece.astype(F32)
    same = iota((3 * LANES, LANES), 0) % send == iota((3 * LANES, LANES), 1) % send
    table = jnp.dot(jnp.concatenate(pieces, axis=1), jnp.where(same, 1.0, 0.0).astype(jnp.bfloat16),
                    preferred_element_type=F32)
    rows = table.shape[0] // len(sums)
    return {key: table[i * rows:(i + 1) * rows] for i, key in enumerate(sums)}


def times(matrix, vector):
    full = {}
    for i, (a, b) in enumerate(SYM):
        full[a, b] = full[b, a] = matrix[i]
    return [full[a, 0] * vector[0] + full[a, 1] * vector[1] + full[a, 2] * vector[2] for a in range(3)]


def recurrence(first, matrices, mass):
    sums, scaled = [], []
    for k in range(ORDER + 1):
        value = first[k]
        for j in range(k):
            back = times(matrices[k - 1 - j], scaled[j])
            value = [value[d] - back[d] for d in range(3)]
        sums.append(value)
        scaled.append([mass * value[d] for d in range(3)])
    total = sums[0]
    for value in sums[1:]:
        total = [total[d] + value[d] for d in range(3)]
    return scaled, total, [mass * total[d] for d in range(3)]


def own_rows(size, place, tiles, tile):
    X, Y, Z = size["mesh"]
    R = Y * Z
    gx, gy, gz = place
    dx, dy, dz, blocks = block_masks(tile, size["send"], R)
    blocks = [b for b in blocks if b < 27]
    wanted = lax.rem(dy + Y, Y) * Z + lax.rem(gz + dz + Z, Z)
    offs = sorted({OFFSETS[b][0] for b in blocks})
    value = choose({o: tiles[o + 1] for o in offs}, dx, offs)
    return jnp.sum(jnp.where(wanted == iota((R, LANES), 0), value, 0.0), axis=0, keepdims=True)


def strided(ref, first, rows, stride):
    if rows <= 8:
        return ref[pl.ds(first, rows, stride=stride), :]
    return jnp.concatenate(
        [ref[pl.ds(first + 8 * i * stride, 8, stride=stride), :] for i in range(rows // 8)], axis=0)


def plane(size, refs, x, row, stride):
    Y, Z = size["mesh"][1:]
    gy = lax.axis_index("gy")
    pieces = []
    for k in range(Y):
        if len(refs) > 1:
            pieces.append(strided(refs[k], x * Z * stride + row, Z, stride))
        else:
            pieces.append(strided(refs[0], (x * Y + lax.rem(gy + k, Y)) * Z * stride + row, Z, stride))
    return jnp.concatenate(pieces, axis=0)


def middle_kernel(size, state_f, state_i, got1, *refs):
    *got2, out_ref, pair_ref, force_ref, matrix_ref, keep_ref, dense = refs
    X, Y, Z = size["mesh"]
    send = size["send"]
    R = Y * Z
    rows2 = size["rows2"]
    place = my_place()
    gx, gy, gz = place

    def load_row(kind, x, r):
        row = plane(size, got2, x, size["map_row"] + r if kind == "map" else r, rows2)
        return row.astype(I32) if kind == "map" else row

    expand_dense(size, load_row, "map", [(q, NQ + q // 2, q % 2) for q in range(NQ)], dense)
    scaled_tiles, total_tiles, own_total = [], [], None
    for t in range(3):
        target = lax.rem(gx + (t - 1 + X), X)
        sums = {}
        for tile in range(4):
            q = [aligned(size, dense, i, target, tile) for i in range(NQ)]
            force, unit, terms = q[0:3], q[3:6], q[6:11]
            for d in range(3):
                force_ref[t, d, :, tile * LANES:(tile + 1) * LANES] = force[d]
                for k in range(ORDER + 1):
                    sums.setdefault(("v", k, d), []).append(force[d] * terms[k])
            for s, (a, b) in enumerate(SYM):
                square = force[a] * force[b]
                sums.setdefault(("b", 0, s), []).append(square)
                for k in range(3):
                    sums.setdefault(("b", k + 1, s), []).append(square * unit[k])
        sums = lane_totals(sums, send)
        mass = pick(plane(size, [got1], target, 0, 1), 6 * send + iota((R, LANES), 1) % send)
        matrices = [[sums["b", k, s] for s in range(6)] for k in range(ORDER)]
        for k in range(ORDER):
            for s in range(6):
                matrix_ref[t, 6 * k + s, :, :] = matrices[k][s]
        matrix_ref[t, 24, :, :] = mass
        scaled, total, full = recurrence(
            [[sums["v", k, d] for d in range(3)] for k in range(ORDER + 1)], matrices, mass)
        scaled_tiles.append(scaled)
        total_tiles.append(full)
        if t == 1:
            own_total = total
    keep_ref[...] = jnp.zeros(keep_ref.shape, F32)
    mine = iota((R, LANES), 0) == gz
    for d in range(3):
        keep_ref[d:d + 1, :] = jnp.sum(jnp.where(mine, own_total[d], 0.0), axis=0, keepdims=True)
    corrections = [[] for _ in range(ORDER)]
    moves = [[] for _ in range(3)]
    for tile in range(4):
        force = []
        for d in range(3):
            value = dense[gx, d, :, tile * LANES:(tile + 1) * LANES]
            row = jnp.sum(jnp.where(mine, value, 0.0), axis=0, keepdims=True)
            keep_ref[8 + 4 * d + tile:9 + 4 * d + tile, :] = row
            force.append(row)
        for j in range(ORDER):
            rows = [own_rows(size, place, [scaled_tiles[t][j][d] for t in range(3)], tile) for d in range(3)]
            corrections[j].append(force[0] * rows[0] + force[1] * rows[1] + force[2] * rows[2])
        for d in range(3):
            moves[d].append(own_rows(size, place, [total_tiles[t][d] for t in range(3)], tile))
    root = i_get(state_i, "root")
    slot = i_get(state_i, "slot")
    solved = f_get(state_f, "base1")
    for j in range(ORDER):
        at = gather_rows(corrections[j], root >> 7, root & 127)
        solved = solved - f_get(state_f, f"g{ORDER - 1 - j}") * at
    moved = [gather_rows(moves[d], slot >> 7, slot & 127) for d in range(3)]
    extra = jnp.max(i_get(state_i, "extra"))
    cidx = i_get(state_i, "cidx")

    def run(many):
        operator = local_from(state_f, state_i, extra, many)
        local = slot < 0
        stretch = []
        for d in range(3):
            force = operator.e[d] * solved
            change = f_get(state_f, "head_mass") * operator.at_head(force)
            other = jnp.where(local, operator.tail_mass * operator.at_tail(force), -moved[d])
            stretch.append(f_get(state_f, f"p{d}") - (change - other))
        length = f_get(state_f, "length")
        current = stretch[0] * stretch[0] + stretch[1] * stretch[1] + stretch[2] * stretch[2]
        target = jnp.sqrt(jnp.maximum(2.0 * length * length - current, 0.5 * length * length))
        terms = [f_get(state_f, "scale") * (length - target)]
        for _ in range(ORDER):
            terms.append(operator.apply(terms[-1]))
        base = terms[0]
        for term in terms[1:]:
            base = base + term
        pair_ref[0:8, :] = solved
        pair_ref[8:16, :] = base
        rows = compact_rows(terms, cidx)
        for r, row in enumerate(rows):
            out_ref[0, r:r + 1, :] = row

    both_ways(extra, run)
    for d in range(1, out_ref.shape[0]):
        out_ref[d, :, :] = out_ref[0, :, :]


def final_kernel(size, table, state_f, state_i, got3, pair_ref, force_ref, matrix_ref, keep_ref, *refs):
    *got2, pos_ref, mult_ref, dense = refs
    X, Y, Z = size["mesh"]
    send = size["send"]
    R = Y * Z
    rows2 = size["rows2"]
    place = my_place()
    gx, gy, gz = place

    def load_row(kind, x, r):
        if kind == "map":
            return plane(size, got2, x, size["map_row"] + r, rows2).astype(I32)
        return plane(size, [got3], x, r, 8)

    nk = ORDER + 1
    expand_dense(size, load_row, "map", [(q, nk + q // 2, q % 2) for q in range(nk)], dense)
    scaled_tiles, own_total = [], None
    for t in range(3):
        target = lax.rem(gx + (t - 1 + X), X)
        sums = {}
        for tile in range(4):
            terms = [aligned(size, dense, i, target, tile) for i in range(nk)]
            for d in range(3):
                force = force_ref[t, d, :, tile * LANES:(tile + 1) * LANES]
                for k in range(nk):
                    sums.setdefault((k, d), []).append(force * terms[k])
        sums = lane_totals(sums, send)
        matrices = [[matrix_ref[t, 6 * k + s, :, :] for s in range(6)] for k in range(ORDER)]
        scaled, total, _ = recurrence(
            [[sums[k, d] for d in range(3)] for k in range(nk)], matrices, matrix_ref[t, 24, :, :])
        scaled_tiles.append(scaled)
        if t == 1:
            own_total = total
    mine = iota((R, LANES), 0) == gz
    corrections = [[] for _ in range(ORDER)]
    for tile in range(4):
        force = [keep_ref[8 + 4 * d + tile:9 + 4 * d + tile, :] for d in range(3)]
        for j in range(ORDER):
            rows = [own_rows(size, place, [scaled_tiles[t][j][d] for t in range(3)], tile) for d in range(3)]
            corrections[j].append(force[0] * rows[0] + force[1] * rows[1] + force[2] * rows[2])
    root = i_get(state_i, "root")
    solved = pair_ref[8:16, :]
    for j in range(ORDER):
        at = gather_rows(corrections[j], root >> 7, root & 127)
        solved = solved - f_get(state_f, f"g{ORDER - 1 - j}") * at
    both = pair_ref[0:8, :] + solved
    for r in range(8):
        mult_ref[0, 0, 0, pl.ds(r * LANES, LANES)] = both[r, :]
    extra = jnp.max(i_get(state_i, "extra"))

    def run(many):
        operator = local_from(state_f, state_i, extra, many)
        for d in range(3):
            force = operator.e[d] * both
            below = value_rows(operator.total(force))
            sent = keep_ref[d:d + 1, :] + jnp.sum(jnp.where(mine, own_total[d], 0.0), axis=0, keepdims=True)
            above = value_rows(force) + [-sent]
            for part, count in enumerate(size["atom_parts"]):
                hinv = i_get(state_i, f"hinv{part}")
                tinv = i_get(state_i, f"tinv{part}")
                change = gather_rows(above, hinv >> 7, hinv & 127) - gather_rows(below, tinv >> 7, tinv & 127)
                for r in range(count):
                    span = pl.ds((8 * part + r) * LANES, LANES)
                    at = 8 * part + r
                    pos_ref[d, 0, 0, 0, span] = (table[(3 + d) * size["atom_pad"] + at, :]
                                                 - table[6 * size["atom_pad"] + at, :] * change[r, :])

    both_ways(extra, run)


def share(message, axes=AXES):
    return lax.all_to_all(message, axes, split_axis=0, concat_axis=0, tiled=True)


def make_per_device(mesh):
    sizes = axis_sizes(mesh)
    X, Y, Z = sizes
    devices = X * Y * Z
    R = Y * Z

    def per_device(old_pos, displacement, inv_mass, bond_head, bond_tail, send_list):
        atoms = old_pos.shape[-1]
        bonds = bond_head.shape[-1]
        send = send_list.shape[-1]
        atom_rows = atoms // LANES
        assert atoms % LANES == 0 and bonds == 8 * LANES and LANES % send == 0 and atom_rows <= 16
        rows2 = NQ + (NQ + 1) // 2 + 4

        def load_send(ref):
            one = ref[0, 0, 0:1, :]
            return jnp.concatenate([one] * (LANES // send), axis=1)

        size = dict(mesh=sizes, send=send, atom_rows=atom_rows, atom_pad=16, ext_rows=16, rows2=rows2,
                    map_row=NQ + (NQ + 1) // 2, load_send=load_send,
                    atom_parts=[min(8, atom_rows), max(atom_rows - 8, 0)])

        def call(kernel, outs, scratch, *args, space=pltpu.VMEM):
            def wrapped(*refs):
                kernel(size, *refs)

            return pl.pallas_call(
                wrapped, out_shape=outs, scratch_shapes=scratch,
                in_specs=[pl.BlockSpec(memory_space=space)] * len(args),
                out_specs=jax.tree.map(lambda _: pl.BlockSpec(memory_space=pltpu.VMEM), outs),
                compiler_params=pltpu.CompilerParams(vmem_limit_bytes=32 * 1024 * 1024),
            )(*[pltpu.with_memory_space_constraint(a, space) for a in args] if space == pltpu.HBM else args)

        S = jax.ShapeDtypeStruct
        one, table, cons = call(
            send_kernel, (S((devices, 1, LANES), F32), S((7 * 16, LANES), F32), S((24, LANES), I32)),
            [pltpu.VMEM(old_pos.shape, F32), pltpu.VMEM(old_pos.shape, F32), pltpu.VMEM(inv_mass.shape, F32),
             pltpu.VMEM(bond_head.shape, I32), pltpu.VMEM(bond_tail.shape, I32), pltpu.VMEM(send_list.shape, I32),
             pltpu.SemaphoreType.DMA((6,))],
            old_pos, displacement, inv_mass, bond_head, bond_tail, send_list, space=pltpu.HBM)
        got1 = share(one)
        state_i, number, head_at, tail_at = call(
            map_kernel,
            (S((8 * len(I_NAMES), LANES), I32), S((8, LANES), F32), S((56, LANES), F32), S((56, LANES), F32)),
            [pltpu.VMEM((16, LANES), I32)], table, cons)
        state_f, two = call(
            geometry_kernel,
            (S((8 * len(F_NAMES), LANES), F32), S((X * Z, rows2, 1, LANES), F32)),
            [pltpu.VMEM((32, LANES), F32), pltpu.VMEM((32, LANES), F32)],
            state_i, number, head_at, tail_at, got1)
        got2 = share(two, ("gx", "gz"))
        got2 = [got2] + [lax.ppermute(got2, "gy", [((i + k) % Y, i) for i in range(Y)]) for k in range(1, Y)]
        got2 = [g.reshape(X * Z * rows2, LANES) for g in got2]
        wide = 4 * LANES
        three, pair, force, matrix, keep = call(
            middle_kernel,
            (S((devices, 8, LANES), F32), S((16, LANES), F32), S((3, 3, R, wide), F32), S((3, 25, R, LANES), F32),
             S((24, LANES), F32)),
            [pltpu.VMEM((X, NQ, R, wide), F32)],
            state_f, state_i, got1.reshape(devices, LANES), *got2)
        got3 = share(three).reshape(devices * 8, LANES)
        return call(
            final_kernel,
            (S(old_pos.shape, F32), S(bond_head.shape, F32)),
            [pltpu.VMEM((X, ORDER + 1, R, wide), F32)],
            table, state_f, state_i, got3, pair, force, matrix, keep, *got2)

    return per_device


def solution(mesh):
    return jax.shard_map(
        make_per_device(mesh),
        mesh=mesh,
        in_specs=(
            P(None, "gx", "gy", "gz", None),
            P(None, "gx", "gy", "gz", None),
            P("gx", "gy", "gz", None),
            P("gx", "gy", "gz", None),
            P("gx", "gy", "gz", None),
            P("gx", "gy", "gz", None),
        ),
        out_specs=(P(None, "gx", "gy", "gz", None), P("gx", "gy", "gz", None)),
        check_vma=False,
    )
```

```python
import math

import jax
import jax.numpy as jnp
from jax import lax
from jax.experimental import pallas as pl
from jax.experimental.pallas import tpu as pltpu
from jax.sharding import PartitionSpec as P

ORDER = 4
HALO = 192
LANES = 128
NQ = 11
AXES = ("gx", "gy", "gz")
OFFSETS = [(b // 9 - 1, b // 3 % 3 - 1, b % 3 - 1) for b in range(27)]
F32 = jnp.float32
I32 = jnp.int32
SYM = [(0, 0), (1, 1), (2, 2), (0, 1), (0, 2), (1, 2)]


def iota(shape, dim):
    return lax.broadcasted_iota(I32, shape, dim)


def pick(table, index):
    return jnp.take_along_axis(table, index, axis=1, mode="promise_in_bounds")


def spread_row(row, like):
    return jnp.broadcast_to(row, like.shape)


def gather_rows(rows, high, low, base=0):
    result = jnp.zeros(high.shape, rows[0].dtype)
    for r, row in enumerate(rows):
        result = jnp.where(high == base + r, pick(spread_row(row, high), low), result)
    return result


def value_rows(value):
    return [value[r:r + 1, :] for r in range(value.shape[0])]


def gather_value(value, index):
    return gather_rows(value_rows(value), index >> 7, index & 127)


def load_flat(ref, lead, scratch, base, count):
    for r in range(count):
        scratch[base + r:base + r + 1, :] = ref[(*lead, pl.ds(r * LANES, LANES))].reshape(1, LANES)


def axis_sizes(mesh):
    return tuple(mesh.shape[a] for a in AXES)


def my_place():
    return tuple(lax.axis_index(a) for a in AXES)


def one_hot_scatter(values, index, high_rows):
    parts = []
    spots = []
    for r in range(index.shape[0]):
        high = index[r:r + 1, :] >> 7
        low = index[r:r + 1, :] & 127
        hit = jnp.broadcast_to(high, (high_rows, LANES)) == iota((high_rows, LANES), 0)
        parts.append(jnp.concatenate(
            [jnp.where(hit, jnp.broadcast_to(v[r:r + 1, :], (high_rows, LANES)), 0.0) for v in values],
            axis=0).astype(jnp.bfloat16))
        spots.append(jnp.where(
            jnp.broadcast_to(low, (LANES, LANES)) == iota((LANES, LANES), 0), 1.0, 0.0).astype(jnp.bfloat16))
    left = jnp.concatenate(parts, axis=1)
    right = jnp.concatenate(spots, axis=1)
    table = lax.dot_general(left, right, (((1,), (1,)), ((), ())), preferred_element_type=F32)
    return [table[i * high_rows:(i + 1) * high_rows] for i in range(len(values))]


def inverse_tables(index, valid, high_rows):
    where_from = iota(index.shape, 0) * LANES + iota(index.shape, 1)
    spot = jnp.where(valid, index, -1)
    ones = jnp.ones(index.shape, F32)
    upper, lower, count = one_hot_scatter(
        [(where_from >> 5).astype(F32), (where_from & 31).astype(F32), ones], spot, high_rows)
    table = (upper * 32.0 + lower).astype(I32)
    return jnp.where(count > 0.5, table, -1), count


def send_kernel(size, old_hbm, move_hbm, mass_hbm, head_hbm, tail_hbm, send_hbm, out_ref, table, cons,
                old_ref, move_ref, mass_ref, head_ref, tail_ref, send_ref, sems):
    atom_rows = size["atom_rows"]
    send = size["send"]
    pad_rows = size["atom_pad"]
    copies = [pltpu.make_async_copy(src, dst, sems.at[i]) for i, (src, dst) in enumerate(
        [(old_hbm, old_ref), (move_hbm, move_ref), (mass_hbm, mass_ref), (send_hbm, send_ref), (head_hbm, head_ref),
         (tail_hbm, tail_ref)])]
    for copy in copies:
        copy.start()
    for copy in copies:
        copy.wait()
    table[...] = jnp.zeros(table.shape, F32)
    for r in range(atom_rows):
        span = pl.ds(r * LANES, LANES)
        for d in range(3):
            old = old_ref[d, 0, 0, 0, span].reshape(1, LANES)
            a, b = d * pad_rows + r, (3 + d) * pad_rows + r
            table[a:a + 1, :] = old
            table[b:b + 1, :] = old + move_ref[d, 0, 0, 0, span].reshape(1, LANES)
    load_flat(mass_ref, (0, 0, 0), table, 6 * pad_rows, atom_rows)
    load_flat(head_ref, (0, 0, 0), cons, 0, 8)
    load_flat(tail_ref, (0, 0, 0), cons, 8, 8)
    lane = iota((pad_rows, LANES), 1)
    send_row = size["load_send"](send_ref)
    cons[16:24, :] = jnp.broadcast_to(send_row, (8, LANES))
    index = jnp.broadcast_to(send_row, (pad_rows, LANES))
    low = index & 127
    hit = (index >> 7) == iota((pad_rows, LANES), 0)
    message = jnp.zeros((1, LANES), F32)
    for q in range(7):
        got = jnp.where(hit, pick(table[q * pad_rows:(q + 1) * pad_rows, :], low), 0.0)
        row = jnp.sum(got, axis=0, keepdims=True)
        message = jnp.where(lane[0:1] // send == q, row, message)
    for d in range(out_ref.shape[0]):
        out_ref[d, :, :] = message


def chain_sum(value, prev, extra):
    def body(_, carry):
        total, current = carry
        current = gather_value(current, prev)
        return total + current, current

    return lax.fori_loop(0, extra, body, (value, value))[0]


class Local:
    def __init__(self, direction, diag, kappa, tail_mass, following, child, prev, last, extra, many):
        self.e, self.diag, self.kappa, self.tail_mass = direction, diag, kappa, tail_mass
        self.following, self.child, self.prev, self.last = following, child, prev, last
        self.extra, self.many = extra, many

    def total(self, value):
        return chain_sum(value, self.prev, self.extra) if self.many else value

    def apply(self, value):
        result = self.diag * value + self.kappa * gather_value(value, self.following)
        result = result + gather_value(self.total(self.kappa * value), self.child)
        if self.many:
            for d in range(3):
                force = self.e[d] * value
                others = gather_value(self.total(force), self.last) - force
                result = result - jnp.where(self.last >= 0, self.tail_mass * self.e[d] * others, 0.0)
        return result

    def at_head(self, force):
        return force - gather_value(self.total(force), self.child)

    def at_tail(self, force):
        below = gather_value(self.total(force), self.last) if self.many else force
        return gather_value(force, self.following) - below


def both_ways(extra, run):
    @pl.when(extra == 0)
    def _():
        run(False)

    @pl.when(extra > 0)
    def _():
        run(True)


F_NAMES = ["e0", "e1", "e2", "p0", "p1", "p2", "length", "scale", "head_mass", "tail_mass", "diag", "kappa",
           "base1", "g0", "g1", "g2", "g3"]
I_NAMES = ["following", "child", "prev", "last", "root", "slot", "cidx", "extra", "tinv0", "tinv1", "hinv0", "hinv1"]


def f_get(ref, name):
    i = F_NAMES.index(name)
    return ref[8 * i:8 * i + 8, :]


def i_get(ref, name):
    i = I_NAMES.index(name)
    return ref[8 * i:8 * i + 8, :]


def f_put(ref, name, value):
    i = F_NAMES.index(name)
    ref[8 * i:8 * i + 8, :] = value


def i_put(ref, name, value):
    i = I_NAMES.index(name)
    ref[8 * i:8 * i + 8, :] = value


def local_from(state_f, state_i, extra, many):
    return Local([f_get(state_f, f"e{d}") for d in range(3)], f_get(state_f, "diag"), f_get(state_f, "kappa"),
                 f_get(state_f, "tail_mass"), i_get(state_i, "following"), i_get(state_i, "child"),
                 i_get(state_i, "prev"), i_get(state_i, "last"), extra, many)


def compact_rows(values, cidx):
    high = cidx >> 7
    low = cidx & 127
    lane = iota((1, LANES), 1)
    firsts, rests = [], []
    for i, value in enumerate(values):
        got = gather_rows(value_rows(value), high, low)
        firsts.append(got[2:3] if i % 2 else got[0:1])
        rests.append(got[1:2])
    rows = list(firsts)
    for i in range(0, len(rests), 2):
        other = rests[i + 1] if i + 1 < len(rests) else rests[i]
        rows.append(jnp.where(lane < 64, rests[i], other))
    return rows


def map_kernel(size, table, cons, state_i, number_ref, head_ref, tail_ref, work):
    atom_rows, pad_rows = size["atom_rows"], size["atom_pad"]
    send = size["send"]
    atoms = atom_rows * LANES
    shape = (8, LANES)
    here = iota(shape, 0) * LANES + iota(shape, 1)
    head = cons[0:8, :]
    tail = cons[8:16, :]
    local = tail < atoms

    ext_rows = size["ext_rows"]
    tinv, count = inverse_tables(tail, tail >= 0, ext_rows)
    hinv, _ = inverse_tables(head, head >= 0, pad_rows)
    most = jnp.max(jnp.where(iota(count.shape, 0) < atom_rows, count, 0.0))
    extra = jnp.maximum(most.astype(I32) - 1, 0)
    send_row = cons[16:17, :]
    atom_id = iota((pad_rows, LANES), 0) * LANES + iota((pad_rows, LANES), 1)
    for e in range(send):
        which = jnp.broadcast_to(send_row[:, e:e + 1], (pad_rows, LANES))
        hinv = jnp.where(atom_id == which, 8 * LANES + e, hinv)
    work[0:ext_rows, :] = tinv
    i_put(state_i, "prev", jnp.full(shape, -1, I32))
    i_put(state_i, "last", jnp.where(local, here, -1))

    @pl.when(extra > 0)
    def _():
        def body(c, carry):
            prev, last, inv = carry
            mark = jnp.max(jnp.where(here == c, tail, -1))
            same = tail == mark
            prev = jnp.where(same & (here > c), c, prev)
            last = jnp.where(same & local, c, last)
            spots = iota(inv.shape, 0) * LANES + iota(inv.shape, 1)
            inv = jnp.where(spots == mark, c, inv)
            return prev, last, inv

        prev, last, inv = lax.fori_loop(
            0, 8 * LANES, body, (jnp.full(shape, -1, I32), jnp.full(shape, -1, I32), tinv))
        i_put(state_i, "prev", prev)
        i_put(state_i, "last", last)
        work[0:ext_rows, :] = inv

    tinv = work[0:ext_rows, :]
    tail_high, tail_low = tail >> 7, tail & 127
    head_high, head_low = head >> 7, head & 127
    hinv_rows = value_rows(hinv)[:atom_rows]
    following = gather_rows(hinv_rows, tail_high, tail_low)
    following = jnp.where(local, following, -1)
    following = jnp.where(following < 8 * LANES, following, -1)
    child = gather_rows(value_rows(tinv)[:atom_rows], head_high, head_low)
    root = jnp.where(local, -1, tail - atoms)
    slot = root
    for _ in range(3):
        ahead = gather_value(root + 1, following) - 1
        root = jnp.where(root < 0, ahead, root)
    slots = tinv[atom_rows:atom_rows + 4]
    used = slots >= 0
    used_f = jnp.where(used, 1.0, 0.0)
    before = lax.dot_general(
        jnp.concatenate([used_f, jnp.zeros((4, LANES), F32)], axis=0).astype(jnp.bfloat16),
        jnp.where(iota((LANES, LANES), 0) < iota((LANES, LANES), 1), 1.0, 0.0).astype(jnp.bfloat16),
        (((1,), (0,)), ((), ())), preferred_element_type=F32)
    rank_rows = []
    starts = []
    offset = jnp.zeros((1, 1), F32)
    for r in range(4):
        rank_rows.append(before[r:r + 1] + offset)
        starts.append(offset)
        offset = offset + jnp.sum(used_f[r:r + 1], axis=1, keepdims=True)
    rank = jnp.concatenate(rank_rows, axis=0)
    number = jnp.where(used, rank, -1.0)
    place = number.astype(I32)
    index4 = jnp.concatenate([place, jnp.where(place >= LANES, place + 64, -1)], axis=0)
    from8 = jnp.concatenate([slots, slots], axis=0)
    upper, lower = one_hot_scatter([(from8 >> 5).astype(F32), (from8 & 31).astype(F32)], index4, 8)
    cidx = (upper * 32.0 + lower).astype(I32)
    turned = pltpu.roll(cidx, LANES // 2, 1)
    cidx = jnp.where(iota(shape, 0) == 2, jnp.broadcast_to(turned[0:1, :], shape), cidx)

    marks = number[3:4, :]
    for r in range(4):
        marks = jnp.where(iota((1, LANES), 1) == size["start_lane"] + r, -2.0 - starts[r], marks)
    number = jnp.concatenate([number[0:3, :], marks], axis=0)
    number_ref[0:4, :] = number
    number_ref[4:8, :] = number
    i_put(state_i, "following", following)
    i_put(state_i, "child", child)
    i_put(state_i, "root", root)
    i_put(state_i, "slot", slot)
    i_put(state_i, "cidx", cidx)
    i_put(state_i, "extra", jnp.broadcast_to(extra, shape))
    i_put(state_i, "tinv0", tinv[0:8])
    i_put(state_i, "tinv1", tinv[8:16])
    i_put(state_i, "hinv0", hinv[0:8])
    i_put(state_i, "hinv1", hinv[8:16])

    def rows_of(q):
        return [table[q * pad_rows + r:q * pad_rows + r + 1, :] for r in range(atom_rows)]

    for q in range(7):
        head_ref[8 * q:8 * q + 8, :] = gather_rows(rows_of(q), head_high, head_low)
        tail_ref[8 * q:8 * q + 8, :] = gather_rows(rows_of(q), tail_high, tail_low)


def geometry_kernel(size, state_i, number_ref, head_ref, tail_ref, got_ref, state_f, out_ref, remote, rtab):
    X, Y, Z = size["mesh"]
    send = size["send"]
    shape = (8, LANES)
    slot = i_get(state_i, "slot")
    local = slot < 0
    following = i_get(state_i, "following")
    cidx = i_get(state_i, "cidx")
    extra = jnp.max(i_get(state_i, "extra"))
    gx, gy, gz = my_place()
    for b, (dx, dy, dz) in enumerate(OFFSETS):
        at = (lax.rem(gx + (dx + X), X) * Y + lax.rem(gy + (dy + Y), Y)) * Z + lax.rem(gz + (dz + Z), Z)
        remote[b:b + 1, :] = got_ref[at, :, :]
    sub, lane = iota(shape, 0), iota(shape, 1)
    own = lane // send == sub
    for j in range(4):
        block = remote[8 * j:8 * j + 8, :]
        for q in range(7):
            got = jnp.where(own, pick(block, q * send + lane % send), 0.0)
            row = jnp.sum(got, axis=0, keepdims=True)
            rtab[4 * q + j:4 * q + j + 1, :] = row
    slot_high, slot_low = slot >> 7, slot & 127
    head_at = [head_ref[8 * q:8 * q + 8, :] for q in range(7)]
    tail_at = []
    for q in range(7):
        afar = gather_rows([rtab[4 * q + j:4 * q + j + 1, :] for j in range(4)], slot_high, slot_low)
        tail_at.append(jnp.where(local, tail_ref[8 * q:8 * q + 8, :], afar))
    bond = [head_at[d] - tail_at[d] for d in range(3)]
    gap = [head_at[3 + d] - tail_at[3 + d] for d in range(3)]
    length = jnp.maximum(jnp.sqrt(bond[0] * bond[0] + bond[1] * bond[1] + bond[2] * bond[2]), 0.5)
    direction = [bond[d] / length for d in range(3)]
    scale = 1.0 / jnp.sqrt(head_at[6] + tail_at[6])
    force = [scale * direction[d] for d in range(3)]
    head_mass = head_at[6]
    tail_mass = jnp.where(local, tail_at[6], 0.0)
    norm = force[0] * force[0] + force[1] * force[1] + force[2] * force[2]
    diag = 1.0 - norm * (head_mass + tail_mass)
    ahead = [gather_value(force[d], following) for d in range(3)]
    kappa = tail_mass * (force[0] * ahead[0] + force[1] * ahead[1] + force[2] * ahead[2])
    right = scale * ((direction[0] * gap[0] + direction[1] * gap[1] + direction[2] * gap[2]) - length)
    for d in range(3):
        f_put(state_f, f"e{d}", force[d])
        f_put(state_f, f"p{d}", gap[d])
    f_put(state_f, "length", length)
    f_put(state_f, "scale", scale)
    f_put(state_f, "head_mass", head_mass)
    f_put(state_f, "tail_mass", tail_mass)
    f_put(state_f, "diag", diag)
    f_put(state_f, "kappa", kappa)
    def run(many):
        operator = local_from(state_f, state_i, extra, many)
        terms = [right]
        unit = [jnp.where(local, 0.0, 1.0)]
        for k in range(ORDER):
            terms.append(operator.apply(terms[-1]))
            if k < ORDER - 1:
                unit.append(operator.apply(unit[-1]))
        base = terms[0]
        for term in terms[1:]:
            base = base + term
        f_put(state_f, "base1", base)
        summed = unit[0]
        f_put(state_f, "g0", summed)
        for k in range(1, ORDER):
            summed = summed + unit[k]
            f_put(state_f, f"g{k}", summed)
        rows = compact_rows(force + unit[1:] + terms, cidx)
        rows = rows + value_rows(number_ref[0:4, :])
        for r, row in enumerate(rows):
            out_ref[0, r, :, :] = row

    both_ways(extra, run)
    for d in range(1, out_ref.shape[0]):
        for r in range(size["rows2"]):
            out_ref[d, r, :, :] = out_ref[0, r, :, :]


def lane_fields(tile):
    lane = iota((1, LANES), 1)
    return lane


def block_masks(tile, send, rows):
    per = LANES // send
    block = iota((rows, LANES), 1) // send + per * tile
    return block // 9 - 1, block // 3 % 3 - 1, block % 3 - 1, [b for b in range(per * tile, per * tile + per)]


def choose(options, field, values):
    result = options[values[0]]
    for v in values[1:]:
        result = jnp.where(field == v, options[v], result)
    return result


def expand_dense(size, load_row, slots, dense):
    X, Y, Z = size["mesh"]
    R = Y * Z
    lane = iota((R, LANES), 1)
    for x in range(X):
        last = load_row("map", x, 3)
        rows = {r: load_row("q", x, r) for r in sorted({r for slot in slots for r in slot[:2]})}
        for l in range(4):
            number = load_row("map", x, l) if l < 3 else last
            start = -2 - pick(last, jnp.full((R, LANES), size["start_lane"] + l, I32))
            low = number & 127
            keep = [lane >= start, (lane < LANES // 2) | (lane - LANES // 2 >= start)]
            for i, (first, rest, half) in enumerate(slots):
                row = jnp.where(keep[half], rows[first], rows[rest])
                value = pick(row, low ^ (half * (LANES // 2)))
                dense[x, i, :, l * LANES:(l + 1) * LANES] = jnp.where(number < 0, 0.0, value)


def aligned(size, dense, q, target, tile):
    X, Y, Z = size["mesh"]
    send = size["send"]
    R = Y * Z
    dx, dy, dz, blocks = block_masks(tile, send, R)
    blocks = [b for b in blocks if b < 27]
    span = pl.ds(tile * LANES, LANES)
    offs = [sorted({OFFSETS[b][k] for b in blocks}) for k in range(3)]
    value = choose({o: dense[lax.rem(target + (X - o), X), q, :, span] for o in offs[0]}, dx, offs[0])
    row_z = iota((R, LANES), 0) % Z
    options = {0: value}
    if 1 in offs[2]:
        options[1] = jnp.where(row_z == 0, turn(value, Z - 1, R), turn(value, -1, R))
    if -1 in offs[2]:
        options[-1] = jnp.where(row_z == Z - 1, turn(value, -(Z - 1), R), turn(value, 1, R))
    value = choose(options, dz, offs[2])
    value = choose({o: turn(value, -o * Z, R) for o in offs[1]}, dy, offs[1])
    return value


def turn(value, by, rows):
    shift = (-by) % rows
    return value if shift == 0 else pltpu.roll(value, shift, 0)


def lane_totals(sums, send):
    stack = jnp.concatenate([parts[0] + parts[1] + parts[2] + parts[3] for parts in sums.values()], axis=0)
    pieces = []
    for _ in range(3):
        piece = stack.astype(jnp.bfloat16)
        pieces.append(piece)
        stack = stack - piece.astype(F32)
    same = iota((3 * LANES, LANES), 0) % send == iota((3 * LANES, LANES), 1) % send
    table = jnp.dot(jnp.concatenate(pieces, axis=1), jnp.where(same, 1.0, 0.0).astype(jnp.bfloat16),
                    preferred_element_type=F32)
    rows = table.shape[0] // len(sums)
    return {key: table[i * rows:(i + 1) * rows] for i, key in enumerate(sums)}


def times(matrix, vector):
    full = {}
    for i, (a, b) in enumerate(SYM):
        full[a, b] = full[b, a] = matrix[i]
    return [full[a, 0] * vector[0] + full[a, 1] * vector[1] + full[a, 2] * vector[2] for a in range(3)]


def recurrence(first, matrices, mass):
    sums, scaled = [], []
    for k in range(ORDER + 1):
        value = first[k]
        for j in range(k):
            back = times(matrices[k - 1 - j], scaled[j])
            value = [value[d] - back[d] for d in range(3)]
        sums.append(value)
        scaled.append([mass * value[d] for d in range(3)])
    total = sums[0]
    for value in sums[1:]:
        total = [total[d] + value[d] for d in range(3)]
    return scaled, total, [mass * total[d] for d in range(3)]


def own_rows(size, place, tiles, tile):
    X, Y, Z = size["mesh"]
    R = Y * Z
    gx, gy, gz = place
    dx, dy, dz, blocks = block_masks(tile, size["send"], R)
    blocks = [b for b in blocks if b < 27]
    wanted = lax.rem(dy + Y, Y) * Z + lax.rem(gz + dz + Z, Z)
    offs = sorted({OFFSETS[b][0] for b in blocks})
    value = choose({o: tiles[o + 1] for o in offs}, dx, offs)
    return jnp.sum(jnp.where(wanted == iota((R, LANES), 0), value, 0.0), axis=0, keepdims=True)


def strided(ref, first, rows, stride):
    if rows <= 8:
        return ref[pl.ds(first, rows, stride=stride), :]
    return jnp.concatenate(
        [ref[pl.ds(first + 8 * i * stride, 8, stride=stride), :] for i in range(rows // 8)], axis=0)


def plane(size, refs, x, row, stride):
    Y, Z = size["mesh"][1:]
    gy = lax.axis_index("gy")
    pieces = []
    for k in range(Y):
        if len(refs) > 1:
            pieces.append(strided(refs[k], x * Z * stride + row, Z, stride))
        else:
            pieces.append(strided(refs[0], (x * Y + lax.rem(gy + k, Y)) * Z * stride + row, Z, stride))
    return jnp.concatenate(pieces, axis=0)


def middle_kernel(size, state_f, state_i, got1, *refs):
    *got2, out_ref, pair_ref, force_ref, matrix_ref, keep_ref, dense = refs
    X, Y, Z = size["mesh"]
    send = size["send"]
    R = Y * Z
    rows2 = size["rows2"]
    place = my_place()
    gx, gy, gz = place

    def load_row(kind, x, r):
        row = plane(size, got2, x, size["map_row"] + r if kind == "map" else r, rows2)
        return row.astype(I32) if kind == "map" else row

    expand_dense(size, load_row, [(q, NQ + q // 2, q % 2) for q in range(NQ)], dense)
    scaled_tiles, total_tiles, own_total = [], [], None
    for t in range(3):
        target = lax.rem(gx + (t - 1 + X), X)
        sums = {}
        for tile in range(4):
            q = [aligned(size, dense, i, target, tile) for i in range(NQ)]
            force, unit, terms = q[0:3], q[3:6], q[6:11]
            for d in range(3):
                force_ref[t, d, :, tile * LANES:(tile + 1) * LANES] = force[d]
                for k in range(ORDER + 1):
                    sums.setdefault(("v", k, d), []).append(force[d] * terms[k])
            for s, (a, b) in enumerate(SYM):
                square = force[a] * force[b]
                sums.setdefault(("b", 0, s), []).append(square)
                for k in range(3):
                    sums.setdefault(("b", k + 1, s), []).append(square * unit[k])
        sums = lane_totals(sums, send)
        mass = pick(plane(size, [got1], target, 0, 1), 6 * send + iota((R, LANES), 1) % send)
        matrices = [[sums["b", k, s] for s in range(6)] for k in range(ORDER)]
        for k in range(ORDER):
            for s in range(6):
                matrix_ref[t, 6 * k + s, :, :] = matrices[k][s]
        matrix_ref[t, 24, :, :] = mass
        scaled, total, full = recurrence(
            [[sums["v", k, d] for d in range(3)] for k in range(ORDER + 1)], matrices, mass)
        scaled_tiles.append(scaled)
        total_tiles.append(full)
        if t == 1:
            own_total = total
    keep_ref[...] = jnp.zeros(keep_ref.shape, F32)
    mine = iota((R, LANES), 0) == gz
    for d in range(3):
        keep_ref[d:d + 1, :] = jnp.sum(jnp.where(mine, own_total[d], 0.0), axis=0, keepdims=True)
    corrections = [[] for _ in range(ORDER)]
    moves = [[] for _ in range(3)]
    for tile in range(4):
        force = []
        for d in range(3):
            value = dense[gx, d, :, tile * LANES:(tile + 1) * LANES]
            row = jnp.sum(jnp.where(mine, value, 0.0), axis=0, keepdims=True)
            keep_ref[8 + 4 * d + tile:9 + 4 * d + tile, :] = row
            force.append(row)
        for j in range(ORDER):
            rows = [own_rows(size, place, [scaled_tiles[t][j][d] for t in range(3)], tile) for d in range(3)]
            corrections[j].append(force[0] * rows[0] + force[1] * rows[1] + force[2] * rows[2])
        for d in range(3):
            moves[d].append(own_rows(size, place, [total_tiles[t][d] for t in range(3)], tile))
    root = i_get(state_i, "root")
    slot = i_get(state_i, "slot")
    solved = f_get(state_f, "base1")
    for j in range(ORDER):
        at = gather_rows(corrections[j], root >> 7, root & 127)
        solved = solved - f_get(state_f, f"g{ORDER - 1 - j}") * at
    moved = [gather_rows(moves[d], slot >> 7, slot & 127) for d in range(3)]
    extra = jnp.max(i_get(state_i, "extra"))
    cidx = i_get(state_i, "cidx")

    def run(many):
        operator = local_from(state_f, state_i, extra, many)
        local = slot < 0
        stretch = []
        for d in range(3):
            force = operator.e[d] * solved
            change = f_get(state_f, "head_mass") * operator.at_head(force)
            other = jnp.where(local, operator.tail_mass * operator.at_tail(force), -moved[d])
            stretch.append(f_get(state_f, f"p{d}") - (change - other))
        length = f_get(state_f, "length")
        current = stretch[0] * stretch[0] + stretch[1] * stretch[1] + stretch[2] * stretch[2]
        target = jnp.sqrt(jnp.maximum(2.0 * length * length - current, 0.5 * length * length))
        terms = [f_get(state_f, "scale") * (length - target)]
        for _ in range(ORDER):
            terms.append(operator.apply(terms[-1]))
        base = terms[0]
        for term in terms[1:]:
            base = base + term
        pair_ref[0:8, :] = solved
        pair_ref[8:16, :] = base
        rows = compact_rows(terms, cidx)
        for r, row in enumerate(rows):
            out_ref[0, r:r + 1, :] = row

    both_ways(extra, run)
    for d in range(1, out_ref.shape[0]):
        out_ref[d, :, :] = out_ref[0, :, :]


def final_kernel(size, table, state_f, state_i, got3, pair_ref, force_ref, matrix_ref, keep_ref, *refs):
    *got2, pos_ref, mult_ref, dense = refs
    X, Y, Z = size["mesh"]
    send = size["send"]
    R = Y * Z
    rows2 = size["rows2"]
    place = my_place()
    gx, gy, gz = place

    def load_row(kind, x, r):
        if kind == "map":
            return plane(size, got2, x, size["map_row"] + r, rows2).astype(I32)
        return plane(size, [got3], x, r, 8)

    nk = ORDER + 1
    expand_dense(size, load_row, [(q, nk + q // 2, q % 2) for q in range(nk)], dense)
    scaled_tiles, own_total = [], None
    for t in range(3):
        target = lax.rem(gx + (t - 1 + X), X)
        sums = {}
        for tile in range(4):
            terms = [aligned(size, dense, i, target, tile) for i in range(nk)]
            for d in range(3):
                force = force_ref[t, d, :, tile * LANES:(tile + 1) * LANES]
                for k in range(nk):
                    sums.setdefault((k, d), []).append(force * terms[k])
        sums = lane_totals(sums, send)
        matrices = [[matrix_ref[t, 6 * k + s, :, :] for s in range(6)] for k in range(ORDER)]
        scaled, total, _ = recurrence(
            [[sums[k, d] for d in range(3)] for k in range(nk)], matrices, matrix_ref[t, 24, :, :])
        scaled_tiles.append(scaled)
        if t == 1:
            own_total = total
    mine = iota((R, LANES), 0) == gz
    corrections = [[] for _ in range(ORDER)]
    for tile in range(4):
        force = [keep_ref[8 + 4 * d + tile:9 + 4 * d + tile, :] for d in range(3)]
        for j in range(ORDER):
            rows = [own_rows(size, place, [scaled_tiles[t][j][d] for t in range(3)], tile) for d in range(3)]
            corrections[j].append(force[0] * rows[0] + force[1] * rows[1] + force[2] * rows[2])
    root = i_get(state_i, "root")
    solved = pair_ref[8:16, :]
    for j in range(ORDER):
        at = gather_rows(corrections[j], root >> 7, root & 127)
        solved = solved - f_get(state_f, f"g{ORDER - 1 - j}") * at
    both = pair_ref[0:8, :] + solved
    for r in range(8):
        mult_ref[0, 0, 0, pl.ds(r * LANES, LANES)] = both[r, :]
    extra = jnp.max(i_get(state_i, "extra"))

    def run(many):
        operator = local_from(state_f, state_i, extra, many)
        for d in range(3):
            force = operator.e[d] * both
            below = value_rows(operator.total(force))
            sent = keep_ref[d:d + 1, :] + jnp.sum(jnp.where(mine, own_total[d], 0.0), axis=0, keepdims=True)
            above = value_rows(force) + [-sent]
            for part, count in enumerate(size["atom_parts"]):
                hinv = i_get(state_i, f"hinv{part}")
                tinv = i_get(state_i, f"tinv{part}")
                change = gather_rows(above, hinv >> 7, hinv & 127) - gather_rows(below, tinv >> 7, tinv & 127)
                for r in range(count):
                    span = pl.ds((8 * part + r) * LANES, LANES)
                    at = 8 * part + r
                    pos_ref[d, 0, 0, 0, span] = (table[(3 + d) * size["atom_pad"] + at, :]
                                                 - table[6 * size["atom_pad"] + at, :] * change[r, :])

    both_ways(extra, run)


def share(message, axes=AXES):
    return lax.all_to_all(message, axes, split_axis=0, concat_axis=0, tiled=True)


def make_per_device(mesh):
    sizes = axis_sizes(mesh)
    X, Y, Z = sizes
    devices = X * Y * Z
    R = Y * Z

    def per_device(old_pos, displacement, inv_mass, bond_head, bond_tail, send_list):
        atoms = old_pos.shape[-1]
        bonds = bond_head.shape[-1]
        send = send_list.shape[-1]
        atom_rows = atoms // LANES
        assert atoms % LANES == 0 and bonds == 8 * LANES and LANES % send == 0 and atom_rows <= 16 and 3 * LANES < 27 * send <= 4 * LANES - 4
        rows2 = NQ + (NQ + 1) // 2 + 4

        def load_send(ref):
            one = ref[0, 0, 0:1, :]
            return jnp.concatenate([one] * (LANES // send), axis=1)

        size = dict(mesh=sizes, send=send, atom_rows=atom_rows, atom_pad=16, ext_rows=16, rows2=rows2,
                    map_row=NQ + (NQ + 1) // 2, load_send=load_send, start_lane=27 * send - 3 * LANES,
                    atom_parts=[min(8, atom_rows), max(atom_rows - 8, 0)])

        def call(kernel, outs, scratch, *args, space=pltpu.VMEM):
            def wrapped(*refs):
                kernel(size, *refs)

            return pl.pallas_call(
                wrapped, out_shape=outs, scratch_shapes=scratch,
                in_specs=[pl.BlockSpec(memory_space=space)] * len(args),
                out_specs=jax.tree.map(lambda _: pl.BlockSpec(memory_space=pltpu.VMEM), outs),
                compiler_params=pltpu.CompilerParams(vmem_limit_bytes=32 * 1024 * 1024),
            )(*[pltpu.with_memory_space_constraint(a, space) for a in args] if space == pltpu.HBM else args)

        S = jax.ShapeDtypeStruct
        one, table, cons = call(
            send_kernel, (S((devices, 1, LANES), F32), S((7 * 16, LANES), F32), S((24, LANES), I32)),
            [pltpu.VMEM(old_pos.shape, F32), pltpu.VMEM(old_pos.shape, F32), pltpu.VMEM(inv_mass.shape, F32),
             pltpu.VMEM(bond_head.shape, I32), pltpu.VMEM(bond_tail.shape, I32), pltpu.VMEM(send_list.shape, I32),
             pltpu.SemaphoreType.DMA((6,))],
            old_pos, displacement, inv_mass, bond_head, bond_tail, send_list, space=pltpu.HBM)
        got1 = share(one)
        state_i, number, head_at, tail_at = call(
            map_kernel,
            (S((8 * len(I_NAMES), LANES), I32), S((8, LANES), F32), S((56, LANES), F32), S((56, LANES), F32)),
            [pltpu.VMEM((16, LANES), I32)], table, cons)
        state_f, two = call(
            geometry_kernel,
            (S((8 * len(F_NAMES), LANES), F32), S((X * Z, rows2, 1, LANES), F32)),
            [pltpu.VMEM((32, LANES), F32), pltpu.VMEM((32, LANES), F32)],
            state_i, number, head_at, tail_at, got1)
        got2 = share(two, ("gx", "gz"))
        got2 = [got2] + [lax.ppermute(got2, "gy", [((i + k) % Y, i) for i in range(Y)]) for k in range(1, Y)]
        got2 = [g.reshape(X * Z * rows2, LANES) for g in got2]
        wide = 4 * LANES
        three, pair, force, matrix, keep = call(
            middle_kernel,
            (S((devices, 8, LANES), F32), S((16, LANES), F32), S((3, 3, R, wide), F32), S((3, 25, R, LANES), F32),
             S((24, LANES), F32)),
            [pltpu.VMEM((X, NQ, R, wide), F32)],
            state_f, state_i, got1.reshape(devices, LANES), *got2)
        got3 = share(three).reshape(devices * 8, LANES)
        return call(
            final_kernel,
            (S(old_pos.shape, F32), S(bond_head.shape, F32)),
            [pltpu.VMEM((X, ORDER + 1, R, wide), F32)],
            table, state_f, state_i, got3, pair, force, matrix, keep, *got2)

    return per_device


def solution(mesh):
    return jax.shard_map(
        make_per_device(mesh),
        mesh=mesh,
        in_specs=(
            P(None, "gx", "gy", "gz", None),
            P(None, "gx", "gy", "gz", None),
            P("gx", "gy", "gz", None),
            P("gx", "gy", "gz", None),
            P("gx", "gy", "gz", None),
            P("gx", "gy", "gz", None),
        ),
        out_specs=(P(None, "gx", "gy", "gz", None), P("gx", "gy", "gz", None)),
        check_vma=False,
    )
```

```python
import math

import jax
import jax.numpy as jnp
from jax import lax
from jax.experimental import pallas as pl
from jax.experimental.pallas import tpu as pltpu
from jax.sharding import PartitionSpec as P

ORDER = 4
HALO = 192
LANES = 128
NQ = 11
AXES = ("gx", "gy", "gz")
OFFSETS = [(b // 9 - 1, b // 3 % 3 - 1, b % 3 - 1) for b in range(27)]
F32 = jnp.float32
I32 = jnp.int32
SYM = [(0, 0), (1, 1), (2, 2), (0, 1), (0, 2), (1, 2)]


def iota(shape, dim):
    return lax.broadcasted_iota(I32, shape, dim)


def pick(table, index):
    return jnp.take_along_axis(table, index, axis=1, mode="promise_in_bounds")


def pick_row(table, index):
    return jnp.take_along_axis(table, index, axis=0, mode="promise_in_bounds")


def spread_row(row, like):
    return jnp.broadcast_to(row, like.shape)


def gather_rows(rows, high, low, base=0):
    result = jnp.zeros(high.shape, rows[0].dtype)
    for r, row in enumerate(rows):
        result = jnp.where(high == base + r, pick(spread_row(row, high), low), result)
    return result


def value_rows(value):
    return [value[r:r + 1, :] for r in range(value.shape[0])]


def gather_value(value, index):
    return gather_rows(value_rows(value), index >> 7, index & 127)


def load_flat(ref, lead, scratch, base, count):
    for r in range(count):
        scratch[base + r:base + r + 1, :] = ref[(*lead, pl.ds(r * LANES, LANES))].reshape(1, LANES)


def axis_sizes(mesh):
    return tuple(mesh.shape[a] for a in AXES)


def my_place():
    return tuple(lax.axis_index(a) for a in AXES)


def one_hot_scatter(values, index, high_rows):
    parts = []
    spots = []
    for r in range(index.shape[0]):
        high = index[r:r + 1, :] >> 7
        low = index[r:r + 1, :] & 127
        hit = jnp.broadcast_to(high, (high_rows, LANES)) == iota((high_rows, LANES), 0)
        parts.append(jnp.concatenate(
            [jnp.where(hit, jnp.broadcast_to(v[r:r + 1, :], (high_rows, LANES)), 0.0) for v in values],
            axis=0).astype(jnp.bfloat16))
        spots.append(jnp.where(
            jnp.broadcast_to(low, (LANES, LANES)) == iota((LANES, LANES), 0), 1.0, 0.0).astype(jnp.bfloat16))
    left = jnp.concatenate(parts, axis=1)
    right = jnp.concatenate(spots, axis=1)
    table = lax.dot_general(left, right, (((1,), (1,)), ((), ())), preferred_element_type=F32)
    return [table[i * high_rows:(i + 1) * high_rows] for i in range(len(values))]


def inverse_tables(index, valid, high_rows):
    where_from = iota(index.shape, 0) * LANES + iota(index.shape, 1)
    spot = jnp.where(valid, index, -1)
    ones = jnp.ones(index.shape, F32)
    upper, lower, count = one_hot_scatter(
        [(where_from >> 5).astype(F32), (where_from & 31).astype(F32), ones], spot, high_rows)
    table = (upper * 32.0 + lower).astype(I32)
    return jnp.where(count > 0.5, table, -1), count


def send_kernel(size, old_hbm, move_hbm, mass_hbm, head_hbm, tail_hbm, send_hbm, out_ref, table, cons,
                old_ref, move_ref, mass_ref, head_ref, tail_ref, send_ref, sems):
    atom_rows = size["atom_rows"]
    send = size["send"]
    pad_rows = size["atom_pad"]
    copies = [pltpu.make_async_copy(src, dst, sems.at[i]) for i, (src, dst) in enumerate(
        [(old_hbm, old_ref), (move_hbm, move_ref), (mass_hbm, mass_ref), (send_hbm, send_ref), (head_hbm, head_ref),
         (tail_hbm, tail_ref)])]
    for copy in copies:
        copy.start()
    for copy in copies:
        copy.wait()
    table[...] = jnp.zeros(table.shape, F32)
    for r in range(atom_rows):
        span = pl.ds(r * LANES, LANES)
        for d in range(3):
            old = old_ref[d, 0, 0, 0, span].reshape(1, LANES)
            a, b = d * pad_rows + r, (3 + d) * pad_rows + r
            table[a:a + 1, :] = old
            table[b:b + 1, :] = old + move_ref[d, 0, 0, 0, span].reshape(1, LANES)
    load_flat(mass_ref, (0, 0, 0), table, 6 * pad_rows, atom_rows)
    load_flat(head_ref, (0, 0, 0), cons, 0, 8)
    load_flat(tail_ref, (0, 0, 0), cons, 8, 8)
    lane = iota((pad_rows, LANES), 1)
    send_row = size["load_send"](send_ref)
    cons[16:24, :] = jnp.broadcast_to(send_row, (8, LANES))
    index = jnp.broadcast_to(send_row, (pad_rows, LANES))
    low = index & 127
    hit = (index >> 7) == iota((pad_rows, LANES), 0)
    message = jnp.zeros((1, LANES), F32)
    for q in range(7):
        got = jnp.where(hit, pick(table[q * pad_rows:(q + 1) * pad_rows, :], low), 0.0)
        row = jnp.sum(got, axis=0, keepdims=True)
        message = jnp.where(lane[0:1] // send == q, row, message)
    for d in range(out_ref.shape[0]):
        out_ref[d, :, :] = message


def chain_sum(value, prev, extra):
    def body(_, carry):
        total, current = carry
        current = gather_value(current, prev)
        return total + current, current

    return lax.fori_loop(0, extra, body, (value, value))[0]


class Local:
    def __init__(self, direction, diag, kappa, tail_mass, following, child, prev, last, extra, many):
        self.e, self.diag, self.kappa, self.tail_mass = direction, diag, kappa, tail_mass
        self.following, self.child, self.prev, self.last = following, child, prev, last
        self.extra, self.many = extra, many

    def total(self, value):
        return chain_sum(value, self.prev, self.extra) if self.many else value

    def apply(self, value):
        result = self.diag * value + self.kappa * gather_value(value, self.following)
        result = result + gather_value(self.total(self.kappa * value), self.child)
        if self.many:
            for d in range(3):
                force = self.e[d] * value
                others = gather_value(self.total(force), self.last) - force
                result = result - jnp.where(self.last >= 0, self.tail_mass * self.e[d] * others, 0.0)
        return result

    def at_head(self, force):
        return force - gather_value(self.total(force), self.child)

    def at_tail(self, force):
        below = gather_value(self.total(force), self.last) if self.many else force
        return gather_value(force, self.following) - below


def both_ways(extra, run):
    @pl.when(extra == 0)
    def _():
        run(False)

    @pl.when(extra > 0)
    def _():
        run(True)


F_NAMES = ["e0", "e1", "e2", "p0", "p1", "p2", "length", "scale", "head_mass", "tail_mass", "diag", "kappa",
           "base1", "g0", "g1", "g2", "g3"]
I_NAMES = ["following", "child", "prev", "last", "root", "slot", "cidx", "extra", "tinv0", "tinv1", "hinv0", "hinv1"]


def f_get(ref, name):
    i = F_NAMES.index(name)
    return ref[8 * i:8 * i + 8, :]


def i_get(ref, name):
    i = I_NAMES.index(name)
    return ref[8 * i:8 * i + 8, :]


def f_put(ref, name, value):
    i = F_NAMES.index(name)
    ref[8 * i:8 * i + 8, :] = value


def i_put(ref, name, value):
    i = I_NAMES.index(name)
    ref[8 * i:8 * i + 8, :] = value


def local_from(state_f, state_i, extra, many):
    return Local([f_get(state_f, f"e{d}") for d in range(3)], f_get(state_f, "diag"), f_get(state_f, "kappa"),
                 f_get(state_f, "tail_mass"), i_get(state_i, "following"), i_get(state_i, "child"),
                 i_get(state_i, "prev"), i_get(state_i, "last"), extra, many)


def compact_rows(values, cidx):
    high = cidx >> 7
    low = cidx & 127
    lane = iota((1, LANES), 1)
    firsts, rests = [], []
    for i, value in enumerate(values):
        got = gather_rows(value_rows(value), high, low)
        firsts.append(got[2:3] if i % 2 else got[0:1])
        rests.append(got[1:2])
    rows = list(firsts)
    for i in range(0, len(rests), 2):
        other = rests[i + 1] if i + 1 < len(rests) else rests[i]
        rows.append(jnp.where(lane < 64, rests[i], other))
    return rows


def map_kernel(size, table, cons, state_i, number_ref, head_ref, tail_ref, work):
    atom_rows, pad_rows = size["atom_rows"], size["atom_pad"]
    send = size["send"]
    atoms = atom_rows * LANES
    shape = (8, LANES)
    here = iota(shape, 0) * LANES + iota(shape, 1)
    head = cons[0:8, :]
    tail = cons[8:16, :]
    local = tail < atoms

    ext_rows = size["ext_rows"]
    tinv, count = inverse_tables(tail, tail >= 0, ext_rows)
    hinv, _ = inverse_tables(head, head >= 0, pad_rows)
    most = jnp.max(jnp.where(iota(count.shape, 0) < atom_rows, count, 0.0))
    extra = jnp.maximum(most.astype(I32) - 1, 0)
    send_row = cons[16:17, :]
    atom_id = iota((pad_rows, LANES), 0) * LANES + iota((pad_rows, LANES), 1)
    for e in range(send):
        which = jnp.broadcast_to(send_row[:, e:e + 1], (pad_rows, LANES))
        hinv = jnp.where(atom_id == which, 8 * LANES + e, hinv)
    work[0:ext_rows, :] = tinv
    i_put(state_i, "prev", jnp.full(shape, -1, I32))
    i_put(state_i, "last", jnp.where(local, here, -1))

    @pl.when(extra > 0)
    def _():
        def body(c, carry):
            prev, last, inv = carry
            mark = jnp.max(jnp.where(here == c, tail, -1))
            same = tail == mark
            prev = jnp.where(same & (here > c), c, prev)
            last = jnp.where(same & local, c, last)
            spots = iota(inv.shape, 0) * LANES + iota(inv.shape, 1)
            inv = jnp.where(spots == mark, c, inv)
            return prev, last, inv

        prev, last, inv = lax.fori_loop(
            0, 8 * LANES, body, (jnp.full(shape, -1, I32), jnp.full(shape, -1, I32), tinv))
        i_put(state_i, "prev", prev)
        i_put(state_i, "last", last)
        work[0:ext_rows, :] = inv

    tinv = work[0:ext_rows, :]
    tail_high, tail_low = tail >> 7, tail & 127
    head_high, head_low = head >> 7, head & 127
    hinv_rows = value_rows(hinv)[:atom_rows]
    following = gather_rows(hinv_rows, tail_high, tail_low)
    following = jnp.where(local, following, -1)
    following = jnp.where(following < 8 * LANES, following, -1)
    child = gather_rows(value_rows(tinv)[:atom_rows], head_high, head_low)
    root = jnp.where(local, -1, tail - atoms)
    slot = root
    for _ in range(3):
        ahead = gather_value(root + 1, following) - 1
        root = jnp.where(root < 0, ahead, root)
    slots = tinv[atom_rows:atom_rows + 4]
    used = slots >= 0
    used_f = jnp.where(used, 1.0, 0.0)
    before = lax.dot_general(
        jnp.concatenate([used_f, jnp.zeros((4, LANES), F32)], axis=0).astype(jnp.bfloat16),
        jnp.where(iota((LANES, LANES), 0) < iota((LANES, LANES), 1), 1.0, 0.0).astype(jnp.bfloat16),
        (((1,), (0,)), ((), ())), preferred_element_type=F32)
    rank_rows = []
    starts = []
    offset = jnp.zeros((1, 1), F32)
    for r in range(4):
        rank_rows.append(before[r:r + 1] + offset)
        starts.append(offset)
        offset = offset + jnp.sum(used_f[r:r + 1], axis=1, keepdims=True)
    rank = jnp.concatenate(rank_rows, axis=0)
    number = jnp.where(used, rank, -1.0)
    place = number.astype(I32)
    index4 = jnp.concatenate([place, jnp.where(place >= LANES, place + 64, -1)], axis=0)
    from8 = jnp.concatenate([slots, slots], axis=0)
    upper, lower = one_hot_scatter([(from8 >> 5).astype(F32), (from8 & 31).astype(F32)], index4, 8)
    cidx = (upper * 32.0 + lower).astype(I32)
    turned = pltpu.roll(cidx, LANES // 2, 1)
    cidx = jnp.where(iota(shape, 0) == 2, jnp.broadcast_to(turned[0:1, :], shape), cidx)

    marks = number[3:4, :]
    for r in range(4):
        marks = jnp.where(iota((1, LANES), 1) == size["start_lane"] + r, -2.0 - starts[r], marks)
    number = jnp.concatenate([number[0:3, :], marks], axis=0)
    number_ref[0:4, :] = number
    number_ref[4:8, :] = number
    i_put(state_i, "following", following)
    i_put(state_i, "child", child)
    i_put(state_i, "root", root)
    i_put(state_i, "slot", slot)
    i_put(state_i, "cidx", cidx)
    i_put(state_i, "extra", jnp.broadcast_to(extra, shape))
    i_put(state_i, "tinv0", tinv[0:8])
    i_put(state_i, "tinv1", tinv[8:16])
    i_put(state_i, "hinv0", hinv[0:8])
    i_put(state_i, "hinv1", hinv[8:16])

    def rows_of(q):
        return [table[q * pad_rows + r:q * pad_rows + r + 1, :] for r in range(atom_rows)]

    for q in range(7):
        head_ref[8 * q:8 * q + 8, :] = gather_rows(rows_of(q), head_high, head_low)
        tail_ref[8 * q:8 * q + 8, :] = gather_rows(rows_of(q), tail_high, tail_low)


def geometry_kernel(size, state_i, number_ref, head_ref, tail_ref, got_ref, state_f, out_ref, remote, rtab):
    X, Y, Z = size["mesh"]
    send = size["send"]
    shape = (8, LANES)
    slot = i_get(state_i, "slot")
    local = slot < 0
    following = i_get(state_i, "following")
    cidx = i_get(state_i, "cidx")
    extra = jnp.max(i_get(state_i, "extra"))
    gx, gy, gz = my_place()
    for b, (dx, dy, dz) in enumerate(OFFSETS):
        at = (lax.rem(gx + (dx + X), X) * Y + lax.rem(gy + (dy + Y), Y)) * Z + lax.rem(gz + (dz + Z), Z)
        remote[b:b + 1, :] = got_ref[at, :, :]
    sub, lane = iota(shape, 0), iota(shape, 1)
    own = lane // send == sub
    for j in range(4):
        block = remote[8 * j:8 * j + 8, :]
        for q in range(7):
            got = jnp.where(own, pick(block, q * send + lane % send), 0.0)
            row = jnp.sum(got, axis=0, keepdims=True)
            rtab[4 * q + j:4 * q + j + 1, :] = row
    slot_high, slot_low = slot >> 7, slot & 127
    head_at = [head_ref[8 * q:8 * q + 8, :] for q in range(7)]
    tail_at = []
    for q in range(7):
        afar = gather_rows([rtab[4 * q + j:4 * q + j + 1, :] for j in range(4)], slot_high, slot_low)
        tail_at.append(jnp.where(local, tail_ref[8 * q:8 * q + 8, :], afar))
    bond = [head_at[d] - tail_at[d] for d in range(3)]
    gap = [head_at[3 + d] - tail_at[3 + d] for d in range(3)]
    length = jnp.maximum(jnp.sqrt(bond[0] * bond[0] + bond[1] * bond[1] + bond[2] * bond[2]), 0.5)
    direction = [bond[d] / length for d in range(3)]
    scale = 1.0 / jnp.sqrt(head_at[6] + tail_at[6])
    force = [scale * direction[d] for d in range(3)]
    head_mass = head_at[6]
    tail_mass = jnp.where(local, tail_at[6], 0.0)
    norm = force[0] * force[0] + force[1] * force[1] + force[2] * force[2]
    diag = 1.0 - norm * (head_mass + tail_mass)
    ahead = [gather_value(force[d], following) for d in range(3)]
    kappa = tail_mass * (force[0] * ahead[0] + force[1] * ahead[1] + force[2] * ahead[2])
    right = scale * ((direction[0] * gap[0] + direction[1] * gap[1] + direction[2] * gap[2]) - length)
    for d in range(3):
        f_put(state_f, f"e{d}", force[d])
        f_put(state_f, f"p{d}", gap[d])
    f_put(state_f, "length", length)
    f_put(state_f, "scale", scale)
    f_put(state_f, "head_mass", head_mass)
    f_put(state_f, "tail_mass", tail_mass)
    f_put(state_f, "diag", diag)
    f_put(state_f, "kappa", kappa)
    def run(many):
        operator = local_from(state_f, state_i, extra, many)
        terms = [right]
        unit = [jnp.where(local, 0.0, 1.0)]
        for k in range(ORDER):
            terms.append(operator.apply(terms[-1]))
            if k < ORDER - 1:
                unit.append(operator.apply(unit[-1]))
        base = terms[0]
        for term in terms[1:]:
            base = base + term
        f_put(state_f, "base1", base)
        summed = unit[0]
        f_put(state_f, "g0", summed)
        for k in range(1, ORDER):
            summed = summed + unit[k]
            f_put(state_f, f"g{k}", summed)
        rows = compact_rows(force + unit[1:] + terms, cidx)
        rows = rows + value_rows(number_ref[0:4, :])
        part_rows = size["part_rows"]
        rows = rows + [rows[-1]] * (Y * part_rows - len(rows))
        for k in range(Y):
            row_y = lax.rem(lax.axis_index("gy") + k, Y)
            for r in range(0, part_rows, 8):
                some = rows[k * part_rows + r:k * part_rows + min(r + 8, part_rows)]
                block = jnp.concatenate(some, axis=0)
                for x in range(X):
                    for z in range(Z):
                        out_ref[(x * Y + row_y) * Z + z, r:r + len(some), 0, :] = block

    both_ways(extra, run)


def lane_fields(tile):
    lane = iota((1, LANES), 1)
    return lane


def block_masks(tile, send, rows):
    per = LANES // send
    block = iota((rows, LANES), 1) // send + per * tile
    return block // 9 - 1, block // 3 % 3 - 1, block % 3 - 1, [b for b in range(per * tile, per * tile + per)]


def choose(options, field, values):
    result = options[values[0]]
    for v in values[1:]:
        result = jnp.where(field == v, options[v], result)
    return result


def expand_dense(size, load_row, slots, dense):
    X, Y, Z = size["mesh"]
    R = Y * Z
    lane = iota((R, LANES), 1)
    for x in range(X):
        last = load_row("map", x, 3)
        rows = {r: load_row("q", x, r) for r in sorted({r for slot in slots for r in slot[:2]})}
        for l in range(4):
            number = load_row("map", x, l) if l < 3 else last
            start = -2 - pick(last, jnp.full((R, LANES), size["start_lane"] + l, I32))
            low = number & 127
            keep = [lane >= start, (lane < LANES // 2) | (lane - LANES // 2 >= start)]
            for i, (first, rest, half) in enumerate(slots):
                row = jnp.where(keep[half], rows[first], rows[rest])
                value = pick(row, low ^ (half * (LANES // 2)))
                dense[x, i, :, l * LANES:(l + 1) * LANES] = jnp.where(number < 0, 0.0, value)


def aligned(size, dense, q, target, tile):
    X, Y, Z = size["mesh"]
    send = size["send"]
    R = Y * Z
    dx, dy, dz, blocks = block_masks(tile, send, R)
    blocks = [b for b in blocks if b < 27]
    span = pl.ds(tile * LANES, LANES)
    offs = [sorted({OFFSETS[b][k] for b in blocks}) for k in range(3)]
    value = choose({o: dense[lax.rem(target + (X - o), X), q, :, span] for o in offs[0]}, dx, offs[0])
    row_z = iota((R, LANES), 0) % Z
    if R == 8:
        row_y = iota((R, LANES), 0) // Z
        source = lax.rem(row_y - dy + Y, Y) * Z + lax.rem(row_z - dz + Z, Z)
        return pick_row(value, source)
    options = {0: value}
    if 1 in offs[2]:
        options[1] = jnp.where(row_z == 0, turn(value, Z - 1, R), turn(value, -1, R))
    if -1 in offs[2]:
        options[-1] = jnp.where(row_z == Z - 1, turn(value, -(Z - 1), R), turn(value, 1, R))
    value = choose(options, dz, offs[2])
    value = choose({o: turn(value, -o * Z, R) for o in offs[1]}, dy, offs[1])
    return value


def turn(value, by, rows):
    shift = (-by) % rows
    return value if shift == 0 else pltpu.roll(value, shift, 0)


def lane_totals(sums, send):
    stack = jnp.concatenate([parts[0] + parts[1] + parts[2] + parts[3] for parts in sums.values()], axis=0)
    pieces = []
    for _ in range(2):
        piece = stack.astype(jnp.bfloat16)
        pieces.append(piece)
        stack = stack - piece.astype(F32)
    same = iota((2 * LANES, LANES), 0) % send == iota((2 * LANES, LANES), 1) % send
    table = jnp.dot(jnp.concatenate(pieces, axis=1), jnp.where(same, 1.0, 0.0).astype(jnp.bfloat16),
                    preferred_element_type=F32)
    rows = table.shape[0] // len(sums)
    return {key: table[i * rows:(i + 1) * rows] for i, key in enumerate(sums)}


def times(matrix, vector):
    full = {}
    for i, (a, b) in enumerate(SYM):
        full[a, b] = full[b, a] = matrix[i]
    return [full[a, 0] * vector[0] + full[a, 1] * vector[1] + full[a, 2] * vector[2] for a in range(3)]


def recurrence(first, matrices, mass):
    sums, scaled = [], []
    for k in range(ORDER + 1):
        value = first[k]
        for j in range(k):
            back = times(matrices[k - 1 - j], scaled[j])
            value = [value[d] - back[d] for d in range(3)]
        sums.append(value)
        scaled.append([mass * value[d] for d in range(3)])
    total = sums[0]
    for value in sums[1:]:
        total = [total[d] + value[d] for d in range(3)]
    return scaled, total, [mass * total[d] for d in range(3)]


def own_rows(size, place, tiles, tile):
    X, Y, Z = size["mesh"]
    R = Y * Z
    gx, gy, gz = place
    dx, dy, dz, blocks = block_masks(tile, size["send"], R)
    blocks = [b for b in blocks if b < 27]
    wanted = lax.rem(dy + Y, Y) * Z + lax.rem(gz + dz + Z, Z)
    offs = sorted({OFFSETS[b][0] for b in blocks})
    value = choose({o: tiles[o + 1] for o in offs}, dx, offs)
    if R == 8:
        return pick_row(value, wanted)[0:1]
    return jnp.sum(jnp.where(wanted == iota((R, LANES), 0), value, 0.0), axis=0, keepdims=True)


def strided(ref, first, rows, stride):
    if rows <= 8:
        return ref[pl.ds(first, rows, stride=stride), :]
    return jnp.concatenate(
        [ref[pl.ds(first + 8 * i * stride, 8, stride=stride), :] for i in range(rows // 8)], axis=0)


def plane(size, refs, x, row, stride):
    Y, Z = size["mesh"][1:]
    gy = lax.axis_index("gy")
    pieces = []
    for k in range(Y):
        first = (x * Y + lax.rem(gy + k, Y)) * Z
        if stride is None:
            part_rows = size["part_rows"]
            ref = refs[(row // part_rows + k) % Y]
            pieces.append(strided(ref, first * part_rows + row % part_rows, Z, part_rows))
        else:
            pieces.append(strided(refs[0], first * stride + row, Z, stride))
    return jnp.concatenate(pieces, axis=0)


def middle_kernel(size, state_f, state_i, got1, *refs):
    *got2, out_ref, pair_ref, force_ref, matrix_ref, keep_ref, dense = refs
    X, Y, Z = size["mesh"]
    send = size["send"]
    R = Y * Z
    place = my_place()
    gx, gy, gz = place

    def load_row(kind, x, r):
        row = plane(size, got2, x, size["map_row"] + r if kind == "map" else r, None)
        return row.astype(I32) if kind == "map" else row

    expand_dense(size, load_row, [(q, NQ + q // 2, q % 2) for q in range(NQ)], dense)
    scaled_tiles, total_tiles, own_total = [], [], None
    for t in range(3):
        target = lax.rem(gx + (t - 1 + X), X)
        sums = {}
        for tile in range(4):
            q = [aligned(size, dense, i, target, tile) for i in range(NQ)]
            force, unit, terms = q[0:3], q[3:6], q[6:11]
            for d in range(3):
                force_ref[t, d, :, tile * LANES:(tile + 1) * LANES] = force[d]
                for k in range(ORDER + 1):
                    sums.setdefault(("v", k, d), []).append(force[d] * terms[k])
            for s, (a, b) in enumerate(SYM):
                square = force[a] * force[b]
                sums.setdefault(("b", 0, s), []).append(square)
                for k in range(3):
                    sums.setdefault(("b", k + 1, s), []).append(square * unit[k])
        sums = lane_totals(sums, send)
        mass = pick(plane(size, [got1], target, 0, 1), 6 * send + iota((R, LANES), 1) % send)
        matrices = [[sums["b", k, s] for s in range(6)] for k in range(ORDER)]
        for k in range(ORDER):
            for s in range(6):
                matrix_ref[t, 6 * k + s, :, :] = matrices[k][s]
        matrix_ref[t, 24, :, :] = mass
        scaled, total, full = recurrence(
            [[sums["v", k, d] for d in range(3)] for k in range(ORDER + 1)], matrices, mass)
        scaled_tiles.append(scaled)
        total_tiles.append(full)
        if t == 1:
            own_total = total
    keep_ref[...] = jnp.zeros(keep_ref.shape, F32)
    mine = iota((R, LANES), 0) == gz
    for d in range(3):
        keep_ref[d:d + 1, :] = jnp.sum(jnp.where(mine, own_total[d], 0.0), axis=0, keepdims=True)
    corrections = [[] for _ in range(ORDER)]
    moves = [[] for _ in range(3)]
    for tile in range(4):
        force = []
        for d in range(3):
            value = dense[gx, d, :, tile * LANES:(tile + 1) * LANES]
            row = jnp.sum(jnp.where(mine, value, 0.0), axis=0, keepdims=True)
            keep_ref[8 + 4 * d + tile:9 + 4 * d + tile, :] = row
            force.append(row)
        for j in range(ORDER):
            rows = [own_rows(size, place, [scaled_tiles[t][j][d] for t in range(3)], tile) for d in range(3)]
            corrections[j].append(force[0] * rows[0] + force[1] * rows[1] + force[2] * rows[2])
        for d in range(3):
            moves[d].append(own_rows(size, place, [total_tiles[t][d] for t in range(3)], tile))
    root = i_get(state_i, "root")
    slot = i_get(state_i, "slot")
    solved = f_get(state_f, "base1")
    for j in range(ORDER):
        at = gather_rows(corrections[j], root >> 7, root & 127)
        solved = solved - f_get(state_f, f"g{ORDER - 1 - j}") * at
    moved = [gather_rows(moves[d], slot >> 7, slot & 127) for d in range(3)]
    extra = jnp.max(i_get(state_i, "extra"))
    cidx = i_get(state_i, "cidx")

    def run(many):
        operator = local_from(state_f, state_i, extra, many)
        local = slot < 0
        stretch = []
        for d in range(3):
            force = operator.e[d] * solved
            change = f_get(state_f, "head_mass") * operator.at_head(force)
            other = jnp.where(local, operator.tail_mass * operator.at_tail(force), -moved[d])
            stretch.append(f_get(state_f, f"p{d}") - (change - other))
        length = f_get(state_f, "length")
        current = stretch[0] * stretch[0] + stretch[1] * stretch[1] + stretch[2] * stretch[2]
        target = jnp.sqrt(jnp.maximum(2.0 * length * length - current, 0.5 * length * length))
        terms = [f_get(state_f, "scale") * (length - target)]
        for _ in range(ORDER):
            terms.append(operator.apply(terms[-1]))
        base = terms[0]
        for term in terms[1:]:
            base = base + term
        pair_ref[0:8, :] = solved
        pair_ref[8:16, :] = base
        rows = compact_rows(terms, cidx)
        for r, row in enumerate(rows):
            out_ref[0, r:r + 1, :] = row

    both_ways(extra, run)
    for d in range(1, out_ref.shape[0]):
        out_ref[d, :, :] = out_ref[0, :, :]


def final_kernel(size, table, state_f, state_i, got3, pair_ref, force_ref, matrix_ref, keep_ref, *refs):
    *got2, pos_ref, mult_ref, dense = refs
    X, Y, Z = size["mesh"]
    send = size["send"]
    R = Y * Z
    place = my_place()
    gx, gy, gz = place

    def load_row(kind, x, r):
        if kind == "map":
            return plane(size, got2, x, size["map_row"] + r, None).astype(I32)
        return plane(size, [got3], x, r, 8)

    nk = ORDER + 1
    expand_dense(size, load_row, [(q, nk + q // 2, q % 2) for q in range(nk)], dense)
    scaled_tiles, own_total = [], None
    for t in range(3):
        target = lax.rem(gx + (t - 1 + X), X)
        sums = {}
        for tile in range(4):
            terms = [aligned(size, dense, i, target, tile) for i in range(nk)]
            for d in range(3):
                force = force_ref[t, d, :, tile * LANES:(tile + 1) * LANES]
                for k in range(nk):
                    sums.setdefault((k, d), []).append(force * terms[k])
        sums = lane_totals(sums, send)
        matrices = [[matrix_ref[t, 6 * k + s, :, :] for s in range(6)] for k in range(ORDER)]
        scaled, total, _ = recurrence(
            [[sums[k, d] for d in range(3)] for k in range(nk)], matrices, matrix_ref[t, 24, :, :])
        scaled_tiles.append(scaled)
        if t == 1:
            own_total = total
    mine = iota((R, LANES), 0) == gz
    corrections = [[] for _ in range(ORDER)]
    for tile in range(4):
        force = [keep_ref[8 + 4 * d + tile:9 + 4 * d + tile, :] for d in range(3)]
        for j in range(ORDER):
            rows = [own_rows(size, place, [scaled_tiles[t][j][d] for t in range(3)], tile) for d in range(3)]
            corrections[j].append(force[0] * rows[0] + force[1] * rows[1] + force[2] * rows[2])
    root = i_get(state_i, "root")
    solved = pair_ref[8:16, :]
    for j in range(ORDER):
        at = gather_rows(corrections[j], root >> 7, root & 127)
        solved = solved - f_get(state_f, f"g{ORDER - 1 - j}") * at
    both = pair_ref[0:8, :] + solved
    for r in range(8):
        mult_ref[0, 0, 0, pl.ds(r * LANES, LANES)] = both[r, :]
    extra = jnp.max(i_get(state_i, "extra"))

    def run(many):
        operator = local_from(state_f, state_i, extra, many)
        for d in range(3):
            force = operator.e[d] * both
            below = value_rows(operator.total(force))
            sent = keep_ref[d:d + 1, :] + jnp.sum(jnp.where(mine, own_total[d], 0.0), axis=0, keepdims=True)
            above = value_rows(force) + [-sent]
            for part, count in enumerate(size["atom_parts"]):
                hinv = i_get(state_i, f"hinv{part}")
                tinv = i_get(state_i, f"tinv{part}")
                change = gather_rows(above, hinv >> 7, hinv & 127) - gather_rows(below, tinv >> 7, tinv & 127)
                for r in range(count):
                    span = pl.ds((8 * part + r) * LANES, LANES)
                    at = 8 * part + r
                    pos_ref[d, 0, 0, 0, span] = (table[(3 + d) * size["atom_pad"] + at, :]
                                                 - table[6 * size["atom_pad"] + at, :] * change[r, :])

    both_ways(extra, run)


def share(message):
    return lax.all_to_all(message, AXES, split_axis=0, concat_axis=0, tiled=True)


def make_per_device(mesh):
    sizes = axis_sizes(mesh)
    X, Y, Z = sizes
    devices = X * Y * Z
    R = Y * Z

    def per_device(old_pos, displacement, inv_mass, bond_head, bond_tail, send_list):
        atoms = old_pos.shape[-1]
        bonds = bond_head.shape[-1]
        send = send_list.shape[-1]
        atom_rows = atoms // LANES
        assert atoms % LANES == 0 and bonds == 8 * LANES and LANES % send == 0 and atom_rows <= 16 and 3 * LANES < 27 * send <= 4 * LANES - 4
        rows2 = NQ + (NQ + 1) // 2 + 4
        part_rows = -(-rows2 // Y)

        def load_send(ref):
            one = ref[0, 0, 0:1, :]
            return jnp.concatenate([one] * (LANES // send), axis=1)

        size = dict(mesh=sizes, send=send, atom_rows=atom_rows, atom_pad=16, ext_rows=16, part_rows=part_rows,
                    map_row=NQ + (NQ + 1) // 2, load_send=load_send, start_lane=27 * send - 3 * LANES,
                    atom_parts=[min(8, atom_rows), max(atom_rows - 8, 0)])

        def call(kernel, outs, scratch, *args, space=pltpu.VMEM):
            def wrapped(*refs):
                kernel(size, *refs)

            return pl.pallas_call(
                wrapped, out_shape=outs, scratch_shapes=scratch,
                in_specs=[pl.BlockSpec(memory_space=space)] * len(args),
                out_specs=jax.tree.map(lambda _: pl.BlockSpec(memory_space=pltpu.VMEM), outs),
                compiler_params=pltpu.CompilerParams(vmem_limit_bytes=32 * 1024 * 1024),
            )(*[pltpu.with_memory_space_constraint(a, space) for a in args] if space == pltpu.HBM else args)

        S = jax.ShapeDtypeStruct
        one, table, cons = call(
            send_kernel, (S((devices, 1, LANES), F32), S((7 * 16, LANES), F32), S((24, LANES), I32)),
            [pltpu.VMEM(old_pos.shape, F32), pltpu.VMEM(old_pos.shape, F32), pltpu.VMEM(inv_mass.shape, F32),
             pltpu.VMEM(bond_head.shape, I32), pltpu.VMEM(bond_tail.shape, I32), pltpu.VMEM(send_list.shape, I32),
             pltpu.SemaphoreType.DMA((6,))],
            old_pos, displacement, inv_mass, bond_head, bond_tail, send_list, space=pltpu.HBM)
        got1 = share(one)
        state_i, number, head_at, tail_at = call(
            map_kernel,
            (S((8 * len(I_NAMES), LANES), I32), S((8, LANES), F32), S((56, LANES), F32), S((56, LANES), F32)),
            [pltpu.VMEM((16, LANES), I32)], table, cons)
        state_f, two = call(
            geometry_kernel,
            (S((8 * len(F_NAMES), LANES), F32), S((devices, part_rows, 1, LANES), F32)),
            [pltpu.VMEM((32, LANES), F32), pltpu.VMEM((32, LANES), F32)],
            state_i, number, head_at, tail_at, got1)
        got2 = share(two)
        got2 = [got2] + [lax.ppermute(got2, "gy", [((i + k) % Y, i) for i in range(Y)]) for k in range(1, Y)]
        got2 = [g.reshape(devices * part_rows, LANES) for g in got2]
        wide = 4 * LANES
        three, pair, force, matrix, keep = call(
            middle_kernel,
            (S((devices, 8, LANES), F32), S((16, LANES), F32), S((3, 3, R, wide), F32), S((3, 25, R, LANES), F32),
             S((24, LANES), F32)),
            [pltpu.VMEM((X, NQ, R, wide), F32)],
            state_f, state_i, got1.reshape(devices, LANES), *got2)
        got3 = share(three).reshape(devices * 8, LANES)
        return call(
            final_kernel,
            (S(old_pos.shape, F32), S(bond_head.shape, F32)),
            [pltpu.VMEM((X, ORDER + 1, R, wide), F32)],
            table, state_f, state_i, got3, pair, force, matrix, keep, *got2)

    return per_device


def solution(mesh):
    return jax.shard_map(
        make_per_device(mesh),
        mesh=mesh,
        in_specs=(
            P(None, "gx", "gy", "gz", None),
            P(None, "gx", "gy", "gz", None),
            P("gx", "gy", "gz", None),
            P("gx", "gy", "gz", None),
            P("gx", "gy", "gz", None),
            P("gx", "gy", "gz", None),
        ),
        out_specs=(P(None, "gx", "gy", "gz", None), P("gx", "gy", "gz", None)),
        check_vma=False,
    )
```

```python
import math

import jax
import jax.numpy as jnp
from jax import lax
from jax.experimental import pallas as pl
from jax.experimental.pallas import tpu as pltpu
from jax.sharding import PartitionSpec as P

ORDER = 4
HALO = 192
LANES = 128
NQ = 11
AXES = ("gx", "gy", "gz")
OFFSETS = [(b // 9 - 1, b // 3 % 3 - 1, b % 3 - 1) for b in range(27)]
F32 = jnp.float32
I32 = jnp.int32
SYM = [(0, 0), (1, 1), (2, 2), (0, 1), (0, 2), (1, 2)]


def iota(shape, dim):
    return lax.broadcasted_iota(I32, shape, dim)


def pick(table, index):
    return jnp.take_along_axis(table, index, axis=1, mode="promise_in_bounds")


def pick_row(table, index):
    return jnp.take_along_axis(table, index, axis=0, mode="promise_in_bounds")


def spread_row(row, like):
    return jnp.broadcast_to(row, like.shape)


def gather_rows(rows, high, low, base=0):
    result = jnp.zeros(high.shape, rows[0].dtype)
    for r, row in enumerate(rows):
        result = jnp.where(high == base + r, pick(spread_row(row, high), low), result)
    return result


def value_rows(value):
    return [value[r:r + 1, :] for r in range(value.shape[0])]


def gather_value(value, index):
    return gather_rows(value_rows(value), index >> 7, index & 127)


def load_flat(ref, lead, scratch, base, count):
    for r in range(count):
        scratch[base + r:base + r + 1, :] = ref[(*lead, pl.ds(r * LANES, LANES))].reshape(1, LANES)


def axis_sizes(mesh):
    return tuple(mesh.shape[a] for a in AXES)


def my_place():
    return tuple(lax.axis_index(a) for a in AXES)


def one_hot_scatter(values, index, high_rows):
    parts = []
    spots = []
    for r in range(index.shape[0]):
        high = index[r:r + 1, :] >> 7
        low = index[r:r + 1, :] & 127
        hit = jnp.broadcast_to(high, (high_rows, LANES)) == iota((high_rows, LANES), 0)
        parts.append(jnp.concatenate(
            [jnp.where(hit, jnp.broadcast_to(v[r:r + 1, :], (high_rows, LANES)), 0.0) for v in values],
            axis=0).astype(jnp.bfloat16))
        spots.append(jnp.where(
            jnp.broadcast_to(low, (LANES, LANES)) == iota((LANES, LANES), 0), 1.0, 0.0).astype(jnp.bfloat16))
    left = jnp.concatenate(parts, axis=1)
    right = jnp.concatenate(spots, axis=1)
    table = lax.dot_general(left, right, (((1,), (1,)), ((), ())), preferred_element_type=F32)
    return [table[i * high_rows:(i + 1) * high_rows] for i in range(len(values))]


def inverse_tables(index, valid, high_rows):
    where_from = iota(index.shape, 0) * LANES + iota(index.shape, 1)
    spot = jnp.where(valid, index, -1)
    ones = jnp.ones(index.shape, F32)
    upper, lower, count = one_hot_scatter(
        [(where_from >> 5).astype(F32), (where_from & 31).astype(F32), ones], spot, high_rows)
    table = (upper * 32.0 + lower).astype(I32)
    return jnp.where(count > 0.5, table, -1), count


def send_kernel(size, old_hbm, move_hbm, mass_hbm, head_hbm, tail_hbm, send_hbm, out_ref, table, cons,
                old_ref, move_ref, mass_ref, head_ref, tail_ref, send_ref, sems):
    atom_rows = size["atom_rows"]
    send = size["send"]
    pad_rows = size["atom_pad"]
    copies = [pltpu.make_async_copy(src, dst, sems.at[i]) for i, (src, dst) in enumerate(
        [(old_hbm, old_ref), (move_hbm, move_ref), (mass_hbm, mass_ref), (send_hbm, send_ref), (head_hbm, head_ref),
         (tail_hbm, tail_ref)])]
    for copy in copies:
        copy.start()
    for copy in copies:
        copy.wait()
    table[...] = jnp.zeros(table.shape, F32)
    for r in range(atom_rows):
        span = pl.ds(r * LANES, LANES)
        for d in range(3):
            old = old_ref[d, 0, 0, 0, span].reshape(1, LANES)
            a, b = d * pad_rows + r, (3 + d) * pad_rows + r
            table[a:a + 1, :] = old
            table[b:b + 1, :] = old + move_ref[d, 0, 0, 0, span].reshape(1, LANES)
    load_flat(mass_ref, (0, 0, 0), table, 6 * pad_rows, atom_rows)
    load_flat(head_ref, (0, 0, 0), cons, 0, 8)
    load_flat(tail_ref, (0, 0, 0), cons, 8, 8)
    lane = iota((pad_rows, LANES), 1)
    send_row = size["load_send"](send_ref)
    cons[16:24, :] = jnp.broadcast_to(send_row, (8, LANES))
    index = jnp.broadcast_to(send_row, (pad_rows, LANES))
    low = index & 127
    hit = (index >> 7) == iota((pad_rows, LANES), 0)
    message = jnp.zeros((1, LANES), F32)
    for q in range(7):
        got = jnp.where(hit, pick(table[q * pad_rows:(q + 1) * pad_rows, :], low), 0.0)
        row = jnp.sum(got, axis=0, keepdims=True)
        message = jnp.where(lane[0:1] // send == q, row, message)
    for d in range(out_ref.shape[0]):
        out_ref[d, :, :] = message


def chain_sum(value, prev, extra):
    def body(_, carry):
        total, current = carry
        current = gather_value(current, prev)
        return total + current, current

    return lax.fori_loop(0, extra, body, (value, value))[0]


class Local:
    def __init__(self, direction, diag, kappa, tail_mass, following, child, prev, last, extra, many):
        self.e, self.diag, self.kappa, self.tail_mass = direction, diag, kappa, tail_mass
        self.following, self.child, self.prev, self.last = following, child, prev, last
        self.extra, self.many = extra, many

    def total(self, value):
        return chain_sum(value, self.prev, self.extra) if self.many else value

    def apply(self, value):
        result = self.diag * value + self.kappa * gather_value(value, self.following)
        result = result + gather_value(self.total(self.kappa * value), self.child)
        if self.many:
            for d in range(3):
                force = self.e[d] * value
                others = gather_value(self.total(force), self.last) - force
                result = result - jnp.where(self.last >= 0, self.tail_mass * self.e[d] * others, 0.0)
        return result

    def at_head(self, force):
        return force - gather_value(self.total(force), self.child)

    def at_tail(self, force):
        below = gather_value(self.total(force), self.last) if self.many else force
        return gather_value(force, self.following) - below


def both_ways(extra, run):
    @pl.when(extra == 0)
    def _():
        run(False)

    @pl.when(extra > 0)
    def _():
        run(True)


F_NAMES = ["e0", "e1", "e2", "p0", "p1", "p2", "length", "scale", "head_mass", "tail_mass", "diag", "kappa",
           "base1", "g0", "g1", "g2", "g3"]
I_NAMES = ["following", "child", "prev", "last", "root", "slot", "cidx", "extra", "tinv0", "tinv1", "hinv0", "hinv1"]


def f_get(ref, name):
    i = F_NAMES.index(name)
    return ref[8 * i:8 * i + 8, :]


def i_get(ref, name):
    i = I_NAMES.index(name)
    return ref[8 * i:8 * i + 8, :]


def f_put(ref, name, value):
    i = F_NAMES.index(name)
    ref[8 * i:8 * i + 8, :] = value


def i_put(ref, name, value):
    i = I_NAMES.index(name)
    ref[8 * i:8 * i + 8, :] = value


def local_from(state_f, state_i, extra, many):
    return Local([f_get(state_f, f"e{d}") for d in range(3)], f_get(state_f, "diag"), f_get(state_f, "kappa"),
                 f_get(state_f, "tail_mass"), i_get(state_i, "following"), i_get(state_i, "child"),
                 i_get(state_i, "prev"), i_get(state_i, "last"), extra, many)


def compact_rows(values, cidx):
    high = cidx >> 7
    low = cidx & 127
    lane = iota((1, LANES), 1)
    firsts, rests = [], []
    for i, value in enumerate(values):
        got = gather_rows(value_rows(value), high, low)
        firsts.append(got[2:3] if i % 2 else got[0:1])
        rests.append(got[1:2])
    rows = list(firsts)
    for i in range(0, len(rests), 2):
        other = rests[i + 1] if i + 1 < len(rests) else rests[i]
        rows.append(jnp.where(lane < 64, rests[i], other))
    return rows


def map_kernel(size, table, cons, state_i, number_ref, head_ref, tail_ref, work):
    atom_rows, pad_rows = size["atom_rows"], size["atom_pad"]
    send = size["send"]
    atoms = atom_rows * LANES
    shape = (8, LANES)
    here = iota(shape, 0) * LANES + iota(shape, 1)
    head = cons[0:8, :]
    tail = cons[8:16, :]
    local = tail < atoms

    ext_rows = size["ext_rows"]
    tinv, count = inverse_tables(tail, tail >= 0, ext_rows)
    hinv, _ = inverse_tables(head, head >= 0, pad_rows)
    most = jnp.max(jnp.where(iota(count.shape, 0) < atom_rows, count, 0.0))
    extra = jnp.maximum(most.astype(I32) - 1, 0)
    send_row = cons[16:17, :]
    atom_id = iota((pad_rows, LANES), 0) * LANES + iota((pad_rows, LANES), 1)
    for e in range(send):
        which = jnp.broadcast_to(send_row[:, e:e + 1], (pad_rows, LANES))
        hinv = jnp.where(atom_id == which, 8 * LANES + e, hinv)
    work[0:ext_rows, :] = tinv
    i_put(state_i, "prev", jnp.full(shape, -1, I32))
    i_put(state_i, "last", jnp.where(local, here, -1))

    @pl.when(extra > 0)
    def _():
        def body(c, carry):
            prev, last, inv = carry
            mark = jnp.max(jnp.where(here == c, tail, -1))
            same = tail == mark
            prev = jnp.where(same & (here > c), c, prev)
            last = jnp.where(same & local, c, last)
            spots = iota(inv.shape, 0) * LANES + iota(inv.shape, 1)
            inv = jnp.where(spots == mark, c, inv)
            return prev, last, inv

        prev, last, inv = lax.fori_loop(
            0, 8 * LANES, body, (jnp.full(shape, -1, I32), jnp.full(shape, -1, I32), tinv))
        i_put(state_i, "prev", prev)
        i_put(state_i, "last", last)
        work[0:ext_rows, :] = inv

    tinv = work[0:ext_rows, :]
    tail_high, tail_low = tail >> 7, tail & 127
    head_high, head_low = head >> 7, head & 127
    hinv_rows = value_rows(hinv)[:atom_rows]
    following = gather_rows(hinv_rows, tail_high, tail_low)
    following = jnp.where(local, following, -1)
    following = jnp.where(following < 8 * LANES, following, -1)
    child = gather_rows(value_rows(tinv)[:atom_rows], head_high, head_low)
    root = jnp.where(local, -1, tail - atoms)
    slot = root
    for _ in range(3):
        ahead = gather_value(root + 1, following) - 1
        root = jnp.where(root < 0, ahead, root)
    slots = tinv[atom_rows:atom_rows + 4]
    used = slots >= 0
    used_f = jnp.where(used, 1.0, 0.0)
    before = lax.dot_general(
        jnp.concatenate([used_f, jnp.zeros((4, LANES), F32)], axis=0).astype(jnp.bfloat16),
        jnp.where(iota((LANES, LANES), 0) < iota((LANES, LANES), 1), 1.0, 0.0).astype(jnp.bfloat16),
        (((1,), (0,)), ((), ())), preferred_element_type=F32)
    rank_rows = []
    starts = []
    offset = jnp.zeros((1, 1), F32)
    for r in range(4):
        rank_rows.append(before[r:r + 1] + offset)
        starts.append(offset)
        offset = offset + jnp.sum(used_f[r:r + 1], axis=1, keepdims=True)
    rank = jnp.concatenate(rank_rows, axis=0)
    number = jnp.where(used, rank, -1.0)
    place = number.astype(I32)
    index4 = jnp.concatenate([place, jnp.where(place >= LANES, place + 64, -1)], axis=0)
    from8 = jnp.concatenate([slots, slots], axis=0)
    upper, lower = one_hot_scatter([(from8 >> 5).astype(F32), (from8 & 31).astype(F32)], index4, 8)
    cidx = (upper * 32.0 + lower).astype(I32)
    turned = pltpu.roll(cidx, LANES // 2, 1)
    cidx = jnp.where(iota(shape, 0) == 2, jnp.broadcast_to(turned[0:1, :], shape), cidx)

    marks = number[3:4, :]
    for r in range(4):
        marks = jnp.where(iota((1, LANES), 1) == size["start_lane"] + r, -2.0 - starts[r], marks)
    marks = pltpu.roll(jnp.broadcast_to(marks, shape), LANES // 2, 1)[0:1, :]
    number = jnp.concatenate([number[0:3, :], marks], axis=0)
    number_ref[0:4, :] = number
    number_ref[4:8, :] = number
    i_put(state_i, "following", following)
    i_put(state_i, "child", child)
    i_put(state_i, "root", root)
    i_put(state_i, "slot", slot)
    i_put(state_i, "cidx", cidx)
    i_put(state_i, "extra", jnp.broadcast_to(extra, shape))
    i_put(state_i, "tinv0", tinv[0:8])
    i_put(state_i, "tinv1", tinv[8:16])
    i_put(state_i, "hinv0", hinv[0:8])
    i_put(state_i, "hinv1", hinv[8:16])

    def rows_of(q):
        return [table[q * pad_rows + r:q * pad_rows + r + 1, :] for r in range(atom_rows)]

    for q in range(7):
        head_ref[8 * q:8 * q + 8, :] = gather_rows(rows_of(q), head_high, head_low)
        tail_ref[8 * q:8 * q + 8, :] = gather_rows(rows_of(q), tail_high, tail_low)


def geometry_kernel(size, state_i, number_ref, head_ref, tail_ref, got_ref, state_f, out_ref, remote, rtab):
    X, Y, Z = size["mesh"]
    send = size["send"]
    shape = (8, LANES)
    slot = i_get(state_i, "slot")
    local = slot < 0
    following = i_get(state_i, "following")
    cidx = i_get(state_i, "cidx")
    extra = jnp.max(i_get(state_i, "extra"))
    gx, gy, gz = my_place()
    for b, (dx, dy, dz) in enumerate(OFFSETS):
        at = (lax.rem(gx + (dx + X), X) * Y + lax.rem(gy + (dy + Y), Y)) * Z + lax.rem(gz + (dz + Z), Z)
        remote[b:b + 1, :] = got_ref[at, :, :]
    sub, lane = iota(shape, 0), iota(shape, 1)
    own = lane // send == sub
    for j in range(4):
        block = remote[8 * j:8 * j + 8, :]
        for q in range(7):
            got = jnp.where(own, pick(block, q * send + lane % send), 0.0)
            row = jnp.sum(got, axis=0, keepdims=True)
            rtab[4 * q + j:4 * q + j + 1, :] = row
    slot_high, slot_low = slot >> 7, slot & 127
    head_at = [head_ref[8 * q:8 * q + 8, :] for q in range(7)]
    tail_at = []
    for q in range(7):
        afar = gather_rows([rtab[4 * q + j:4 * q + j + 1, :] for j in range(4)], slot_high, slot_low)
        tail_at.append(jnp.where(local, tail_ref[8 * q:8 * q + 8, :], afar))
    bond = [head_at[d] - tail_at[d] for d in range(3)]
    gap = [head_at[3 + d] - tail_at[3 + d] for d in range(3)]
    length = jnp.maximum(jnp.sqrt(bond[0] * bond[0] + bond[1] * bond[1] + bond[2] * bond[2]), 0.5)
    direction = [bond[d] / length for d in range(3)]
    scale = 1.0 / jnp.sqrt(head_at[6] + tail_at[6])
    force = [scale * direction[d] for d in range(3)]
    head_mass = head_at[6]
    tail_mass = jnp.where(local, tail_at[6], 0.0)
    norm = force[0] * force[0] + force[1] * force[1] + force[2] * force[2]
    diag = 1.0 - norm * (head_mass + tail_mass)
    ahead = [gather_value(force[d], following) for d in range(3)]
    kappa = tail_mass * (force[0] * ahead[0] + force[1] * ahead[1] + force[2] * ahead[2])
    right = scale * ((direction[0] * gap[0] + direction[1] * gap[1] + direction[2] * gap[2]) - length)
    for d in range(3):
        f_put(state_f, f"e{d}", force[d])
        f_put(state_f, f"p{d}", gap[d])
    f_put(state_f, "length", length)
    f_put(state_f, "scale", scale)
    f_put(state_f, "head_mass", head_mass)
    f_put(state_f, "tail_mass", tail_mass)
    f_put(state_f, "diag", diag)
    f_put(state_f, "kappa", kappa)
    def run(many):
        operator = local_from(state_f, state_i, extra, many)
        terms = [right]
        unit = [jnp.where(local, 0.0, 1.0)]
        for k in range(ORDER):
            terms.append(operator.apply(terms[-1]))
            if k < ORDER - 1:
                unit.append(operator.apply(unit[-1]))
        base = terms[0]
        for term in terms[1:]:
            base = base + term
        f_put(state_f, "base1", base)
        summed = unit[0]
        f_put(state_f, "g0", summed)
        for k in range(1, ORDER):
            summed = summed + unit[k]
            f_put(state_f, f"g{k}", summed)
        rows = compact_rows(force + unit[1:] + terms, cidx)
        rows[-1] = jnp.where(iota((1, LANES), 1) < LANES // 2, rows[-1], number_ref[3:4, :])
        rows = rows + value_rows(number_ref[0:3, :])
        part_rows = size["part_rows"]
        rows = rows + [rows[-1]] * (Y * part_rows - len(rows))
        for k in range(Y):
            row_y = lax.rem(lax.axis_index("gy") + k, Y)
            for r in range(0, part_rows, 8):
                some = rows[k * part_rows + r:k * part_rows + min(r + 8, part_rows)]
                block = jnp.concatenate(some, axis=0)
                for x in range(X):
                    for z in range(Z):
                        out_ref[(x * Y + row_y) * Z + z, r:r + len(some), 0, :] = block

    both_ways(extra, run)


def lane_fields(tile):
    lane = iota((1, LANES), 1)
    return lane


def block_masks(tile, send, rows):
    per = LANES // send
    block = iota((rows, LANES), 1) // send + per * tile
    return block // 9 - 1, block // 3 % 3 - 1, block % 3 - 1, [b for b in range(per * tile, per * tile + per)]


def choose(options, field, values):
    result = options[values[0]]
    for v in values[1:]:
        result = jnp.where(field == v, options[v], result)
    return result


def expand_dense(size, load_row, slots, dense):
    X, Y, Z = size["mesh"]
    R = Y * Z
    lane = iota((R, LANES), 1)
    for x in range(X):
        last = load_row("map", x, 3)
        marks = load_row("mark", x, 0)
        rows = {r: load_row("q", x, r) for r in sorted({r for slot in slots for r in slot[:2]})}
        for l in range(4):
            number = load_row("map", x, l) if l < 3 else last
            start = -2 - pick(marks, jnp.full((R, LANES), LANES // 2 + size["start_lane"] + l, I32)).astype(I32)
            low = number & 127
            keep = [lane >= start, (lane < LANES // 2) | (lane - LANES // 2 >= start)]
            for i, (first, rest, half) in enumerate(slots):
                row = jnp.where(keep[half], rows[first], rows[rest])
                value = pick(row, low ^ (half * (LANES // 2)))
                dense[x, i, :, l * LANES:(l + 1) * LANES] = jnp.where(number < 0, 0.0, value)


def aligned(size, dense, q, target, tile):
    X, Y, Z = size["mesh"]
    send = size["send"]
    R = Y * Z
    dx, dy, dz, blocks = block_masks(tile, send, R)
    blocks = [b for b in blocks if b < 27]
    span = pl.ds(tile * LANES, LANES)
    offs = [sorted({OFFSETS[b][k] for b in blocks}) for k in range(3)]
    value = choose({o: dense[lax.rem(target + (X - o), X), q, :, span] for o in offs[0]}, dx, offs[0])
    row_z = iota((R, LANES), 0) % Z
    if R == 8:
        row_y = iota((R, LANES), 0) // Z
        source = lax.rem(row_y - dy + Y, Y) * Z + lax.rem(row_z - dz + Z, Z)
        return pick_row(value, source)
    options = {0: value}
    if 1 in offs[2]:
        options[1] = jnp.where(row_z == 0, turn(value, Z - 1, R), turn(value, -1, R))
    if -1 in offs[2]:
        options[-1] = jnp.where(row_z == Z - 1, turn(value, -(Z - 1), R), turn(value, 1, R))
    value = choose(options, dz, offs[2])
    value = choose({o: turn(value, -o * Z, R) for o in offs[1]}, dy, offs[1])
    return value


def turn(value, by, rows):
    shift = (-by) % rows
    return value if shift == 0 else pltpu.roll(value, shift, 0)


def lane_totals(sums, send):
    stack = jnp.concatenate([parts[0] + parts[1] + parts[2] + parts[3] for parts in sums.values()], axis=0)
    pieces = []
    for _ in range(2):
        piece = stack.astype(jnp.bfloat16)
        pieces.append(piece)
        stack = stack - piece.astype(F32)
    same = iota((2 * LANES, LANES), 0) % send == iota((2 * LANES, LANES), 1) % send
    table = jnp.dot(jnp.concatenate(pieces, axis=1), jnp.where(same, 1.0, 0.0).astype(jnp.bfloat16),
                    preferred_element_type=F32)
    rows = table.shape[0] // len(sums)
    return {key: table[i * rows:(i + 1) * rows] for i, key in enumerate(sums)}


def times(matrix, vector):
    full = {}
    for i, (a, b) in enumerate(SYM):
        full[a, b] = full[b, a] = matrix[i]
    return [full[a, 0] * vector[0] + full[a, 1] * vector[1] + full[a, 2] * vector[2] for a in range(3)]


def recurrence(first, matrices, mass):
    sums, scaled = [], []
    for k in range(ORDER + 1):
        value = first[k]
        for j in range(k):
            back = times(matrices[k - 1 - j], scaled[j])
            value = [value[d] - back[d] for d in range(3)]
        sums.append(value)
        scaled.append([mass * value[d] for d in range(3)])
    total = sums[0]
    for value in sums[1:]:
        total = [total[d] + value[d] for d in range(3)]
    return scaled, total, [mass * total[d] for d in range(3)]


def own_rows(size, place, tiles, tile):
    X, Y, Z = size["mesh"]
    R = Y * Z
    gx, gy, gz = place
    dx, dy, dz, blocks = block_masks(tile, size["send"], R)
    blocks = [b for b in blocks if b < 27]
    wanted = lax.rem(dy + Y, Y) * Z + lax.rem(gz + dz + Z, Z)
    offs = sorted({OFFSETS[b][0] for b in blocks})
    value = choose({o: tiles[o + 1] for o in offs}, dx, offs)
    if R == 8:
        return pick_row(value, wanted)[0:1]
    return jnp.sum(jnp.where(wanted == iota((R, LANES), 0), value, 0.0), axis=0, keepdims=True)


def strided(ref, first, rows, stride):
    if rows <= 8:
        return ref[pl.ds(first, rows, stride=stride), :]
    return jnp.concatenate(
        [ref[pl.ds(first + 8 * i * stride, 8, stride=stride), :] for i in range(rows // 8)], axis=0)


def plane(size, refs, x, row, stride):
    Y, Z = size["mesh"][1:]
    gy = lax.axis_index("gy")
    pieces = []
    for k in range(Y):
        first = (x * Y + lax.rem(gy + k, Y)) * Z
        if stride is None:
            part_rows = size["part_rows"]
            ref = refs[(row // part_rows + k) % Y]
            pieces.append(strided(ref, first * part_rows + row % part_rows, Z, part_rows))
        else:
            pieces.append(strided(refs[0], first * stride + row, Z, stride))
    return jnp.concatenate(pieces, axis=0)


def map_row(size, refs, x, tile):
    if tile < 3:
        return plane(size, refs, x, size["map_row"] + tile, None).astype(I32)
    row = plane(size, refs, x, size["map_row"] - 1, None)
    lane = iota(row.shape, 1)
    return jnp.where(lane < LANES // 2, pick(row, lane ^ (LANES // 2)), -1.0).astype(I32)


def middle_kernel(size, state_f, state_i, got1, *refs):
    *got2, out_ref, pair_ref, force_ref, matrix_ref, keep_ref, dense = refs
    X, Y, Z = size["mesh"]
    send = size["send"]
    R = Y * Z
    place = my_place()
    gx, gy, gz = place

    def load_row(kind, x, r):
        if kind == "mark":
            return plane(size, got2, x, size["map_row"] - 1, None)
        return map_row(size, got2, x, r) if kind == "map" else plane(size, got2, x, r, None)

    expand_dense(size, load_row, [(q, NQ + q // 2, q % 2) for q in range(NQ)], dense)
    scaled_tiles, total_tiles, own_total = [], [], None
    for t in range(3):
        target = lax.rem(gx + (t - 1 + X), X)
        sums = {}
        for tile in range(4):
            q = [aligned(size, dense, i, target, tile) for i in range(NQ)]
            force, unit, terms = q[0:3], q[3:6], q[6:11]
            for d in range(3):
                force_ref[t, d, :, tile * LANES:(tile + 1) * LANES] = force[d]
                for k in range(ORDER + 1):
                    sums.setdefault(("v", k, d), []).append(force[d] * terms[k])
            for s, (a, b) in enumerate(SYM):
                square = force[a] * force[b]
                sums.setdefault(("b", 0, s), []).append(square)
                for k in range(3):
                    sums.setdefault(("b", k + 1, s), []).append(square * unit[k])
        sums = lane_totals(sums, send)
        mass = pick(plane(size, [got1], target, 0, 1), 6 * send + iota((R, LANES), 1) % send)
        matrices = [[sums["b", k, s] for s in range(6)] for k in range(ORDER)]
        for k in range(ORDER):
            for s in range(6):
                matrix_ref[t, 6 * k + s, :, :] = matrices[k][s]
        matrix_ref[t, 24, :, :] = mass
        scaled, total, full = recurrence(
            [[sums["v", k, d] for d in range(3)] for k in range(ORDER + 1)], matrices, mass)
        scaled_tiles.append(scaled)
        total_tiles.append(full)
        if t == 1:
            own_total = total
    keep_ref[...] = jnp.zeros(keep_ref.shape, F32)
    mine = iota((R, LANES), 0) == gz
    for d in range(3):
        keep_ref[d:d + 1, :] = jnp.sum(jnp.where(mine, own_total[d], 0.0), axis=0, keepdims=True)
    corrections = [[] for _ in range(ORDER)]
    moves = [[] for _ in range(3)]
    for tile in range(4):
        force = []
        for d in range(3):
            value = dense[gx, d, :, tile * LANES:(tile + 1) * LANES]
            row = jnp.sum(jnp.where(mine, value, 0.0), axis=0, keepdims=True)
            keep_ref[8 + 4 * d + tile:9 + 4 * d + tile, :] = row
            force.append(row)
        for j in range(ORDER):
            rows = [own_rows(size, place, [scaled_tiles[t][j][d] for t in range(3)], tile) for d in range(3)]
            corrections[j].append(force[0] * rows[0] + force[1] * rows[1] + force[2] * rows[2])
        for d in range(3):
            moves[d].append(own_rows(size, place, [total_tiles[t][d] for t in range(3)], tile))
    root = i_get(state_i, "root")
    slot = i_get(state_i, "slot")
    solved = f_get(state_f, "base1")
    for j in range(ORDER):
        at = gather_rows(corrections[j], root >> 7, root & 127)
        solved = solved - f_get(state_f, f"g{ORDER - 1 - j}") * at
    moved = [gather_rows(moves[d], slot >> 7, slot & 127) for d in range(3)]
    extra = jnp.max(i_get(state_i, "extra"))
    cidx = i_get(state_i, "cidx")

    def run(many):
        operator = local_from(state_f, state_i, extra, many)
        local = slot < 0
        stretch = []
        for d in range(3):
            force = operator.e[d] * solved
            change = f_get(state_f, "head_mass") * operator.at_head(force)
            other = jnp.where(local, operator.tail_mass * operator.at_tail(force), -moved[d])
            stretch.append(f_get(state_f, f"p{d}") - (change - other))
        length = f_get(state_f, "length")
        current = stretch[0] * stretch[0] + stretch[1] * stretch[1] + stretch[2] * stretch[2]
        target = jnp.sqrt(jnp.maximum(2.0 * length * length - current, 0.5 * length * length))
        terms = [f_get(state_f, "scale") * (length - target)]
        for _ in range(ORDER):
            terms.append(operator.apply(terms[-1]))
        base = terms[0]
        for term in terms[1:]:
            base = base + term
        pair_ref[0:8, :] = solved
        pair_ref[8:16, :] = base
        rows = compact_rows(terms, cidx)
        for r, row in enumerate(rows):
            out_ref[0, r:r + 1, :] = row

    both_ways(extra, run)
    for d in range(1, out_ref.shape[0]):
        out_ref[d, :, :] = out_ref[0, :, :]


def final_kernel(size, table, state_f, state_i, got3, pair_ref, force_ref, matrix_ref, keep_ref, *refs):
    *got2, pos_ref, mult_ref, dense = refs
    X, Y, Z = size["mesh"]
    send = size["send"]
    R = Y * Z
    place = my_place()
    gx, gy, gz = place

    def load_row(kind, x, r):
        if kind == "mark":
            return plane(size, got2, x, size["map_row"] - 1, None)
        return map_row(size, got2, x, r) if kind == "map" else plane(size, [got3], x, r, 8)

    nk = ORDER + 1
    expand_dense(size, load_row, [(q, nk + q // 2, q % 2) for q in range(nk)], dense)
    scaled_tiles, own_total = [], None
    for t in range(3):
        target = lax.rem(gx + (t - 1 + X), X)
        sums = {}
        for tile in range(4):
            terms = [aligned(size, dense, i, target, tile) for i in range(nk)]
            for d in range(3):
                force = force_ref[t, d, :, tile * LANES:(tile + 1) * LANES]
                for k in range(nk):
                    sums.setdefault((k, d), []).append(force * terms[k])
        sums = lane_totals(sums, send)
        matrices = [[matrix_ref[t, 6 * k + s, :, :] for s in range(6)] for k in range(ORDER)]
        scaled, total, _ = recurrence(
            [[sums[k, d] for d in range(3)] for k in range(nk)], matrices, matrix_ref[t, 24, :, :])
        scaled_tiles.append(scaled)
        if t == 1:
            own_total = total
    mine = iota((R, LANES), 0) == gz
    corrections = [[] for _ in range(ORDER)]
    for tile in range(4):
        force = [keep_ref[8 + 4 * d + tile:9 + 4 * d + tile, :] for d in range(3)]
        for j in range(ORDER):
            rows = [own_rows(size, place, [scaled_tiles[t][j][d] for t in range(3)], tile) for d in range(3)]
            corrections[j].append(force[0] * rows[0] + force[1] * rows[1] + force[2] * rows[2])
    root = i_get(state_i, "root")
    solved = pair_ref[8:16, :]
    for j in range(ORDER):
        at = gather_rows(corrections[j], root >> 7, root & 127)
        solved = solved - f_get(state_f, f"g{ORDER - 1 - j}") * at
    both = pair_ref[0:8, :] + solved
    for r in range(8):
        mult_ref[0, 0, 0, pl.ds(r * LANES, LANES)] = both[r, :]
    extra = jnp.max(i_get(state_i, "extra"))

    def run(many):
        operator = local_from(state_f, state_i, extra, many)
        for d in range(3):
            force = operator.e[d] * both
            below = value_rows(operator.total(force))
            sent = keep_ref[d:d + 1, :] + jnp.sum(jnp.where(mine, own_total[d], 0.0), axis=0, keepdims=True)
            above = value_rows(force) + [-sent]
            for part, count in enumerate(size["atom_parts"]):
                hinv = i_get(state_i, f"hinv{part}")
                tinv = i_get(state_i, f"tinv{part}")
                change = gather_rows(above, hinv >> 7, hinv & 127) - gather_rows(below, tinv >> 7, tinv & 127)
                for r in range(count):
                    span = pl.ds((8 * part + r) * LANES, LANES)
                    at = 8 * part + r
                    pos_ref[d, 0, 0, 0, span] = (table[(3 + d) * size["atom_pad"] + at, :]
                                                 - table[6 * size["atom_pad"] + at, :] * change[r, :])

    both_ways(extra, run)


def share(message):
    return lax.all_to_all(message, AXES, split_axis=0, concat_axis=0, tiled=True)


def make_per_device(mesh):
    sizes = axis_sizes(mesh)
    X, Y, Z = sizes
    devices = X * Y * Z
    R = Y * Z

    def per_device(old_pos, displacement, inv_mass, bond_head, bond_tail, send_list):
        atoms = old_pos.shape[-1]
        bonds = bond_head.shape[-1]
        send = send_list.shape[-1]
        atom_rows = atoms // LANES
        assert atoms % LANES == 0 and bonds == 8 * LANES and LANES % send == 0 and atom_rows <= 16 and 3 * LANES < 27 * send <= 3 * LANES + LANES // 2 - 4
        rows2 = NQ + (NQ + 1) // 2 + 3
        assert NQ % 2 == 1
        part_rows = -(-rows2 // Y)

        def load_send(ref):
            one = ref[0, 0, 0:1, :]
            return jnp.concatenate([one] * (LANES // send), axis=1)

        size = dict(mesh=sizes, send=send, atom_rows=atom_rows, atom_pad=16, ext_rows=16, part_rows=part_rows,
                    map_row=NQ + (NQ + 1) // 2, load_send=load_send, start_lane=27 * send - 3 * LANES,
                    atom_parts=[min(8, atom_rows), max(atom_rows - 8, 0)])

        def call(kernel, outs, scratch, *args, space=pltpu.VMEM):
            def wrapped(*refs):
                kernel(size, *refs)

            return pl.pallas_call(
                wrapped, out_shape=outs, scratch_shapes=scratch,
                in_specs=[pl.BlockSpec(memory_space=space)] * len(args),
                out_specs=jax.tree.map(lambda _: pl.BlockSpec(memory_space=pltpu.VMEM), outs),
                compiler_params=pltpu.CompilerParams(vmem_limit_bytes=32 * 1024 * 1024),
            )(*[pltpu.with_memory_space_constraint(a, space) for a in args] if space == pltpu.HBM else args)

        S = jax.ShapeDtypeStruct
        one, table, cons = call(
            send_kernel, (S((devices, 1, LANES), F32), S((7 * 16, LANES), F32), S((24, LANES), I32)),
            [pltpu.VMEM(old_pos.shape, F32), pltpu.VMEM(old_pos.shape, F32), pltpu.VMEM(inv_mass.shape, F32),
             pltpu.VMEM(bond_head.shape, I32), pltpu.VMEM(bond_tail.shape, I32), pltpu.VMEM(send_list.shape, I32),
             pltpu.SemaphoreType.DMA((6,))],
            old_pos, displacement, inv_mass, bond_head, bond_tail, send_list, space=pltpu.HBM)
        got1 = share(one)
        state_i, number, head_at, tail_at = call(
            map_kernel,
            (S((8 * len(I_NAMES), LANES), I32), S((8, LANES), F32), S((56, LANES), F32), S((56, LANES), F32)),
            [pltpu.VMEM((16, LANES), I32)], table, cons)
        state_f, two = call(
            geometry_kernel,
            (S((8 * len(F_NAMES), LANES), F32), S((devices, part_rows, 1, LANES), F32)),
            [pltpu.VMEM((32, LANES), F32), pltpu.VMEM((32, LANES), F32)],
            state_i, number, head_at, tail_at, got1)
        got2 = share(two)
        got2 = [got2] + [lax.ppermute(got2, "gy", [((i + k) % Y, i) for i in range(Y)]) for k in range(1, Y)]
        got2 = [g.reshape(devices * part_rows, LANES) for g in got2]
        wide = 4 * LANES
        three, pair, force, matrix, keep = call(
            middle_kernel,
            (S((devices, 8, LANES), F32), S((16, LANES), F32), S((3, 3, R, wide), F32), S((3, 25, R, LANES), F32),
             S((24, LANES), F32)),
            [pltpu.VMEM((X, NQ, R, wide), F32)],
            state_f, state_i, got1.reshape(devices, LANES), *got2)
        got3 = share(three).reshape(devices * 8, LANES)
        return call(
            final_kernel,
            (S(old_pos.shape, F32), S(bond_head.shape, F32)),
            [pltpu.VMEM((X, ORDER + 1, R, wide), F32)],
            table, state_f, state_i, got3, pair, force, matrix, keep, *got2)

    return per_device


def solution(mesh):
    return jax.shard_map(
        make_per_device(mesh),
        mesh=mesh,
        in_specs=(
            P(None, "gx", "gy", "gz", None),
            P(None, "gx", "gy", "gz", None),
            P("gx", "gy", "gz", None),
            P("gx", "gy", "gz", None),
            P("gx", "gy", "gz", None),
            P("gx", "gy", "gz", None),
        ),
        out_specs=(P(None, "gx", "gy", "gz", None), P("gx", "gy", "gz", None)),
        check_vma=False,
    )
```

```python
import math

import jax
import jax.numpy as jnp
from jax import lax
from jax.experimental import pallas as pl
from jax.experimental.pallas import tpu as pltpu
from jax.sharding import PartitionSpec as P

ORDER = 4
HALO = 192
LANES = 128
NQ = 11
AXES = ("gx", "gy", "gz")
OFFSETS = [(b // 9 - 1, b // 3 % 3 - 1, b % 3 - 1) for b in range(27)]
F32 = jnp.float32
I32 = jnp.int32
SYM = [(0, 0), (1, 1), (2, 2), (0, 1), (0, 2), (1, 2)]


def iota(shape, dim):
    return lax.broadcasted_iota(I32, shape, dim)


def pick(table, index):
    return jnp.take_along_axis(table, index, axis=1, mode="promise_in_bounds")


def pick_row(table, index):
    return jnp.take_along_axis(table, index, axis=0, mode="promise_in_bounds")


def spread_row(row, like):
    return jnp.broadcast_to(row, like.shape)


def gather_rows(rows, high, low, base=0):
    result = jnp.zeros(high.shape, rows[0].dtype)
    for r, row in enumerate(rows):
        result = jnp.where(high == base + r, pick(spread_row(row, high), low), result)
    return result


def value_rows(value):
    return [value[r:r + 1, :] for r in range(value.shape[0])]


def gather_value(value, index):
    return gather_rows(value_rows(value), index >> 7, index & 127)


def load_flat(ref, lead, scratch, base, count):
    for r in range(count):
        scratch[base + r:base + r + 1, :] = ref[(*lead, pl.ds(r * LANES, LANES))].reshape(1, LANES)


def axis_sizes(mesh):
    return tuple(mesh.shape[a] for a in AXES)


def my_place():
    return tuple(lax.axis_index(a) for a in AXES)


def one_hot_scatter(values, index, high_rows):
    parts = []
    spots = []
    for r in range(index.shape[0]):
        high = index[r:r + 1, :] >> 7
        low = index[r:r + 1, :] & 127
        hit = jnp.broadcast_to(high, (high_rows, LANES)) == iota((high_rows, LANES), 0)
        parts.append(jnp.concatenate(
            [jnp.where(hit, jnp.broadcast_to(v[r:r + 1, :], (high_rows, LANES)), 0.0) for v in values],
            axis=0).astype(jnp.bfloat16))
        spots.append(jnp.where(
            jnp.broadcast_to(low, (LANES, LANES)) == iota((LANES, LANES), 0), 1.0, 0.0).astype(jnp.bfloat16))
    left = jnp.concatenate(parts, axis=1)
    right = jnp.concatenate(spots, axis=1)
    table = lax.dot_general(left, right, (((1,), (1,)), ((), ())), preferred_element_type=F32)
    return [table[i * high_rows:(i + 1) * high_rows] for i in range(len(values))]


def inverse_tables(index, valid, high_rows):
    where_from = iota(index.shape, 0) * LANES + iota(index.shape, 1)
    spot = jnp.where(valid, index, -1)
    ones = jnp.ones(index.shape, F32)
    upper, lower, count = one_hot_scatter(
        [(where_from >> 5).astype(F32), (where_from & 31).astype(F32), ones], spot, high_rows)
    table = (upper * 32.0 + lower).astype(I32)
    return jnp.where(count > 0.5, table, -1), count


def send_kernel(size, old_hbm, move_hbm, mass_hbm, head_hbm, tail_hbm, send_hbm, out_ref, table, cons,
                old_ref, move_ref, mass_ref, head_ref, tail_ref, send_ref, sems):
    atom_rows = size["atom_rows"]
    send = size["send"]
    pad_rows = size["atom_pad"]
    copies = [pltpu.make_async_copy(src, dst, sems.at[i]) for i, (src, dst) in enumerate(
        [(old_hbm, old_ref), (move_hbm, move_ref), (mass_hbm, mass_ref), (send_hbm, send_ref), (head_hbm, head_ref),
         (tail_hbm, tail_ref)])]
    for copy in copies:
        copy.start()
    for copy in copies:
        copy.wait()
    table[...] = jnp.zeros(table.shape, F32)
    for r in range(atom_rows):
        span = pl.ds(r * LANES, LANES)
        for d in range(3):
            old = old_ref[d, 0, 0, 0, span].reshape(1, LANES)
            a, b = d * pad_rows + r, (3 + d) * pad_rows + r
            table[a:a + 1, :] = old
            table[b:b + 1, :] = old + move_ref[d, 0, 0, 0, span].reshape(1, LANES)
    load_flat(mass_ref, (0, 0, 0), table, 6 * pad_rows, atom_rows)
    load_flat(head_ref, (0, 0, 0), cons, 0, 8)
    load_flat(tail_ref, (0, 0, 0), cons, 8, 8)
    lane = iota((pad_rows, LANES), 1)
    send_row = size["load_send"](send_ref)
    cons[16:24, :] = jnp.broadcast_to(send_row, (8, LANES))
    index = jnp.broadcast_to(send_row, (pad_rows, LANES))
    low = index & 127
    hit = (index >> 7) == iota((pad_rows, LANES), 0)
    message = jnp.zeros((1, LANES), F32)
    for q in range(7):
        got = jnp.where(hit, pick(table[q * pad_rows:(q + 1) * pad_rows, :], low), 0.0)
        row = jnp.sum(got, axis=0, keepdims=True)
        message = jnp.where(lane[0:1] // send == q, row, message)
    for d in range(out_ref.shape[0]):
        out_ref[d, :, :] = message


def chain_sum(value, prev, extra):
    def body(_, carry):
        total, current = carry
        current = gather_value(current, prev)
        return total + current, current

    return lax.fori_loop(0, extra, body, (value, value))[0]


class Local:
    def __init__(self, direction, diag, kappa, tail_mass, following, child, prev, last, extra, many):
        self.e, self.diag, self.kappa, self.tail_mass = direction, diag, kappa, tail_mass
        self.following, self.child, self.prev, self.last = following, child, prev, last
        self.extra, self.many = extra, many
        self.child_kappa = None if many else gather_value(kappa, child)

    def total(self, value):
        return chain_sum(value, self.prev, self.extra) if self.many else value

    def apply(self, value):
        result = self.diag * value + self.kappa * gather_value(value, self.following)
        if not self.many:
            return result + self.child_kappa * gather_value(value, self.child)
        result = result + gather_value(self.total(self.kappa * value), self.child)
        if self.many:
            for d in range(3):
                force = self.e[d] * value
                others = gather_value(self.total(force), self.last) - force
                result = result - jnp.where(self.last >= 0, self.tail_mass * self.e[d] * others, 0.0)
        return result

    def powers(self, value):
        terms = [value]
        if self.many or ORDER != 4:
            for _ in range(ORDER):
                terms.append(self.apply(terms[-1]))
            return terms
        n, c, k, d, kc = self.following, self.child, self.kappa, self.diag, self.child_kappa
        n2 = gather_value(n + 1, n) - 1
        c2 = gather_value(c + 1, c) - 1
        far_n = k * gather_value(k, n)
        far_c = kc * gather_value(kc, c)
        near_n = k * (d + gather_value(d, n))
        near_c = kc * (d + gather_value(d, c))
        own = d * d + k * k + kc * kc

        def twice(u, u_n, u_c):
            return (own * u + near_n * u_n + near_c * u_c) + (
                far_n * gather_value(u, n2) + far_c * gather_value(u, c2))

        u_n, u_c = gather_value(value, n), gather_value(value, c)
        one = d * value + k * u_n + kc * u_c
        two = twice(value, u_n, u_c)
        three = twice(one, gather_value(one, n), gather_value(one, c))
        four = twice(two, gather_value(two, n), gather_value(two, c))
        return [value, one, two, three, four]

    def at_head(self, force):
        return force - gather_value(self.total(force), self.child)

    def at_tail(self, force):
        below = gather_value(self.total(force), self.last) if self.many else force
        return gather_value(force, self.following) - below


def both_ways(extra, run):
    @pl.when(extra == 0)
    def _():
        run(False)

    @pl.when(extra > 0)
    def _():
        run(True)


F_NAMES = ["e0", "e1", "e2", "p0", "p1", "p2", "length", "scale", "head_mass", "tail_mass", "diag", "kappa",
           "base1", "g0", "g1", "g2", "g3"]
I_NAMES = ["following", "child", "prev", "last", "root", "slot", "cidx", "extra", "tinv0", "tinv1", "hinv0", "hinv1"]


def f_get(ref, name):
    i = F_NAMES.index(name)
    return ref[8 * i:8 * i + 8, :]


def i_get(ref, name):
    i = I_NAMES.index(name)
    return ref[8 * i:8 * i + 8, :]


def f_put(ref, name, value):
    i = F_NAMES.index(name)
    ref[8 * i:8 * i + 8, :] = value


def i_put(ref, name, value):
    i = I_NAMES.index(name)
    ref[8 * i:8 * i + 8, :] = value


def local_from(state_f, state_i, extra, many):
    return Local([f_get(state_f, f"e{d}") for d in range(3)], f_get(state_f, "diag"), f_get(state_f, "kappa"),
                 f_get(state_f, "tail_mass"), i_get(state_i, "following"), i_get(state_i, "child"),
                 i_get(state_i, "prev"), i_get(state_i, "last"), extra, many)


def compact_rows(values, cidx):
    high = cidx >> 7
    low = cidx & 127
    lane = iota((1, LANES), 1)
    firsts, rests = [], []
    for i, value in enumerate(values):
        got = gather_rows(value_rows(value), high, low)
        firsts.append(got[2:3] if i % 2 else got[0:1])
        rests.append(got[1:2])
    rows = list(firsts)
    for i in range(0, len(rests), 2):
        other = rests[i + 1] if i + 1 < len(rests) else rests[i]
        rows.append(jnp.where(lane < 64, rests[i], other))
    return rows


def map_kernel(size, table, cons, state_i, number_ref, head_ref, tail_ref, work):
    atom_rows, pad_rows = size["atom_rows"], size["atom_pad"]
    send = size["send"]
    atoms = atom_rows * LANES
    shape = (8, LANES)
    here = iota(shape, 0) * LANES + iota(shape, 1)
    head = cons[0:8, :]
    tail = cons[8:16, :]
    local = tail < atoms

    ext_rows = size["ext_rows"]
    tinv, count = inverse_tables(tail, tail >= 0, ext_rows)
    hinv, _ = inverse_tables(head, head >= 0, pad_rows)
    most = jnp.max(jnp.where(iota(count.shape, 0) < atom_rows, count, 0.0))
    extra = jnp.maximum(most.astype(I32) - 1, 0)
    send_row = cons[16:17, :]
    atom_id = iota((pad_rows, LANES), 0) * LANES + iota((pad_rows, LANES), 1)
    for e in range(send):
        which = jnp.broadcast_to(send_row[:, e:e + 1], (pad_rows, LANES))
        hinv = jnp.where(atom_id == which, 8 * LANES + e, hinv)
    work[0:ext_rows, :] = tinv
    i_put(state_i, "prev", jnp.full(shape, -1, I32))
    i_put(state_i, "last", jnp.where(local, here, -1))

    @pl.when(extra > 0)
    def _():
        def body(c, carry):
            prev, last, inv = carry
            mark = jnp.max(jnp.where(here == c, tail, -1))
            same = tail == mark
            prev = jnp.where(same & (here > c), c, prev)
            last = jnp.where(same & local, c, last)
            spots = iota(inv.shape, 0) * LANES + iota(inv.shape, 1)
            inv = jnp.where(spots == mark, c, inv)
            return prev, last, inv

        prev, last, inv = lax.fori_loop(
            0, 8 * LANES, body, (jnp.full(shape, -1, I32), jnp.full(shape, -1, I32), tinv))
        i_put(state_i, "prev", prev)
        i_put(state_i, "last", last)
        work[0:ext_rows, :] = inv

    tinv = work[0:ext_rows, :]
    tail_high, tail_low = tail >> 7, tail & 127
    head_high, head_low = head >> 7, head & 127
    hinv_rows = value_rows(hinv)[:atom_rows]
    following = gather_rows(hinv_rows, tail_high, tail_low)
    following = jnp.where(local, following, -1)
    following = jnp.where(following < 8 * LANES, following, -1)
    child = gather_rows(value_rows(tinv)[:atom_rows], head_high, head_low)
    root = jnp.where(local, -1, tail - atoms)
    slot = root
    for _ in range(3):
        ahead = gather_value(root + 1, following) - 1
        root = jnp.where(root < 0, ahead, root)
    slots = tinv[atom_rows:atom_rows + 4]
    used = slots >= 0
    used_f = jnp.where(used, 1.0, 0.0)
    before = lax.dot_general(
        jnp.concatenate([used_f, jnp.zeros((4, LANES), F32)], axis=0).astype(jnp.bfloat16),
        jnp.where(iota((LANES, LANES), 0) < iota((LANES, LANES), 1), 1.0, 0.0).astype(jnp.bfloat16),
        (((1,), (0,)), ((), ())), preferred_element_type=F32)
    rank_rows = []
    starts = []
    offset = jnp.zeros((1, 1), F32)
    for r in range(4):
        rank_rows.append(before[r:r + 1] + offset)
        starts.append(offset)
        offset = offset + jnp.sum(used_f[r:r + 1], axis=1, keepdims=True)
    rank = jnp.concatenate(rank_rows, axis=0)
    number = jnp.where(used, rank, -1.0)
    place = number.astype(I32)
    index4 = jnp.concatenate([place, jnp.where(place >= LANES, place + 64, -1)], axis=0)
    from8 = jnp.concatenate([slots, slots], axis=0)
    upper, lower = one_hot_scatter([(from8 >> 5).astype(F32), (from8 & 31).astype(F32)], index4, 8)
    cidx = (upper * 32.0 + lower).astype(I32)
    turned = pltpu.roll(cidx, LANES // 2, 1)
    cidx = jnp.where(iota(shape, 0) == 2, jnp.broadcast_to(turned[0:1, :], shape), cidx)

    marks = number[3:4, :]
    for r in range(4):
        marks = jnp.where(iota((1, LANES), 1) == size["start_lane"] + r, -2.0 - starts[r], marks)
    marks = pltpu.roll(jnp.broadcast_to(marks, shape), LANES // 2, 1)[0:1, :]
    number = jnp.concatenate([number[0:3, :], marks], axis=0)
    number_ref[0:4, :] = number
    number_ref[4:8, :] = number
    i_put(state_i, "following", following)
    i_put(state_i, "child", child)
    i_put(state_i, "root", root)
    i_put(state_i, "slot", slot)
    i_put(state_i, "cidx", cidx)
    i_put(state_i, "extra", jnp.broadcast_to(extra, shape))
    i_put(state_i, "tinv0", tinv[0:8])
    i_put(state_i, "tinv1", tinv[8:16])
    i_put(state_i, "hinv0", hinv[0:8])
    i_put(state_i, "hinv1", hinv[8:16])

    def rows_of(q):
        return [table[q * pad_rows + r:q * pad_rows + r + 1, :] for r in range(atom_rows)]

    for q in range(7):
        head_ref[8 * q:8 * q + 8, :] = gather_rows(rows_of(q), head_high, head_low)
        tail_ref[8 * q:8 * q + 8, :] = gather_rows(rows_of(q), tail_high, tail_low)


def geometry_kernel(size, state_i, number_ref, head_ref, tail_ref, got_ref, state_f, out_ref, remote, rtab):
    X, Y, Z = size["mesh"]
    send = size["send"]
    shape = (8, LANES)
    slot = i_get(state_i, "slot")
    local = slot < 0
    following = i_get(state_i, "following")
    cidx = i_get(state_i, "cidx")
    extra = jnp.max(i_get(state_i, "extra"))
    gx, gy, gz = my_place()
    for b, (dx, dy, dz) in enumerate(OFFSETS):
        at = (lax.rem(gx + (dx + X), X) * Y + lax.rem(gy + (dy + Y), Y)) * Z + lax.rem(gz + (dz + Z), Z)
        remote[b:b + 1, :] = got_ref[at, :, :]
    lane = iota(shape, 1)
    for j in range(4):
        block = remote[8 * j:8 * j + 8, :]
        for q in range(7):
            row = pick_row(pick(block, q * send + lane % send), lane // send % 8)[0:1]
            rtab[4 * q + j:4 * q + j + 1, :] = row
    slot_high, slot_low = slot >> 7, slot & 127
    head_at = [head_ref[8 * q:8 * q + 8, :] for q in range(7)]
    tail_at = []
    for q in range(7):
        afar = gather_rows([rtab[4 * q + j:4 * q + j + 1, :] for j in range(4)], slot_high, slot_low)
        tail_at.append(jnp.where(local, tail_ref[8 * q:8 * q + 8, :], afar))
    bond = [head_at[d] - tail_at[d] for d in range(3)]
    gap = [head_at[3 + d] - tail_at[3 + d] for d in range(3)]
    length = jnp.maximum(jnp.sqrt(bond[0] * bond[0] + bond[1] * bond[1] + bond[2] * bond[2]), 0.5)
    direction = [bond[d] / length for d in range(3)]
    scale = 1.0 / jnp.sqrt(head_at[6] + tail_at[6])
    force = [scale * direction[d] for d in range(3)]
    head_mass = head_at[6]
    tail_mass = jnp.where(local, tail_at[6], 0.0)
    norm = force[0] * force[0] + force[1] * force[1] + force[2] * force[2]
    diag = 1.0 - norm * (head_mass + tail_mass)
    ahead = [gather_value(force[d], following) for d in range(3)]
    kappa = tail_mass * (force[0] * ahead[0] + force[1] * ahead[1] + force[2] * ahead[2])
    right = scale * ((direction[0] * gap[0] + direction[1] * gap[1] + direction[2] * gap[2]) - length)
    for d in range(3):
        f_put(state_f, f"e{d}", force[d])
        f_put(state_f, f"p{d}", gap[d])
    f_put(state_f, "length", length)
    f_put(state_f, "scale", scale)
    f_put(state_f, "head_mass", head_mass)
    f_put(state_f, "tail_mass", tail_mass)
    f_put(state_f, "diag", diag)
    f_put(state_f, "kappa", kappa)
    def run(many):
        operator = local_from(state_f, state_i, extra, many)
        terms = [right]
        unit = [jnp.where(local, 0.0, 1.0)]
        for k in range(ORDER):
            terms.append(operator.apply(terms[-1]))
            if k < ORDER - 1:
                unit.append(operator.apply(unit[-1]))
        base = terms[0]
        for term in terms[1:]:
            base = base + term
        f_put(state_f, "base1", base)
        summed = unit[0]
        f_put(state_f, "g0", summed)
        for k in range(1, ORDER):
            summed = summed + unit[k]
            f_put(state_f, f"g{k}", summed)
        rows = compact_rows(force + unit[1:] + terms, cidx)
        rows[-1] = jnp.where(iota((1, LANES), 1) < LANES // 2, rows[-1], number_ref[3:4, :])
        rows = rows + value_rows(number_ref[0:3, :])
        part_rows = size["part_rows"]
        rows = rows + [rows[-1]] * (Y * part_rows - len(rows))
        for k in range(Y):
            row_y = lax.rem(lax.axis_index("gy") + k, Y)
            for r in range(0, part_rows, 8):
                some = rows[k * part_rows + r:k * part_rows + min(r + 8, part_rows)]
                block = jnp.concatenate(some, axis=0)
                for x in range(X):
                    for z in range(Z):
                        out_ref[(x * Y + row_y) * Z + z, r:r + len(some), 0, :] = block

    both_ways(extra, run)


def lane_fields(tile):
    lane = iota((1, LANES), 1)
    return lane


def block_masks(tile, send, rows):
    per = LANES // send
    block = iota((rows, LANES), 1) // send + per * tile
    return block // 9 - 1, block // 3 % 3 - 1, block % 3 - 1, [b for b in range(per * tile, per * tile + per)]


def choose(options, field, values):
    result = options[values[0]]
    for v in values[1:]:
        result = jnp.where(field == v, options[v], result)
    return result


def expand_dense(size, load_row, slots, dense):
    X, Y, Z = size["mesh"]
    R = Y * Z
    lane = iota((R, LANES), 1)
    for x in range(X):
        last = load_row("map", x, 3)
        marks = load_row("mark", x, 0)
        rows = {r: load_row("q", x, r) for r in sorted({r for slot in slots for r in slot[:2]})}
        for l in range(4):
            number = load_row("map", x, l) if l < 3 else last
            start = -2 - pick(marks, jnp.full((R, LANES), LANES // 2 + size["start_lane"] + l, I32)).astype(I32)
            low = number & 127
            keep = [lane >= start, (lane < LANES // 2) | (lane - LANES // 2 >= start)]
            for i, (first, rest, half) in enumerate(slots):
                row = jnp.where(keep[half], rows[first], rows[rest])
                value = pick(row, low ^ (half * (LANES // 2)))
                dense[x, i, :, l * LANES:(l + 1) * LANES] = jnp.where(number < 0, 0.0, value)


def aligned(size, dense, q, target, tile):
    X, Y, Z = size["mesh"]
    send = size["send"]
    R = Y * Z
    dx, dy, dz, blocks = block_masks(tile, send, R)
    blocks = [b for b in blocks if b < 27]
    span = pl.ds(tile * LANES, LANES)
    offs = [sorted({OFFSETS[b][k] for b in blocks}) for k in range(3)]
    value = choose({o: dense[lax.rem(target + (X - o), X), q, :, span] for o in offs[0]}, dx, offs[0])
    row_z = iota((R, LANES), 0) % Z
    if R == 8:
        row_y = iota((R, LANES), 0) // Z
        source = lax.rem(row_y - dy + Y, Y) * Z + lax.rem(row_z - dz + Z, Z)
        return pick_row(value, source)
    options = {0: value}
    if 1 in offs[2]:
        options[1] = jnp.where(row_z == 0, turn(value, Z - 1, R), turn(value, -1, R))
    if -1 in offs[2]:
        options[-1] = jnp.where(row_z == Z - 1, turn(value, -(Z - 1), R), turn(value, 1, R))
    value = choose(options, dz, offs[2])
    value = choose({o: turn(value, -o * Z, R) for o in offs[1]}, dy, offs[1])
    return value


def turn(value, by, rows):
    shift = (-by) % rows
    return value if shift == 0 else pltpu.roll(value, shift, 0)


def lane_totals(sums, send):
    stack = jnp.concatenate([parts[0] + parts[1] + parts[2] + parts[3] for parts in sums.values()], axis=0)
    pieces = []
    for _ in range(2):
        piece = stack.astype(jnp.bfloat16)
        pieces.append(piece)
        stack = stack - piece.astype(F32)
    same = iota((2 * LANES, LANES), 0) % send == iota((2 * LANES, LANES), 1) % send
    table = jnp.dot(jnp.concatenate(pieces, axis=1), jnp.where(same, 1.0, 0.0).astype(jnp.bfloat16),
                    preferred_element_type=F32)
    rows = table.shape[0] // len(sums)
    return {key: table[i * rows:(i + 1) * rows] for i, key in enumerate(sums)}


def times(matrix, vector):
    full = {}
    for i, (a, b) in enumerate(SYM):
        full[a, b] = full[b, a] = matrix[i]
    return [full[a, 0] * vector[0] + full[a, 1] * vector[1] + full[a, 2] * vector[2] for a in range(3)]


def recurrence(first, matrices, mass):
    sums, scaled = [], []
    for k in range(ORDER + 1):
        value = first[k]
        for j in range(k):
            back = times(matrices[k - 1 - j], scaled[j])
            value = [value[d] - back[d] for d in range(3)]
        sums.append(value)
        scaled.append([mass * value[d] for d in range(3)])
    total = sums[0]
    for value in sums[1:]:
        total = [total[d] + value[d] for d in range(3)]
    return scaled, total, [mass * total[d] for d in range(3)]


def own_rows(size, place, tiles, tile):
    X, Y, Z = size["mesh"]
    R = Y * Z
    gx, gy, gz = place
    dx, dy, dz, blocks = block_masks(tile, size["send"], R)
    blocks = [b for b in blocks if b < 27]
    wanted = lax.rem(dy + Y, Y) * Z + lax.rem(gz + dz + Z, Z)
    offs = sorted({OFFSETS[b][0] for b in blocks})
    value = choose({o: tiles[o + 1] for o in offs}, dx, offs)
    if R == 8:
        return pick_row(value, wanted)[0:1]
    return jnp.sum(jnp.where(wanted == iota((R, LANES), 0), value, 0.0), axis=0, keepdims=True)


def strided(ref, first, rows, stride):
    if rows <= 8:
        return ref[pl.ds(first, rows, stride=stride), :]
    return jnp.concatenate(
        [ref[pl.ds(first + 8 * i * stride, 8, stride=stride), :] for i in range(rows // 8)], axis=0)


def plane(size, refs, x, row, stride):
    Y, Z = size["mesh"][1:]
    gy = lax.axis_index("gy")
    pieces = []
    for k in range(Y):
        first = (x * Y + lax.rem(gy + k, Y)) * Z
        if stride is None:
            part_rows = size["part_rows"]
            ref = refs[(row // part_rows + k) % Y]
            pieces.append(strided(ref, first * part_rows + row % part_rows, Z, part_rows))
        else:
            pieces.append(strided(refs[0], first * stride + row, Z, stride))
    return jnp.concatenate(pieces, axis=0)


def map_row(size, refs, x, tile):
    if tile < 3:
        return plane(size, refs, x, size["map_row"] + tile, None).astype(I32)
    row = plane(size, refs, x, size["map_row"] - 1, None)
    lane = iota(row.shape, 1)
    return jnp.where(lane < LANES // 2, pick(row, lane ^ (LANES // 2)), -1.0).astype(I32)


def middle_kernel(size, state_f, state_i, got1, *refs):
    *got2, out_ref, pair_ref, force_ref, matrix_ref, keep_ref, dense = refs
    X, Y, Z = size["mesh"]
    send = size["send"]
    R = Y * Z
    place = my_place()
    gx, gy, gz = place

    def load_row(kind, x, r):
        if kind == "mark":
            return plane(size, got2, x, size["map_row"] - 1, None)
        return map_row(size, got2, x, r) if kind == "map" else plane(size, got2, x, r, None)

    expand_dense(size, load_row, [(q, NQ + q // 2, q % 2) for q in range(NQ)], dense)
    scaled_tiles, total_tiles, own_total = [], [], None
    for t in range(3):
        target = lax.rem(gx + (t - 1 + X), X)
        sums = {}
        for tile in range(4):
            q = [aligned(size, dense, i, target, tile) for i in range(NQ)]
            force, unit, terms = q[0:3], q[3:6], q[6:11]
            for d in range(3):
                force_ref[t, d, :, tile * LANES:(tile + 1) * LANES] = force[d]
                for k in range(ORDER + 1):
                    sums.setdefault(("v", k, d), []).append(force[d] * terms[k])
            for s, (a, b) in enumerate(SYM):
                square = force[a] * force[b]
                sums.setdefault(("b", 0, s), []).append(square)
                for k in range(3):
                    sums.setdefault(("b", k + 1, s), []).append(square * unit[k])
        sums = lane_totals(sums, send)
        mass = pick(plane(size, [got1], target, 0, 1), 6 * send + iota((R, LANES), 1) % send)
        matrices = [[sums["b", k, s] for s in range(6)] for k in range(ORDER)]
        for k in range(ORDER):
            for s in range(6):
                matrix_ref[t, 6 * k + s, :, :] = matrices[k][s]
        matrix_ref[t, 24, :, :] = mass
        scaled, total, full = recurrence(
            [[sums["v", k, d] for d in range(3)] for k in range(ORDER + 1)], matrices, mass)
        scaled_tiles.append(scaled)
        total_tiles.append(full)
        if t == 1:
            own_total = total
    keep_ref[...] = jnp.zeros(keep_ref.shape, F32)
    mine = iota((R, LANES), 0) == gz
    for d in range(3):
        keep_ref[d:d + 1, :] = jnp.sum(jnp.where(mine, own_total[d], 0.0), axis=0, keepdims=True)
    corrections = [[] for _ in range(ORDER)]
    moves = [[] for _ in range(3)]
    for tile in range(4):
        force = []
        for d in range(3):
            value = dense[gx, d, :, tile * LANES:(tile + 1) * LANES]
            row = jnp.sum(jnp.where(mine, value, 0.0), axis=0, keepdims=True)
            keep_ref[8 + 4 * d + tile:9 + 4 * d + tile, :] = row
            force.append(row)
        for j in range(ORDER):
            rows = [own_rows(size, place, [scaled_tiles[t][j][d] for t in range(3)], tile) for d in range(3)]
            corrections[j].append(force[0] * rows[0] + force[1] * rows[1] + force[2] * rows[2])
        for d in range(3):
            moves[d].append(own_rows(size, place, [total_tiles[t][d] for t in range(3)], tile))
    root = i_get(state_i, "root")
    slot = i_get(state_i, "slot")
    solved = f_get(state_f, "base1")
    for j in range(ORDER):
        at = gather_rows(corrections[j], root >> 7, root & 127)
        solved = solved - f_get(state_f, f"g{ORDER - 1 - j}") * at
    moved = [gather_rows(moves[d], slot >> 7, slot & 127) for d in range(3)]
    extra = jnp.max(i_get(state_i, "extra"))
    cidx = i_get(state_i, "cidx")

    def run(many):
        operator = local_from(state_f, state_i, extra, many)
        local = slot < 0
        stretch = []
        for d in range(3):
            force = operator.e[d] * solved
            change = f_get(state_f, "head_mass") * operator.at_head(force)
            other = jnp.where(local, operator.tail_mass * operator.at_tail(force), -moved[d])
            stretch.append(f_get(state_f, f"p{d}") - (change - other))
        length = f_get(state_f, "length")
        current = stretch[0] * stretch[0] + stretch[1] * stretch[1] + stretch[2] * stretch[2]
        target = jnp.sqrt(jnp.maximum(2.0 * length * length - current, 0.5 * length * length))
        terms = operator.powers(f_get(state_f, "scale") * (length - target))
        base = terms[0]
        for term in terms[1:]:
            base = base + term
        pair_ref[0:8, :] = solved
        pair_ref[8:16, :] = base
        rows = compact_rows(terms, cidx)
        for r, row in enumerate(rows):
            out_ref[0, r:r + 1, :] = row

    both_ways(extra, run)
    for d in range(1, out_ref.shape[0]):
        out_ref[d, :, :] = out_ref[0, :, :]


def final_kernel(size, table, state_f, state_i, got3, pair_ref, force_ref, matrix_ref, keep_ref, *refs):
    *got2, pos_ref, mult_ref, dense = refs
    X, Y, Z = size["mesh"]
    send = size["send"]
    R = Y * Z
    place = my_place()
    gx, gy, gz = place

    def load_row(kind, x, r):
        if kind == "mark":
            return plane(size, got2, x, size["map_row"] - 1, None)
        return map_row(size, got2, x, r) if kind == "map" else plane(size, [got3], x, r, 8)

    nk = ORDER + 1
    expand_dense(size, load_row, [(q, nk + q // 2, q % 2) for q in range(nk)], dense)
    scaled_tiles, own_total = [], None
    for t in range(3):
        target = lax.rem(gx + (t - 1 + X), X)
        sums = {}
        for tile in range(4):
            terms = [aligned(size, dense, i, target, tile) for i in range(nk)]
            for d in range(3):
                force = force_ref[t, d, :, tile * LANES:(tile + 1) * LANES]
                for k in range(nk):
                    sums.setdefault((k, d), []).append(force * terms[k])
        sums = lane_totals(sums, send)
        matrices = [[matrix_ref[t, 6 * k + s, :, :] for s in range(6)] for k in range(ORDER)]
        scaled, total, _ = recurrence(
            [[sums[k, d] for d in range(3)] for k in range(nk)], matrices, matrix_ref[t, 24, :, :])
        scaled_tiles.append(scaled)
        if t == 1:
            own_total = total
    mine = iota((R, LANES), 0) == gz
    corrections = [[] for _ in range(ORDER)]
    for tile in range(4):
        force = [keep_ref[8 + 4 * d + tile:9 + 4 * d + tile, :] for d in range(3)]
        for j in range(ORDER):
            rows = [own_rows(size, place, [scaled_tiles[t][j][d] for t in range(3)], tile) for d in range(3)]
            corrections[j].append(force[0] * rows[0] + force[1] * rows[1] + force[2] * rows[2])
    root = i_get(state_i, "root")
    solved = pair_ref[8:16, :]
    for j in range(ORDER):
        at = gather_rows(corrections[j], root >> 7, root & 127)
        solved = solved - f_get(state_f, f"g{ORDER - 1 - j}") * at
    both = pair_ref[0:8, :] + solved
    for r in range(8):
        mult_ref[0, 0, 0, pl.ds(r * LANES, LANES)] = both[r, :]
    extra = jnp.max(i_get(state_i, "extra"))

    def run(many):
        operator = local_from(state_f, state_i, extra, many)
        for d in range(3):
            force = operator.e[d] * both
            below = value_rows(operator.total(force))
            sent = keep_ref[d:d + 1, :] + jnp.sum(jnp.where(mine, own_total[d], 0.0), axis=0, keepdims=True)
            above = value_rows(force) + [-sent]
            for part, count in enumerate(size["atom_parts"]):
                hinv = i_get(state_i, f"hinv{part}")
                tinv = i_get(state_i, f"tinv{part}")
                change = gather_rows(above, hinv >> 7, hinv & 127) - gather_rows(below, tinv >> 7, tinv & 127)
                for r in range(count):
                    span = pl.ds((8 * part + r) * LANES, LANES)
                    at = 8 * part + r
                    pos_ref[d, 0, 0, 0, span] = (table[(3 + d) * size["atom_pad"] + at, :]
                                                 - table[6 * size["atom_pad"] + at, :] * change[r, :])

    both_ways(extra, run)


def share(message):
    return lax.all_to_all(message, AXES, split_axis=0, concat_axis=0, tiled=True)


def make_per_device(mesh):
    sizes = axis_sizes(mesh)
    X, Y, Z = sizes
    devices = X * Y * Z
    R = Y * Z

    def per_device(old_pos, displacement, inv_mass, bond_head, bond_tail, send_list):
        atoms = old_pos.shape[-1]
        bonds = bond_head.shape[-1]
        send = send_list.shape[-1]
        atom_rows = atoms // LANES
        assert atoms % LANES == 0 and bonds == 8 * LANES and LANES % send == 0 and atom_rows <= 16 and 3 * LANES < 27 * send <= 3 * LANES + LANES // 2 - 4
        rows2 = NQ + (NQ + 1) // 2 + 3
        assert NQ % 2 == 1
        part_rows = -(-rows2 // Y)

        def load_send(ref):
            one = ref[0, 0, 0:1, :]
            return jnp.concatenate([one] * (LANES // send), axis=1)

        size = dict(mesh=sizes, send=send, atom_rows=atom_rows, atom_pad=16, ext_rows=16, part_rows=part_rows,
                    map_row=NQ + (NQ + 1) // 2, load_send=load_send, start_lane=27 * send - 3 * LANES,
                    atom_parts=[min(8, atom_rows), max(atom_rows - 8, 0)])

        def call(kernel, outs, scratch, *args, space=pltpu.VMEM):
            def wrapped(*refs):
                kernel(size, *refs)

            return pl.pallas_call(
                wrapped, out_shape=outs, scratch_shapes=scratch,
                in_specs=[pl.BlockSpec(memory_space=space)] * len(args),
                out_specs=jax.tree.map(lambda _: pl.BlockSpec(memory_space=pltpu.VMEM), outs),
                compiler_params=pltpu.CompilerParams(vmem_limit_bytes=32 * 1024 * 1024),
            )(*[pltpu.with_memory_space_constraint(a, space) for a in args] if space == pltpu.HBM else args)

        S = jax.ShapeDtypeStruct
        one, table, cons = call(
            send_kernel, (S((devices, 1, LANES), F32), S((7 * 16, LANES), F32), S((24, LANES), I32)),
            [pltpu.VMEM(old_pos.shape, F32), pltpu.VMEM(old_pos.shape, F32), pltpu.VMEM(inv_mass.shape, F32),
             pltpu.VMEM(bond_head.shape, I32), pltpu.VMEM(bond_tail.shape, I32), pltpu.VMEM(send_list.shape, I32),
             pltpu.SemaphoreType.DMA((6,))],
            old_pos, displacement, inv_mass, bond_head, bond_tail, send_list, space=pltpu.HBM)
        got1 = share(one)
        state_i, number, head_at, tail_at = call(
            map_kernel,
            (S((8 * len(I_NAMES), LANES), I32), S((8, LANES), F32), S((56, LANES), F32), S((56, LANES), F32)),
            [pltpu.VMEM((16, LANES), I32)], table, cons)
        state_f, two = call(
            geometry_kernel,
            (S((8 * len(F_NAMES), LANES), F32), S((devices, part_rows, 1, LANES), F32)),
            [pltpu.VMEM((32, LANES), F32), pltpu.VMEM((32, LANES), F32)],
            state_i, number, head_at, tail_at, got1)
        got2 = share(two)
        got2 = [got2] + [lax.ppermute(got2, "gy", [((i + k) % Y, i) for i in range(Y)]) for k in range(1, Y)]
        got2 = [g.reshape(devices * part_rows, LANES) for g in got2]
        wide = 4 * LANES
        three, pair, force, matrix, keep = call(
            middle_kernel,
            (S((devices, 8, LANES), F32), S((16, LANES), F32), S((3, 3, R, wide), F32), S((3, 25, R, LANES), F32),
             S((24, LANES), F32)),
            [pltpu.VMEM((X, NQ, R, wide), F32)],
            state_f, state_i, got1.reshape(devices, LANES), *got2)
        got3 = share(three).reshape(devices * 8, LANES)
        return call(
            final_kernel,
            (S(old_pos.shape, F32), S(bond_head.shape, F32)),
            [pltpu.VMEM((X, ORDER + 1, R, wide), F32)],
            table, state_f, state_i, got3, pair, force, matrix, keep, *got2)

    return per_device


def solution(mesh):
    return jax.shard_map(
        make_per_device(mesh),
        mesh=mesh,
        in_specs=(
            P(None, "gx", "gy", "gz", None),
            P(None, "gx", "gy", "gz", None),
            P("gx", "gy", "gz", None),
            P("gx", "gy", "gz", None),
            P("gx", "gy", "gz", None),
            P("gx", "gy", "gz", None),
        ),
        out_specs=(P(None, "gx", "gy", "gz", None), P("gx", "gy", "gz", None)),
        check_vma=False,
    )
```

```python
import math

import jax
import jax.numpy as jnp
from jax import lax
from jax.experimental import pallas as pl
from jax.experimental.pallas import tpu as pltpu
from jax.sharding import PartitionSpec as P

ORDER = 4
HALO = 192
LANES = 128
NQ = 11
AXES = ("gx", "gy", "gz")
OFFSETS = [(b // 9 - 1, b // 3 % 3 - 1, b % 3 - 1) for b in range(27)]
F32 = jnp.float32
I32 = jnp.int32
SYM = [(0, 0), (1, 1), (2, 2), (0, 1), (0, 2), (1, 2)]


def iota(shape, dim):
    return lax.broadcasted_iota(I32, shape, dim)


def pick(table, index):
    return jnp.take_along_axis(table, index, axis=1, mode="promise_in_bounds")


def pick_row(table, index):
    return jnp.take_along_axis(table, index, axis=0, mode="promise_in_bounds")


def spread_row(row, like):
    return jnp.broadcast_to(row, like.shape)


def gather_rows(rows, high, low, base=0):
    result = jnp.zeros(high.shape, rows[0].dtype)
    for r, row in enumerate(rows):
        result = jnp.where(high == base + r, pick(spread_row(row, high), low), result)
    return result


def value_rows(value):
    return [value[r:r + 1, :] for r in range(value.shape[0])]


def gather_value(value, index):
    return gather_rows(value_rows(value), index >> 7, index & 127)


def load_flat(ref, lead, scratch, base, count):
    for r in range(count):
        scratch[base + r:base + r + 1, :] = ref[(*lead, pl.ds(r * LANES, LANES))].reshape(1, LANES)


def axis_sizes(mesh):
    return tuple(mesh.shape[a] for a in AXES)


def my_place():
    return tuple(lax.axis_index(a) for a in AXES)


def one_hot_scatter(values, index, high_rows):
    parts = []
    spots = []
    for r in range(index.shape[0]):
        high = index[r:r + 1, :] >> 7
        low = index[r:r + 1, :] & 127
        hit = jnp.broadcast_to(high, (high_rows, LANES)) == iota((high_rows, LANES), 0)
        parts.append(jnp.concatenate(
            [jnp.where(hit, jnp.broadcast_to(v[r:r + 1, :], (high_rows, LANES)), 0.0) for v in values],
            axis=0).astype(jnp.bfloat16))
        spots.append(jnp.where(
            jnp.broadcast_to(low, (LANES, LANES)) == iota((LANES, LANES), 0), 1.0, 0.0).astype(jnp.bfloat16))
    left = jnp.concatenate(parts, axis=1)
    right = jnp.concatenate(spots, axis=1)
    table = lax.dot_general(left, right, (((1,), (1,)), ((), ())), preferred_element_type=F32)
    return [table[i * high_rows:(i + 1) * high_rows] for i in range(len(values))]


def inverse_tables(index, valid, high_rows):
    where_from = iota(index.shape, 0) * LANES + iota(index.shape, 1)
    spot = jnp.where(valid, index, -1)
    ones = jnp.ones(index.shape, F32)
    upper, lower, count = one_hot_scatter(
        [(where_from >> 5).astype(F32), (where_from & 31).astype(F32), ones], spot, high_rows)
    table = (upper * 32.0 + lower).astype(I32)
    return jnp.where(count > 0.5, table, -1), count


def send_kernel(size, old_hbm, move_hbm, mass_hbm, head_hbm, tail_hbm, send_hbm, out_ref, table, cons,
                old_ref, move_ref, mass_ref, head_ref, tail_ref, send_ref, sems, out_vmem, out_sem):
    atom_rows = size["atom_rows"]
    send = size["send"]
    pad_rows = size["atom_pad"]
    copies = [pltpu.make_async_copy(src, dst, sems.at[i]) for i, (src, dst) in enumerate(
        [(old_hbm, old_ref), (move_hbm, move_ref), (mass_hbm, mass_ref), (send_hbm, send_ref), (head_hbm, head_ref),
         (tail_hbm, tail_ref)])]
    for copy in copies:
        copy.start()
    for copy in copies[:4]:
        copy.wait()
    table[...] = jnp.zeros(table.shape, F32)
    for r in range(atom_rows):
        span = pl.ds(r * LANES, LANES)
        for d in range(3):
            old = old_ref[d, 0, 0, 0, span].reshape(1, LANES)
            a, b = d * pad_rows + r, (3 + d) * pad_rows + r
            table[a:a + 1, :] = old
            table[b:b + 1, :] = old + move_ref[d, 0, 0, 0, span].reshape(1, LANES)
    load_flat(mass_ref, (0, 0, 0), table, 6 * pad_rows, atom_rows)
    lane = iota((pad_rows, LANES), 1)
    send_row = size["load_send"](send_ref)
    index = jnp.broadcast_to(send_row, (pad_rows, LANES))
    low = index & 127
    hit = (index >> 7) == iota((pad_rows, LANES), 0)
    message = jnp.zeros((1, LANES), F32)
    for q in range(7):
        got = jnp.where(hit, pick(table[q * pad_rows:(q + 1) * pad_rows, :], low), 0.0)
        row = jnp.sum(got, axis=0, keepdims=True)
        message = jnp.where(lane[0:1] // send == q, row, message)
    for d in range(out_ref.shape[0]):
        out_vmem[d, :, :] = message
    leaving = pltpu.make_async_copy(out_vmem, out_ref, out_sem)
    leaving.start()
    for copy in copies[4:]:
        copy.wait()
    load_flat(head_ref, (0, 0, 0), cons, 0, 8)
    load_flat(tail_ref, (0, 0, 0), cons, 8, 8)
    cons[16:24, :] = jnp.broadcast_to(send_row, (8, LANES))
    leaving.wait()


def chain_sum(value, prev, extra):
    def body(_, carry):
        total, current = carry
        current = gather_value(current, prev)
        return total + current, current

    return lax.fori_loop(0, extra, body, (value, value))[0]


class Local:
    def __init__(self, direction, diag, kappa, tail_mass, following, child, prev, last, extra, many):
        self.e, self.diag, self.kappa, self.tail_mass = direction, diag, kappa, tail_mass
        self.following, self.child, self.prev, self.last = following, child, prev, last
        self.extra, self.many = extra, many
        self.child_kappa = None if many else gather_value(kappa, child)

    def total(self, value):
        return chain_sum(value, self.prev, self.extra) if self.many else value

    def apply(self, value):
        result = self.diag * value + self.kappa * gather_value(value, self.following)
        if not self.many:
            return result + self.child_kappa * gather_value(value, self.child)
        result = result + gather_value(self.total(self.kappa * value), self.child)
        if self.many:
            for d in range(3):
                force = self.e[d] * value
                others = gather_value(self.total(force), self.last) - force
                result = result - jnp.where(self.last >= 0, self.tail_mass * self.e[d] * others, 0.0)
        return result

    def powers(self, value):
        terms = [value]
        if self.many or ORDER != 4:
            for _ in range(ORDER):
                terms.append(self.apply(terms[-1]))
            return terms
        n, c, k, d, kc = self.following, self.child, self.kappa, self.diag, self.child_kappa
        n2 = gather_value(n + 1, n) - 1
        c2 = gather_value(c + 1, c) - 1
        far_n = k * gather_value(k, n)
        far_c = kc * gather_value(kc, c)
        near_n = k * (d + gather_value(d, n))
        near_c = kc * (d + gather_value(d, c))
        own = d * d + k * k + kc * kc

        def twice(u, u_n, u_c):
            return (own * u + near_n * u_n + near_c * u_c) + (
                far_n * gather_value(u, n2) + far_c * gather_value(u, c2))

        u_n, u_c = gather_value(value, n), gather_value(value, c)
        one = d * value + k * u_n + kc * u_c
        two = twice(value, u_n, u_c)
        three = twice(one, gather_value(one, n), gather_value(one, c))
        four = twice(two, gather_value(two, n), gather_value(two, c))
        return [value, one, two, three, four]

    def at_head(self, force):
        return force - gather_value(self.total(force), self.child)

    def at_tail(self, force):
        below = gather_value(self.total(force), self.last) if self.many else force
        return gather_value(force, self.following) - below


def both_ways(extra, run):
    @pl.when(extra == 0)
    def _():
        run(False)

    @pl.when(extra > 0)
    def _():
        run(True)


F_NAMES = ["e0", "e1", "e2", "p0", "p1", "p2", "length", "scale", "head_mass", "tail_mass", "diag", "kappa",
           "base1", "g0", "g1", "g2", "g3"]
I_NAMES = ["following", "child", "prev", "last", "root", "slot", "cidx", "extra", "tinv0", "tinv1", "hinv0", "hinv1"]


def f_get(ref, name):
    i = F_NAMES.index(name)
    return ref[8 * i:8 * i + 8, :]


def i_get(ref, name):
    i = I_NAMES.index(name)
    return ref[8 * i:8 * i + 8, :]


def f_put(ref, name, value):
    i = F_NAMES.index(name)
    ref[8 * i:8 * i + 8, :] = value


def i_put(ref, name, value):
    i = I_NAMES.index(name)
    ref[8 * i:8 * i + 8, :] = value


def local_from(state_f, state_i, extra, many):
    return Local([f_get(state_f, f"e{d}") for d in range(3)], f_get(state_f, "diag"), f_get(state_f, "kappa"),
                 f_get(state_f, "tail_mass"), i_get(state_i, "following"), i_get(state_i, "child"),
                 i_get(state_i, "prev"), i_get(state_i, "last"), extra, many)


def compact_rows(values, cidx):
    high = cidx >> 7
    low = cidx & 127
    lane = iota((1, LANES), 1)
    firsts, rests = [], []
    for i, value in enumerate(values):
        got = gather_rows(value_rows(value), high, low)
        firsts.append(got[2:3] if i % 2 else got[0:1])
        rests.append(got[1:2])
    rows = list(firsts)
    for i in range(0, len(rests), 2):
        other = rests[i + 1] if i + 1 < len(rests) else rests[i]
        rows.append(jnp.where(lane < 64, rests[i], other))
    return rows


def map_kernel(size, table, cons, state_i, number_ref, head_ref, tail_ref, work):
    atom_rows, pad_rows = size["atom_rows"], size["atom_pad"]
    send = size["send"]
    atoms = atom_rows * LANES
    shape = (8, LANES)
    here = iota(shape, 0) * LANES + iota(shape, 1)
    head = cons[0:8, :]
    tail = cons[8:16, :]
    local = tail < atoms

    ext_rows = size["ext_rows"]
    tinv, count = inverse_tables(tail, tail >= 0, ext_rows)
    hinv, _ = inverse_tables(head, head >= 0, pad_rows)
    most = jnp.max(jnp.where(iota(count.shape, 0) < atom_rows, count, 0.0))
    extra = jnp.maximum(most.astype(I32) - 1, 0)
    send_row = cons[16:17, :]
    atom_id = iota((pad_rows, LANES), 0) * LANES + iota((pad_rows, LANES), 1)
    for e in range(send):
        which = jnp.broadcast_to(send_row[:, e:e + 1], (pad_rows, LANES))
        hinv = jnp.where(atom_id == which, 8 * LANES + e, hinv)
    work[0:ext_rows, :] = tinv
    i_put(state_i, "prev", jnp.full(shape, -1, I32))
    i_put(state_i, "last", jnp.where(local, here, -1))

    @pl.when(extra > 0)
    def _():
        def body(c, carry):
            prev, last, inv = carry
            mark = jnp.max(jnp.where(here == c, tail, -1))
            same = tail == mark
            prev = jnp.where(same & (here > c), c, prev)
            last = jnp.where(same & local, c, last)
            spots = iota(inv.shape, 0) * LANES + iota(inv.shape, 1)
            inv = jnp.where(spots == mark, c, inv)
            return prev, last, inv

        prev, last, inv = lax.fori_loop(
            0, 8 * LANES, body, (jnp.full(shape, -1, I32), jnp.full(shape, -1, I32), tinv))
        i_put(state_i, "prev", prev)
        i_put(state_i, "last", last)
        work[0:ext_rows, :] = inv

    tinv = work[0:ext_rows, :]
    tail_high, tail_low = tail >> 7, tail & 127
    head_high, head_low = head >> 7, head & 127
    hinv_rows = value_rows(hinv)[:atom_rows]
    following = gather_rows(hinv_rows, tail_high, tail_low)
    following = jnp.where(local, following, -1)
    following = jnp.where(following < 8 * LANES, following, -1)
    child = gather_rows(value_rows(tinv)[:atom_rows], head_high, head_low)
    root = jnp.where(local, -1, tail - atoms)
    slot = root
    for _ in range(3):
        ahead = gather_value(root + 1, following) - 1
        root = jnp.where(root < 0, ahead, root)
    slots = tinv[atom_rows:atom_rows + 4]
    used = slots >= 0
    used_f = jnp.where(used, 1.0, 0.0)
    before = lax.dot_general(
        jnp.concatenate([used_f, jnp.zeros((4, LANES), F32)], axis=0).astype(jnp.bfloat16),
        jnp.where(iota((LANES, LANES), 0) < iota((LANES, LANES), 1), 1.0, 0.0).astype(jnp.bfloat16),
        (((1,), (0,)), ((), ())), preferred_element_type=F32)
    rank_rows = []
    starts = []
    offset = jnp.zeros((1, 1), F32)
    for r in range(4):
        rank_rows.append(before[r:r + 1] + offset)
        starts.append(offset)
        offset = offset + jnp.sum(used_f[r:r + 1], axis=1, keepdims=True)
    rank = jnp.concatenate(rank_rows, axis=0)
    number = jnp.where(used, rank, -1.0)
    place = number.astype(I32)
    index4 = jnp.concatenate([place, jnp.where(place >= LANES, place + 64, -1)], axis=0)
    from8 = jnp.concatenate([slots, slots], axis=0)
    upper, lower = one_hot_scatter([(from8 >> 5).astype(F32), (from8 & 31).astype(F32)], index4, 8)
    cidx = (upper * 32.0 + lower).astype(I32)
    turned = pltpu.roll(cidx, LANES // 2, 1)
    cidx = jnp.where(iota(shape, 0) == 2, jnp.broadcast_to(turned[0:1, :], shape), cidx)

    marks = number[3:4, :]
    for r in range(4):
        marks = jnp.where(iota((1, LANES), 1) == size["start_lane"] + r, -2.0 - starts[r], marks)
    marks = pltpu.roll(jnp.broadcast_to(marks, shape), LANES // 2, 1)[0:1, :]
    number = jnp.concatenate([number[0:3, :], marks], axis=0)
    number_ref[0:4, :] = number
    number_ref[4:8, :] = number
    i_put(state_i, "following", following)
    i_put(state_i, "child", child)
    i_put(state_i, "root", root)
    i_put(state_i, "slot", slot)
    i_put(state_i, "cidx", cidx)
    i_put(state_i, "extra", jnp.broadcast_to(extra, shape))
    i_put(state_i, "tinv0", tinv[0:8])
    i_put(state_i, "tinv1", tinv[8:16])
    i_put(state_i, "hinv0", hinv[0:8])
    i_put(state_i, "hinv1", hinv[8:16])

    def rows_of(q):
        return [table[q * pad_rows + r:q * pad_rows + r + 1, :] for r in range(atom_rows)]

    for q in range(7):
        head_ref[8 * q:8 * q + 8, :] = gather_rows(rows_of(q), head_high, head_low)
        tail_ref[8 * q:8 * q + 8, :] = gather_rows(rows_of(q), tail_high, tail_low)


def geometry_kernel(size, state_i, number_ref, head_ref, tail_ref, got_ref, state_f, out_ref, remote, rtab):
    X, Y, Z = size["mesh"]
    send = size["send"]
    shape = (8, LANES)
    slot = i_get(state_i, "slot")
    local = slot < 0
    following = i_get(state_i, "following")
    cidx = i_get(state_i, "cidx")
    extra = jnp.max(i_get(state_i, "extra"))
    gx, gy, gz = my_place()
    for b, (dx, dy, dz) in enumerate(OFFSETS):
        at = (lax.rem(gx + (dx + X), X) * Y + lax.rem(gy + (dy + Y), Y)) * Z + lax.rem(gz + (dz + Z), Z)
        remote[b:b + 1, :] = got_ref[at, :, :]
    lane = iota(shape, 1)
    for j in range(4):
        block = remote[8 * j:8 * j + 8, :]
        for q in range(7):
            row = pick_row(pick(block, q * send + lane % send), lane // send % 8)[0:1]
            rtab[4 * q + j:4 * q + j + 1, :] = row
    slot_high, slot_low = slot >> 7, slot & 127
    head_at = [head_ref[8 * q:8 * q + 8, :] for q in range(7)]
    tail_at = []
    for q in range(7):
        afar = gather_rows([rtab[4 * q + j:4 * q + j + 1, :] for j in range(4)], slot_high, slot_low)
        tail_at.append(jnp.where(local, tail_ref[8 * q:8 * q + 8, :], afar))
    bond = [head_at[d] - tail_at[d] for d in range(3)]
    gap = [head_at[3 + d] - tail_at[3 + d] for d in range(3)]
    length = jnp.maximum(jnp.sqrt(bond[0] * bond[0] + bond[1] * bond[1] + bond[2] * bond[2]), 0.5)
    direction = [bond[d] / length for d in range(3)]
    scale = 1.0 / jnp.sqrt(head_at[6] + tail_at[6])
    force = [scale * direction[d] for d in range(3)]
    head_mass = head_at[6]
    tail_mass = jnp.where(local, tail_at[6], 0.0)
    norm = force[0] * force[0] + force[1] * force[1] + force[2] * force[2]
    diag = 1.0 - norm * (head_mass + tail_mass)
    ahead = [gather_value(force[d], following) for d in range(3)]
    kappa = tail_mass * (force[0] * ahead[0] + force[1] * ahead[1] + force[2] * ahead[2])
    right = scale * ((direction[0] * gap[0] + direction[1] * gap[1] + direction[2] * gap[2]) - length)
    for d in range(3):
        f_put(state_f, f"e{d}", force[d])
        f_put(state_f, f"p{d}", gap[d])
    f_put(state_f, "length", length)
    f_put(state_f, "scale", scale)
    f_put(state_f, "head_mass", head_mass)
    f_put(state_f, "tail_mass", tail_mass)
    f_put(state_f, "diag", diag)
    f_put(state_f, "kappa", kappa)
    def run(many):
        operator = local_from(state_f, state_i, extra, many)
        terms = [right]
        unit = [jnp.where(local, 0.0, 1.0)]
        for k in range(ORDER):
            terms.append(operator.apply(terms[-1]))
            if k < ORDER - 1:
                unit.append(operator.apply(unit[-1]))
        base = terms[0]
        for term in terms[1:]:
            base = base + term
        f_put(state_f, "base1", base)
        summed = unit[0]
        f_put(state_f, "g0", summed)
        for k in range(1, ORDER):
            summed = summed + unit[k]
            f_put(state_f, f"g{k}", summed)
        rows = compact_rows(force + unit[1:] + terms, cidx)
        rows[-1] = jnp.where(iota((1, LANES), 1) < LANES // 2, rows[-1], number_ref[3:4, :])
        rows = rows + value_rows(number_ref[0:3, :])
        part_rows = size["part_rows"]
        rows = rows + [rows[-1]] * (Y * part_rows - len(rows))
        for k in range(Y):
            row_y = lax.rem(lax.axis_index("gy") + k, Y)
            for r in range(0, part_rows, 8):
                some = rows[k * part_rows + r:k * part_rows + min(r + 8, part_rows)]
                block = jnp.concatenate(some, axis=0)
                for x in range(X):
                    for z in range(Z):
                        out_ref[(x * Y + row_y) * Z + z, r:r + len(some), 0, :] = block

    both_ways(extra, run)


def lane_fields(tile):
    lane = iota((1, LANES), 1)
    return lane


def block_masks(tile, send, rows):
    per = LANES // send
    block = iota((rows, LANES), 1) // send + per * tile
    return block // 9 - 1, block // 3 % 3 - 1, block % 3 - 1, [b for b in range(per * tile, per * tile + per)]


def choose(options, field, values):
    result = options[values[0]]
    for v in values[1:]:
        result = jnp.where(field == v, options[v], result)
    return result


def expand_dense(size, load_row, slots, dense):
    X, Y, Z = size["mesh"]
    R = Y * Z
    lane = iota((R, LANES), 1)
    for x in range(X):
        last = load_row("map", x, 3)
        marks = load_row("mark", x, 0)
        rows = {r: load_row("q", x, r) for r in sorted({r for slot in slots for r in slot[:2]})}
        for l in range(4):
            number = load_row("map", x, l) if l < 3 else last
            start = -2 - pick(marks, jnp.full((R, LANES), LANES // 2 + size["start_lane"] + l, I32)).astype(I32)
            low = number & 127
            keep = [lane >= start, (lane < LANES // 2) | (lane - LANES // 2 >= start)]
            for i, (first, rest, half) in enumerate(slots):
                row = jnp.where(keep[half], rows[first], rows[rest])
                value = pick(row, low ^ (half * (LANES // 2)))
                dense[x, i, :, l * LANES:(l + 1) * LANES] = jnp.where(number < 0, 0.0, value)


def aligned(size, dense, q, target, tile):
    X, Y, Z = size["mesh"]
    send = size["send"]
    R = Y * Z
    dx, dy, dz, blocks = block_masks(tile, send, R)
    blocks = [b for b in blocks if b < 27]
    span = pl.ds(tile * LANES, LANES)
    offs = [sorted({OFFSETS[b][k] for b in blocks}) for k in range(3)]
    value = choose({o: dense[lax.rem(target + (X - o), X), q, :, span] for o in offs[0]}, dx, offs[0])
    row_z = iota((R, LANES), 0) % Z
    if R == 8:
        row_y = iota((R, LANES), 0) // Z
        source = lax.rem(row_y - dy + Y, Y) * Z + lax.rem(row_z - dz + Z, Z)
        return pick_row(value, source)
    options = {0: value}
    if 1 in offs[2]:
        options[1] = jnp.where(row_z == 0, turn(value, Z - 1, R), turn(value, -1, R))
    if -1 in offs[2]:
        options[-1] = jnp.where(row_z == Z - 1, turn(value, -(Z - 1), R), turn(value, 1, R))
    value = choose(options, dz, offs[2])
    value = choose({o: turn(value, -o * Z, R) for o in offs[1]}, dy, offs[1])
    return value


def turn(value, by, rows):
    shift = (-by) % rows
    return value if shift == 0 else pltpu.roll(value, shift, 0)


def lane_totals(sums, send):
    stack = jnp.concatenate([parts[0] + parts[1] + parts[2] + parts[3] for parts in sums.values()], axis=0)
    pieces = []
    for _ in range(2):
        piece = stack.astype(jnp.bfloat16)
        pieces.append(piece)
        stack = stack - piece.astype(F32)
    same = iota((2 * LANES, LANES), 0) % send == iota((2 * LANES, LANES), 1) % send
    table = jnp.dot(jnp.concatenate(pieces, axis=1), jnp.where(same, 1.0, 0.0).astype(jnp.bfloat16),
                    preferred_element_type=F32)
    rows = table.shape[0] // len(sums)
    return {key: table[i * rows:(i + 1) * rows] for i, key in enumerate(sums)}


def times(matrix, vector):
    full = {}
    for i, (a, b) in enumerate(SYM):
        full[a, b] = full[b, a] = matrix[i]
    return [full[a, 0] * vector[0] + full[a, 1] * vector[1] + full[a, 2] * vector[2] for a in range(3)]


def recurrence(first, matrices, mass):
    sums, scaled = [], []
    for k in range(ORDER + 1):
        value = first[k]
        for j in range(k):
            back = times(matrices[k - 1 - j], scaled[j])
            value = [value[d] - back[d] for d in range(3)]
        sums.append(value)
        scaled.append([mass * value[d] for d in range(3)])
    total = sums[0]
    for value in sums[1:]:
        total = [total[d] + value[d] for d in range(3)]
    return scaled, total, [mass * total[d] for d in range(3)]


def own_rows(size, place, tiles, tile):
    X, Y, Z = size["mesh"]
    R = Y * Z
    gx, gy, gz = place
    dx, dy, dz, blocks = block_masks(tile, size["send"], R)
    blocks = [b for b in blocks if b < 27]
    wanted = lax.rem(dy + Y, Y) * Z + lax.rem(gz + dz + Z, Z)
    offs = sorted({OFFSETS[b][0] for b in blocks})
    value = choose({o: tiles[o + 1] for o in offs}, dx, offs)
    if R == 8:
        return pick_row(value, wanted)[0:1]
    return jnp.sum(jnp.where(wanted == iota((R, LANES), 0), value, 0.0), axis=0, keepdims=True)


def strided(ref, first, rows, stride):
    if rows <= 8:
        return ref[pl.ds(first, rows, stride=stride), :]
    return jnp.concatenate(
        [ref[pl.ds(first + 8 * i * stride, 8, stride=stride), :] for i in range(rows // 8)], axis=0)


def plane(size, refs, x, row, stride):
    Y, Z = size["mesh"][1:]
    gy = lax.axis_index("gy")
    pieces = []
    for k in range(Y):
        first = (x * Y + lax.rem(gy + k, Y)) * Z
        if stride is None:
            part_rows = size["part_rows"]
            ref = refs[(row // part_rows + k) % Y]
            pieces.append(strided(ref, first * part_rows + row % part_rows, Z, part_rows))
        else:
            pieces.append(strided(refs[0], first * stride + row, Z, stride))
    return jnp.concatenate(pieces, axis=0)


def map_row(size, refs, x, tile):
    if tile < 3:
        return plane(size, refs, x, size["map_row"] + tile, None).astype(I32)
    row = plane(size, refs, x, size["map_row"] - 1, None)
    lane = iota(row.shape, 1)
    return jnp.where(lane < LANES // 2, pick(row, lane ^ (LANES // 2)), -1.0).astype(I32)


def middle_kernel(size, state_f, state_i, got1, *refs):
    *got2, out_ref, pair_ref, force_ref, matrix_ref, keep_ref, dense = refs
    X, Y, Z = size["mesh"]
    send = size["send"]
    R = Y * Z
    place = my_place()
    gx, gy, gz = place

    def load_row(kind, x, r):
        if kind == "mark":
            return plane(size, got2, x, size["map_row"] - 1, None)
        return map_row(size, got2, x, r) if kind == "map" else plane(size, got2, x, r, None)

    expand_dense(size, load_row, [(q, NQ + q // 2, q % 2) for q in range(NQ)], dense)
    scaled_tiles, total_tiles, own_total = [], [], None
    for t in range(3):
        target = lax.rem(gx + (t - 1 + X), X)
        sums = {}
        for tile in range(4):
            q = [aligned(size, dense, i, target, tile) for i in range(NQ)]
            force, unit, terms = q[0:3], q[3:6], q[6:11]
            for d in range(3):
                force_ref[t, d, :, tile * LANES:(tile + 1) * LANES] = force[d]
                for k in range(ORDER + 1):
                    sums.setdefault(("v", k, d), []).append(force[d] * terms[k])
            for s, (a, b) in enumerate(SYM):
                square = force[a] * force[b]
                sums.setdefault(("b", 0, s), []).append(square)
                for k in range(3):
                    sums.setdefault(("b", k + 1, s), []).append(square * unit[k])
        sums = lane_totals(sums, send)
        mass = pick(plane(size, [got1], target, 0, 1), 6 * send + iota((R, LANES), 1) % send)
        matrices = [[sums["b", k, s] for s in range(6)] for k in range(ORDER)]
        for k in range(ORDER):
            for s in range(6):
                matrix_ref[t, 6 * k + s, :, :] = matrices[k][s]
        matrix_ref[t, 24, :, :] = mass
        scaled, total, full = recurrence(
            [[sums["v", k, d] for d in range(3)] for k in range(ORDER + 1)], matrices, mass)
        scaled_tiles.append(scaled)
        total_tiles.append(full)
        if t == 1:
            own_total = total
    keep_ref[...] = jnp.zeros(keep_ref.shape, F32)
    mine = iota((R, LANES), 0) == gz
    for d in range(3):
        keep_ref[d:d + 1, :] = jnp.sum(jnp.where(mine, own_total[d], 0.0), axis=0, keepdims=True)
    corrections = [[] for _ in range(ORDER)]
    moves = [[] for _ in range(3)]
    for tile in range(4):
        force = []
        for d in range(3):
            value = dense[gx, d, :, tile * LANES:(tile + 1) * LANES]
            row = jnp.sum(jnp.where(mine, value, 0.0), axis=0, keepdims=True)
            keep_ref[8 + 4 * d + tile:9 + 4 * d + tile, :] = row
            force.append(row)
        for j in range(ORDER):
            rows = [own_rows(size, place, [scaled_tiles[t][j][d] for t in range(3)], tile) for d in range(3)]
            corrections[j].append(force[0] * rows[0] + force[1] * rows[1] + force[2] * rows[2])
        for d in range(3):
            moves[d].append(own_rows(size, place, [total_tiles[t][d] for t in range(3)], tile))
    root = i_get(state_i, "root")
    slot = i_get(state_i, "slot")
    solved = f_get(state_f, "base1")
    for j in range(ORDER):
        at = gather_rows(corrections[j], root >> 7, root & 127)
        solved = solved - f_get(state_f, f"g{ORDER - 1 - j}") * at
    moved = [gather_rows(moves[d], slot >> 7, slot & 127) for d in range(3)]
    extra = jnp.max(i_get(state_i, "extra"))
    cidx = i_get(state_i, "cidx")

    def run(many):
        operator = local_from(state_f, state_i, extra, many)
        local = slot < 0
        stretch = []
        for d in range(3):
            force = operator.e[d] * solved
            change = f_get(state_f, "head_mass") * operator.at_head(force)
            other = jnp.where(local, operator.tail_mass * operator.at_tail(force), -moved[d])
            stretch.append(f_get(state_f, f"p{d}") - (change - other))
        length = f_get(state_f, "length")
        current = stretch[0] * stretch[0] + stretch[1] * stretch[1] + stretch[2] * stretch[2]
        target = jnp.sqrt(jnp.maximum(2.0 * length * length - current, 0.5 * length * length))
        terms = operator.powers(f_get(state_f, "scale") * (length - target))
        base = terms[0]
        for term in terms[1:]:
            base = base + term
        pair_ref[0:8, :] = solved
        pair_ref[8:16, :] = base
        rows = compact_rows(terms, cidx)
        for r, row in enumerate(rows):
            out_ref[0, r:r + 1, :] = row

    both_ways(extra, run)
    for d in range(1, out_ref.shape[0]):
        out_ref[d, :, :] = out_ref[0, :, :]


def final_kernel(size, table, state_f, state_i, got3, pair_ref, force_ref, matrix_ref, keep_ref, *refs):
    *got2, pos_ref, mult_ref, dense = refs
    X, Y, Z = size["mesh"]
    send = size["send"]
    R = Y * Z
    place = my_place()
    gx, gy, gz = place

    def load_row(kind, x, r):
        if kind == "mark":
            return plane(size, got2, x, size["map_row"] - 1, None)
        return map_row(size, got2, x, r) if kind == "map" else plane(size, [got3], x, r, 8)

    nk = ORDER + 1
    expand_dense(size, load_row, [(q, nk + q // 2, q % 2) for q in range(nk)], dense)
    scaled_tiles, own_total = [], None
    for t in range(3):
        target = lax.rem(gx + (t - 1 + X), X)
        sums = {}
        for tile in range(4):
            terms = [aligned(size, dense, i, target, tile) for i in range(nk)]
            for d in range(3):
                force = force_ref[t, d, :, tile * LANES:(tile + 1) * LANES]
                for k in range(nk):
                    sums.setdefault((k, d), []).append(force * terms[k])
        sums = lane_totals(sums, send)
        matrices = [[matrix_ref[t, 6 * k + s, :, :] for s in range(6)] for k in range(ORDER)]
        scaled, total, _ = recurrence(
            [[sums[k, d] for d in range(3)] for k in range(nk)], matrices, matrix_ref[t, 24, :, :])
        scaled_tiles.append(scaled)
        if t == 1:
            own_total = total
    mine = iota((R, LANES), 0) == gz
    corrections = [[] for _ in range(ORDER)]
    for tile in range(4):
        force = [keep_ref[8 + 4 * d + tile:9 + 4 * d + tile, :] for d in range(3)]
        for j in range(ORDER):
            rows = [own_rows(size, place, [scaled_tiles[t][j][d] for t in range(3)], tile) for d in range(3)]
            corrections[j].append(force[0] * rows[0] + force[1] * rows[1] + force[2] * rows[2])
    root = i_get(state_i, "root")
    solved = pair_ref[8:16, :]
    for j in range(ORDER):
        at = gather_rows(corrections[j], root >> 7, root & 127)
        solved = solved - f_get(state_f, f"g{ORDER - 1 - j}") * at
    both = pair_ref[0:8, :] + solved
    for r in range(8):
        mult_ref[0, 0, 0, pl.ds(r * LANES, LANES)] = both[r, :]
    extra = jnp.max(i_get(state_i, "extra"))

    def run(many):
        operator = local_from(state_f, state_i, extra, many)
        for d in range(3):
            force = operator.e[d] * both
            below = value_rows(operator.total(force))
            sent = keep_ref[d:d + 1, :] + jnp.sum(jnp.where(mine, own_total[d], 0.0), axis=0, keepdims=True)
            above = value_rows(force) + [-sent]
            for part, count in enumerate(size["atom_parts"]):
                hinv = i_get(state_i, f"hinv{part}")
                tinv = i_get(state_i, f"tinv{part}")
                change = gather_rows(above, hinv >> 7, hinv & 127) - gather_rows(below, tinv >> 7, tinv & 127)
                for r in range(count):
                    span = pl.ds((8 * part + r) * LANES, LANES)
                    at = 8 * part + r
                    pos_ref[d, 0, 0, 0, span] = (table[(3 + d) * size["atom_pad"] + at, :]
                                                 - table[6 * size["atom_pad"] + at, :] * change[r, :])

    both_ways(extra, run)


def share(message):
    return lax.all_to_all(message, AXES, split_axis=0, concat_axis=0, tiled=True)


def make_per_device(mesh):
    sizes = axis_sizes(mesh)
    X, Y, Z = sizes
    devices = X * Y * Z
    R = Y * Z

    def per_device(old_pos, displacement, inv_mass, bond_head, bond_tail, send_list):
        atoms = old_pos.shape[-1]
        bonds = bond_head.shape[-1]
        send = send_list.shape[-1]
        atom_rows = atoms // LANES
        assert atoms % LANES == 0 and bonds == 8 * LANES and LANES % send == 0 and atom_rows <= 16 and 3 * LANES < 27 * send <= 3 * LANES + LANES // 2 - 4
        rows2 = NQ + (NQ + 1) // 2 + 3
        assert NQ % 2 == 1
        part_rows = -(-rows2 // Y)

        def load_send(ref):
            one = ref[0, 0, 0:1, :]
            return jnp.concatenate([one] * (LANES // send), axis=1)

        size = dict(mesh=sizes, send=send, atom_rows=atom_rows, atom_pad=16, ext_rows=16, part_rows=part_rows,
                    map_row=NQ + (NQ + 1) // 2, load_send=load_send, start_lane=27 * send - 3 * LANES,
                    atom_parts=[min(8, atom_rows), max(atom_rows - 8, 0)])

        def call(kernel, outs, scratch, *args, space=pltpu.VMEM, first_out=pltpu.VMEM):
            first = jax.tree.leaves(outs)[0]

            def wrapped(*refs):
                kernel(size, *refs)

            return pl.pallas_call(
                wrapped, out_shape=outs, scratch_shapes=scratch,
                in_specs=[pl.BlockSpec(memory_space=space)] * len(args),
                out_specs=jax.tree.map(
                    lambda o: pl.BlockSpec(memory_space=first_out if o is first else pltpu.VMEM), outs),
                compiler_params=pltpu.CompilerParams(vmem_limit_bytes=32 * 1024 * 1024),
            )(*[pltpu.with_memory_space_constraint(a, space) for a in args] if space == pltpu.HBM else args)

        S = jax.ShapeDtypeStruct
        one, table, cons = call(
            send_kernel, (S((devices, 1, LANES), F32), S((7 * 16, LANES), F32), S((24, LANES), I32)),
            [pltpu.VMEM(old_pos.shape, F32), pltpu.VMEM(old_pos.shape, F32), pltpu.VMEM(inv_mass.shape, F32),
             pltpu.VMEM(bond_head.shape, I32), pltpu.VMEM(bond_tail.shape, I32), pltpu.VMEM(send_list.shape, I32),
             pltpu.SemaphoreType.DMA((6,)), pltpu.VMEM((devices, 1, LANES), F32), pltpu.SemaphoreType.DMA],
            old_pos, displacement, inv_mass, bond_head, bond_tail, send_list, space=pltpu.HBM,
            first_out=pltpu.HBM)
        got1 = share(one)
        state_i, number, head_at, tail_at = call(
            map_kernel,
            (S((8 * len(I_NAMES), LANES), I32), S((8, LANES), F32), S((56, LANES), F32), S((56, LANES), F32)),
            [pltpu.VMEM((16, LANES), I32)], table, cons)
        state_f, two = call(
            geometry_kernel,
            (S((8 * len(F_NAMES), LANES), F32), S((devices, part_rows, 1, LANES), F32)),
            [pltpu.VMEM((32, LANES), F32), pltpu.VMEM((32, LANES), F32)],
            state_i, number, head_at, tail_at, got1)
        got2 = share(two)
        got2 = [got2] + [lax.ppermute(got2, "gy", [((i + k) % Y, i) for i in range(Y)]) for k in range(1, Y)]
        got2 = [g.reshape(devices * part_rows, LANES) for g in got2]
        wide = 4 * LANES
        three, pair, force, matrix, keep = call(
            middle_kernel,
            (S((devices, 8, LANES), F32), S((16, LANES), F32), S((3, 3, R, wide), F32), S((3, 25, R, LANES), F32),
             S((24, LANES), F32)),
            [pltpu.VMEM((X, NQ, R, wide), F32)],
            state_f, state_i, got1.reshape(devices, LANES), *got2)
        got3 = share(three).reshape(devices * 8, LANES)
        return call(
            final_kernel,
            (S(old_pos.shape, F32), S(bond_head.shape, F32)),
            [pltpu.VMEM((X, ORDER + 1, R, wide), F32)],
            table, state_f, state_i, got3, pair, force, matrix, keep, *got2)

    return per_device


def solution(mesh):
    return jax.shard_map(
        make_per_device(mesh),
        mesh=mesh,
        in_specs=(
            P(None, "gx", "gy", "gz", None),
            P(None, "gx", "gy", "gz", None),
            P("gx", "gy", "gz", None),
            P("gx", "gy", "gz", None),
            P("gx", "gy", "gz", None),
            P("gx", "gy", "gz", None),
        ),
        out_specs=(P(None, "gx", "gy", "gz", None), P("gx", "gy", "gz", None)),
        check_vma=False,
    )
```
